128 devices in a mesh: grp: 8 (over z, core), col: 16 (over x, y).
Axes of the slice: x: 4, y: 4, z: 4, core: 2. Of those that a mesh axis runs over, the one named last changes fastest.
Arguments:
- x_blocks: bfloat16 [32, 16, 6, 256, 256], P('grp', 'col'), may hold values from -6 to 6
- columns: int32 [32, 16, 6], replicated, may hold values from -1 to 511, as said below
- filter_ids: int32 [32, 16, 6], replicated, may hold values from 0 to 511, as said below
Outputs:
- sign_step: bfloat16 [32, 16, 6, 256, 256], P('grp', 'col')
The draws below stay inside these ranges and needn't reach their ends.
Inputs may be any that keep to these rules, and one draw needn't show every extreme that they name: `columns`: in each block row of the grid, slot 0 holds the row's own id; the other used slots hold distinct ids of block rows at most one step away along each grid dimension, with periodic wrap; used slots come first, then -1; at least 3 slots are used. `filter_ids`: in each block row, slot 0 holds the row's own id and the others distinct ids of block rows at most one step away along each grid dimension, with periodic wrap.
All inputs are finite; a program needn't handle non-finite values.
Results may differ from the reference program's by a relative error of at most 0.0019.
Values may be sent and summed in bfloat16 or wider, within the bound.
A program may use at most 128 MiB of HBM per device.

```python
import jax
import jax.numpy as jnp
from jax import lax

B = 256
KB = 6
KF = 6
NA = 32
NBC = 16


def neighbour_ids(key, slots):
    total_rows = NA * NBC
    row_keys = jax.random.split(key, total_rows)
    shuffled = jax.vmap(lambda one_key: jax.random.permutation(one_key, 8))(row_keys)
    others = shuffled + (shuffled >= 4).astype(shuffled.dtype)
    offset_code = jnp.concatenate([jnp.full((total_rows, 1), 4, jnp.int32), others.astype(jnp.int32)], axis=1)[:, :slots]
    step_a = offset_code // 3 - 1
    step_c = offset_code % 3 - 1
    row_index = jnp.arange(total_rows, dtype=jnp.int32)
    home_a = row_index // NBC
    home_c = row_index % NBC
    block_ids = (home_a[:, None] + step_a) % NA * NBC + (home_c[:, None] + step_c) % NBC
    return block_ids.astype(jnp.int32)


def draw_columns(key, part):
    total_rows = NA * NBC
    block_ids = neighbour_ids(jax.random.fold_in(key, 11), KB)
    counts = jax.random.randint(jax.random.fold_in(key, 12), (total_rows, 1), 3, KB + 1)
    slot_index = jnp.arange(KB, dtype=jnp.int32)[None, :]
    block_ids = jnp.where(slot_index < counts, block_ids, -1)
    return block_ids.reshape(NA, NBC, KB).astype(jnp.int32)


def draw_filter_ids(key, part):
    block_ids = neighbour_ids(jax.random.fold_in(key, 21), KF)
    return block_ids.reshape(NA, NBC, KF).astype(jnp.int32)


def level_of(stream_key, shape, pieces, low, top_value):
    gain = 1.0
    for axis_at, blocks in pieces:
        draws = jax.random.uniform(jax.random.fold_in(jax.random.fold_in(stream_key, 6), axis_at), (blocks,), jnp.float32, low / len(pieces), top_value / len(pieces))
        gain = gain * jnp.repeat(jnp.exp(draws), shape[axis_at] // blocks).reshape((-1,) + (1,) * (len(shape) - 1 - axis_at))
    return gain


def bell_draw(key, shape, scale, most, cuts=(), kind=jnp.bfloat16):
    loudness = level_of(key, shape, cuts, -0.22, 0.18) if cuts else 1.0
    values = jax.random.normal(key, shape, jnp.float32) * scale * loudness
    return jnp.minimum(jnp.maximum(values, -most), most).astype(kind)


def setup_inputs(seed: int = 0) -> dict:
    key_of = jax.random.split(jax.random.key(seed), 4)
    return {
        "x_blocks": bell_draw(key_of[0], (NA, NBC, KB, B, B), 1.0, 6.0, ((0, 8), (1, 16))),
        "columns": draw_columns(jax.random.fold_in(key_of[3], 71), 0),
        "filter_ids": draw_filter_ids(jax.random.fold_in(key_of[3], 71), 0),
    }


def locate(stored, wanted):
    matches = stored[:, None, :] == wanted[None, :, None]
    present = jnp.any(matches, axis=2) & (wanted[None, :] >= 0)
    slot_of = jnp.argmax(matches.astype(jnp.int32), axis=2).astype(jnp.int32)
    return slot_of, present


def reference(x_blocks, columns, filter_ids):
    total_rows = NA * NBC
    blocks = x_blocks.reshape(total_rows, KB, B, B)
    col_table = columns.reshape(total_rows, KB)
    filt_table = filter_ids.reshape(total_rows, KF)

    def square_row(row_index):
        row_cols = col_table[row_index]
        in_use = row_cols >= 0
        source = jnp.where(in_use, row_cols, 0)
        slot_of, present = locate(col_table[source], filt_table[row_index])
        present = present & in_use[:, None]
        picked = blocks[source[:, None], slot_of].astype(jnp.float32) * present[:, :, None, None].astype(jnp.float32)
        own = blocks[row_index].astype(jnp.float32)
        return jnp.einsum("kab,kfbc->fac", own, picked).astype(jnp.bfloat16)

    square = lax.map(square_row, jnp.arange(total_rows, dtype=jnp.int32))

    def sign_row(row_index):
        row_cols = col_table[row_index]
        in_use = row_cols >= 0
        source = jnp.where(in_use, row_cols, 0)
        slot_of, present = locate(filt_table[source], row_cols)
        present = present & in_use[:, None]
        picked = square[source[:, None], slot_of].astype(jnp.float32) * present[:, :, None, None].astype(jnp.float32)
        own = blocks[row_index].astype(jnp.float32)
        cubed = jnp.einsum("kab,kjbc->jac", own, picked)
        result = (1.5 * own - cubed * (0.5 / (KB * B))) * in_use[:, None, None].astype(jnp.float32)
        return result.astype(jnp.bfloat16)

    updated = lax.map(sign_row, jnp.arange(total_rows, dtype=jnp.int32))
    return updated.reshape(NA, NBC, KB, B, B)
```

```python
import functools

import jax
import jax.numpy as jnp
from jax import lax
from jax.experimental import pallas as pl
from jax.experimental.pallas import tpu as pltpu
from jax.sharding import PartitionSpec as P

B = 256
KB = 6
KF = 6
RA = 4
OWN = RA * KB
CR = 2 * RA + 2
COLN = CR * KB
ZERO = COLN
FIRST = 5
LEVELS = ((13, 16), (16, 20))

SRC1, SRC2, PICK1, PICK2, USED = 0, 64, 128, 272, 416
MESH = pl.DeviceIdType.MESH


def padded(cells, sides, width):
    for axis, dim in sides:
        count = lax.axis_size(axis)
        head = lax.slice_in_dim(cells, 0, width, axis=dim)
        tail = lax.slice_in_dim(cells, cells.shape[dim] - width, cells.shape[dim], axis=dim)
        cells = jnp.concatenate(
            [
                lax.ppermute(tail, axis, [(i, (i + 1) % count) for i in range(count)]),
                cells,
                lax.ppermute(head, axis, [((i + 1) % count, i) for i in range(count)]),
            ],
            axis=dim,
        )
    return cells


def block_terms(
    halo, pos_a, pos_c, row_ids, row_cols, left_blocks, stored_table, wanted, grid_a, grid_c
):
    slot_count = halo.shape[2]
    width = halo.shape[3]
    in_use = row_cols >= 0
    source = jnp.where(in_use, row_cols, 0)
    home_a = row_ids // grid_c
    home_c = row_ids % grid_c
    step_a = (source // grid_c - home_a[:, None] + 1) % grid_a - 1
    step_c = (source % grid_c - home_c[:, None] + 1) % grid_c - 1
    place = (pos_a[:, None] + step_a) * halo.shape[1] + pos_c[:, None] + step_c
    flat = halo.reshape((halo.shape[0] * halo.shape[1] * slot_count, width, width))
    stored = stored_table[source]
    matches = stored[:, :, None, :] == wanted[:, None, :, None]
    present = jnp.any(matches, axis=3) & (wanted[:, None, :] >= 0) & in_use[:, :, None]
    slot_of = jnp.argmax(matches.astype(jnp.int32), axis=3)
    block_index = place[:, :, None] * slot_count + slot_of

    def one_row(inputs):
        index_row, present_row, left_row = inputs
        picked = flat[index_row]
        picked = jnp.where(present_row[:, :, None, None], picked, jnp.zeros((), picked.dtype))
        return jnp.einsum("kab,kfbc->fac", left_row, picked, preferred_element_type=jnp.float32)

    return lax.map(one_row, (block_index, present, left_blocks))


def dense(x_blocks, columns, filter_ids):
    grp_count = lax.axis_size("grp")
    col_count = lax.axis_size("col")
    rows_a = x_blocks.shape[0]
    rows_c = x_blocks.shape[1]
    grid_a = rows_a * grp_count
    grid_c = rows_c * col_count
    col_table = columns.reshape(grid_a * grid_c, KB)
    filt_table = filter_ids.reshape(grid_a * grid_c, KF)
    local_rows = rows_a * rows_c
    offsets = jnp.arange(local_rows, dtype=jnp.int32)
    local_a = offsets // rows_c
    local_c = offsets % rows_c
    row_ids = (
        (lax.axis_index("grp") * rows_a + local_a) * grid_c
        + lax.axis_index("col") * rows_c
        + local_c
    )
    row_cols = col_table[row_ids]
    left_blocks = x_blocks.reshape(local_rows, KB, B, B)
    along_col = padded(x_blocks, (("col", 1),), 1)
    near_x = padded(along_col, (("grp", 0),), 1)
    square = block_terms(
        near_x,
        local_a + 1,
        local_c + 1,
        row_ids,
        row_cols,
        left_blocks,
        col_table,
        filt_table[row_ids],
        grid_a,
        grid_c,
    ).astype(jnp.bfloat16)
    square = square.reshape(rows_a, rows_c, KF, B, B)
    square_along = padded(square, (("col", 1),), 1)
    near_square = padded(square_along, (("grp", 0),), 1)
    cubed = block_terms(
        near_square,
        local_a + 1,
        local_c + 1,
        row_ids,
        row_cols,
        left_blocks,
        filt_table,
        row_cols,
        grid_a,
        grid_c,
    )
    in_use = (row_cols >= 0).astype(jnp.float32)
    result = (1.5 * left_blocks.astype(jnp.float32) - cubed * (0.5 / (KB * B))) * in_use[
        :, :, None, None
    ]
    return result.astype(jnp.bfloat16).reshape(x_blocks.shape)


def list_codes(columns, filter_ids):
    grid_a, grid_c, _ = columns.shape
    chips = grid_a // (2 * RA)
    ids = (
        lax.broadcasted_iota(jnp.int32, (grid_a, grid_c), 0) * grid_c
        + lax.broadcasted_iota(jnp.int32, (grid_a, grid_c), 1)
    )
    row_in_chip = lax.broadcasted_iota(jnp.int32, (grid_a, grid_c, 1), 0) % (2 * RA)
    own, halo = [], []
    for step_c in (1, -1):
        found = []
        for step_a in (-1, 0, 1):
            cols_r = jnp.roll(columns, (-step_a, -step_c), (0, 1))
            filt_r = jnp.roll(filter_ids, (-step_a, -step_c), (0, 1))
            member = jnp.any(cols_r == ids[:, :, None], axis=2)[:, :, None]
            one = jnp.any(columns[:, :, :, None] == filt_r[:, :, None, :], axis=3) & (columns >= 0)
            two = jnp.any(filter_ids[:, :, :, None] == cols_r[:, :, None, :], axis=3)
            found.append((one & member, two & member))
        up, mid, down = found
        for phase in (0, 1):
            first = row_in_chip == 0
            last = row_in_chip == 2 * RA - 1
            own.append(mid[phase] | (up[phase] & ~first) | (down[phase] & ~last))
            halo.append((up[phase] & first) | (down[phase] & last))
    shape = (2, 2, chips, 2 * RA, grid_c, KB)
    own = jnp.stack(own).reshape(shape).swapaxes(0, 1)
    halo = jnp.stack(halo).reshape(shape).swapaxes(0, 1)
    above = jnp.roll(halo[:, :, :, -1:], 1, axis=2)
    below = jnp.roll(halo[:, :, :, :1], -1, axis=2)
    need = jnp.concatenate([above, own, below], axis=3)
    flags = need.astype(jnp.int32)
    in_row = jnp.cumsum(flags, axis=5) - flags
    per_row = flags.sum(axis=5, keepdims=True)
    row0 = [per_row[:, :, :, i : i + 1] for i in range(CR)]
    n0 = row0[1] + row0[2] + row0[3] + row0[4]
    n1 = row0[5] + row0[6] + row0[7] + row0[8]
    total = n0 + n1 + row0[0] + row0[9]
    half = (total + 1) // 2
    base = [n0]
    run = jnp.zeros_like(n0)
    for i in range(1, 5):
        base.append(run)
        run = run + row0[i]
    back = jnp.zeros_like(n0)
    ends = []
    for i in range(5, 9):
        ends.append(back)
        back = back + row0[i]
    front = jnp.concatenate(base, axis=3) + in_row[:, :, :, 0:5]
    rear = total - 1 - (jnp.concatenate(ends, axis=3) + in_row[:, :, :, 5:9])
    last_halo = n0 + row0[0] + in_row[:, :, :, 9:10]
    place = jnp.concatenate([front, rear, last_halo], axis=3)
    row = lax.broadcasted_iota(jnp.int32, place.shape, 3)
    of0 = (row >= 1) & (row <= 4)
    of1 = (row >= 5) & (row <= 8)
    slot0 = jnp.where(of0, place, place + jnp.maximum(FIRST - n0, 0))
    turned = total - 1 - place
    slot1 = jnp.where(of1, turned, turned + jnp.maximum(FIRST - n1, 0))
    core = (place >= half).astype(jnp.int32)
    slot = jnp.where(core == 0, slot0, slot1)
    most = jnp.max(jnp.where(need, slot + 1, 0), axis=(1, 2, 3, 4, 5))
    return need, core * 32 + slot, most


def tables(columns, filter_ids, need, code, grp, col):
    grid_a, grid_c, _ = columns.shape
    z = grp // 2
    core = grp % 2
    near_c = jnp.stack([(col - 1) % grid_c, col, (col + 1) % grid_c])
    chip_need = need[:, :, z]
    chip_code = code[:, :, z]
    mine_need = chip_need[:, :, :, col].reshape(2, 2, COLN)
    mine_code = chip_code[:, :, :, col].reshape(2, 2, COLN)
    wanted_code = core * 32 + jnp.arange(32, dtype=jnp.int32)
    hit = mine_need[:, :, None, :] & (mine_code[:, :, None, :] == wanted_code[None, None, :, None])
    entries = jnp.arange(COLN, dtype=jnp.int32)
    source = jnp.sum(jnp.where(hit, entries, 0), axis=3)
    rows_a = (grp * RA - 1 + jnp.arange(RA + 2, dtype=jnp.int32)) % grid_a
    col_near = columns[rows_a][:, near_c]
    filt_near = filter_ids[rows_a][:, near_c]
    row_ids = rows_a[:, None] * grid_c + near_c[None, :]
    left = lax.dynamic_slice_in_dim(chip_code[:, 0, :, near_c[0]], core * RA, RA + 2, axis=1)
    right = lax.dynamic_slice_in_dim(chip_code[:, 1, :, near_c[2]], core * RA, RA + 2, axis=1)
    middle = (core * RA * KB + jnp.arange((RA + 2) * KB, dtype=jnp.int32)).reshape(RA + 2, KB)
    middle = jnp.broadcast_to(middle, (2, RA + 2, KB))
    held = jnp.stack([left + 64, middle, right + 128], axis=2)
    row_cols = col_near[1 : RA + 1, 1]
    row_filt = filt_near[1 : RA + 1, 1]

    def picks(stored, wanted, where):
        near = jnp.stack([stored[i : i + 3] for i in range(RA)])
        spot = jnp.stack([where[i : i + 3] for i in range(RA)])
        name = jnp.stack([row_ids[i : i + 3] for i in range(RA)])
        near = near.reshape(RA, 1, 1, 9, 6)
        spot = spot.reshape(RA, 1, 1, 9, 6)
        name = name.reshape(RA, 1, 1, 9, 1)
        same = (row_cols[:, None, :, None, None] == name) & (near == wanted[:, :, None, None, None])
        return ZERO + jnp.sum(jnp.where(same, spot - ZERO, 0), axis=(3, 4))

    pick1 = picks(col_near, row_filt, held[0])
    pick2 = picks(filt_near, row_cols, held[1])
    used = (row_cols >= 0).astype(jnp.int32)
    parts = [source, pick1, pick2, used]
    return jnp.concatenate([p.astype(jnp.int32).reshape(-1) for p in parts])


def kernel(q1, q2, grp_count, col_count, idx, x_hbm, out_hbm, xv, colp1, rcv1, snd1, colp2, rcv2,
           snd2, sown, outv, lsem, osem, zsem, hs1, hr1, fs1, fr1, hs2, hr2, fs2, fr2):
    grp = lax.axis_index("grp")
    col = lax.axis_index("col")
    core = lax.rem(grp, 2)
    partner = (grp + 1 - 2 * core, col)
    zpeer = (lax.rem(grp + grp_count - 1 + 2 * core, grp_count), col)
    right = (grp, lax.rem(col + 1, col_count))
    left = (grp, lax.rem(col + col_count - 1, col_count))
    own0 = (1 + RA * core) * KB
    zout = (RA - 1) * core * KB
    zdst = (CR - 1) * (1 - core) * KB
    zin = (CR - 1) * core * KB

    to_xv = pltpu.make_async_copy(x_hbm, xv, lsem.at[0])
    to_col = pltpu.make_async_copy(x_hbm, colp1.at[pl.ds(own0, OWN)], lsem.at[1])
    to_xv.start()
    to_col.start()

    barrier = pltpu.get_barrier_semaphore()
    for peer in (partner, zpeer, right, left):
        pl.semaphore_signal(barrier, inc=1, device_id=peer, device_id_type=MESH)
    pl.semaphore_wait(barrier, 4)

    def remote(src, dst, send, recv, device):
        return pltpu.make_async_remote_copy(
            src_ref=src, dst_ref=dst, send_sem=send, recv_sem=recv,
            device_id=device, device_id_type=MESH,
        )

    def zsend(src, colp, p):
        return remote(src.at[pl.ds(zout, KB)], colp.at[pl.ds(zdst, KB)],
                      zsem.at[p, 0], zsem.at[p, 1], zpeer)

    def zfwd(colp, p):
        here = colp.at[pl.ds(zin, KB)]
        return remote(here, here, zsem.at[p, 2], zsem.at[p, 3], partner)

    def share(src, colp, p):
        return remote(src, colp.at[pl.ds(own0, OWN)], zsem.at[p, 4], zsem.at[p, 5], partner)

    def hop(snd, rcv, hs, hr, d, s):
        return remote(snd.at[d, s], rcv.at[2 * d + core, s], hs.at[d, s], hr.at[d, s],
                      (right, left)[d])

    def fwd(rcv, fs, fr, d, s):
        here = rcv.at[2 * d + core, s]
        return remote(here, here, fs.at[d, s], fr.at[d, s], partner)

    def right_factor(colp, rcv, v):
        is_col = v < 64
        at_col = jnp.where(is_col, v, ZERO)
        at_rcv = jnp.where(is_col, 0, v - 64)
        return jnp.where(is_col, colp[at_col], rcv[at_rcv >> 5, at_rcv & 31])

    def product(colp, rcv, table, row, entry):
        acc = None
        for k in range(KB):
            v = idx[table + entry * KB + k]
            term = jnp.dot(xv[row * KB + k], right_factor(colp, rcv, v),
                           preferred_element_type=jnp.float32)
            acc = term if acc is None else acc + term
        return acc

    def list_entry(table, d, s):
        return jnp.clip(idx[table + d * 32 + s] - own0, 0, OWN - 1)

    zero = jnp.zeros((B, B), jnp.bfloat16)

    to_xv.wait()
    zs1, zf1, sh1 = zsend(xv, colp1, 0), zfwd(colp1, 0), share(xv, colp1, 0)
    zs1.start()
    sh1.start()
    hop1 = functools.partial(hop, snd1, rcv1, hs1, hr1)
    fwd1 = functools.partial(fwd, rcv1, fs1, fr1)

    @pl.loop(0, FIRST)
    def _(s):
        for d in range(2):
            snd1[d, s] = xv[list_entry(SRC1, d, s)]

        @pl.when(s > 0)
        def _():
            for d in range(2):
                hop1(d, s - 1).start()

    colp1[ZERO] = zero
    colp2[ZERO] = zero
    for d in range(2):
        hop1(d, FIRST - 1).start()
    to_col.wait()
    zs1.wait_recv()
    zf1.start()
    sh1.wait_recv()
    zf1.wait_recv()

    @pl.loop(FIRST, q1)
    def _(s):
        for d in range(2):
            snd1[d, s] = colp1[idx[SRC1 + d * 32 + s]]

        @pl.when(s > FIRST)
        def _():
            for d in range(2):
                hop1(d, s - 1).start()

    for d in range(2):
        hop1(d, q1 - 1).start()

    @pl.loop(0, q1)
    def _(s):
        for d in range(2):
            hop1(d, s).wait_recv()
            fwd1(d, s).start()

    @pl.loop(0, q1)
    def _(s):
        for d in range(2):
            fwd1(d, s).wait_recv()

    zs2, zf2, sh2 = zsend(sown, colp2, 1), zfwd(colp2, 1), share(sown, colp2, 1)
    hop2 = functools.partial(hop, snd2, rcv2, hs2, hr2)
    fwd2 = functools.partial(fwd, rcv2, fs2, fr2)

    @pl.loop(0, 2)
    def _(s):
        for d in range(2):
            entry = list_entry(SRC2, d, s)
            snd2[d, s] = product(colp1, rcv1, PICK1, entry // KB, entry).astype(jnp.bfloat16)

        @pl.when(s > 0)
        def _():
            for d in range(2):
                hop2(d, s - 1).start()

    @pl.loop(0, OWN // 2)
    def _(t):
        step = t // 3
        row = step + core * (RA - 1 - 2 * step)
        for u in range(2):
            entry = row * KB + (t - 3 * step) * 2 + u
            block = product(colp1, rcv1, PICK1, row, entry).astype(jnp.bfloat16)
            sown[entry] = block
            colp2[own0 + entry] = block

        @pl.when(t == 0)
        def _():
            for d in range(2):
                hop2(d, 1).start()

        @pl.when(t == 3)
        def _():
            zs2.start()

    @pl.loop(2, FIRST)
    def _(s):
        for d in range(2):
            snd2[d, s] = sown[list_entry(SRC2, d, s)]

        @pl.when(s > 2)
        def _():
            for d in range(2):
                hop2(d, s - 1).start()

    sh2.start()
    for d in range(2):
        hop2(d, FIRST - 1).start()
    zs2.wait_recv()
    zf2.start()
    sh2.wait_recv()
    zf2.wait_recv()

    @pl.loop(FIRST, q2)
    def _(s):
        for d in range(2):
            snd2[d, s] = colp2[idx[SRC2 + d * 32 + s]]

        @pl.when(s > FIRST)
        def _():
            for d in range(2):
                hop2(d, s - 1).start()

    for d in range(2):
        hop2(d, q2 - 1).start()

    @pl.loop(0, q2)
    def _(s):
        for d in range(2):
            hop2(d, s).wait_recv()
            fwd2(d, s).start()

    @pl.loop(0, q2)
    def _(s):
        for d in range(2):
            fwd2(d, s).wait_recv()

    def write(row):
        rows = pl.ds(row * KB, KB)
        return pltpu.make_async_copy(outv.at[rows], out_hbm.at[rows], osem.at[row])

    @pl.loop(0, OWN // 2)
    def _(t):
        row = t // 3
        for u in range(2):
            entry = 2 * t + u
            cubed = product(colp2, rcv2, PICK2, row, entry)
            in_use = idx[USED + entry].astype(jnp.float32)
            own = xv[entry].astype(jnp.float32)
            outv[entry] = ((1.5 * own - cubed * (0.5 / (KB * B))) * in_use).astype(jnp.bfloat16)

        @pl.when((t > 0) & (t - 3 * row == 0))
        def _():
            write(row - 1).start()

    zs1.wait_send()
    zf1.wait_send()
    sh1.wait_send()
    zs2.wait_send()
    zf2.wait_send()
    sh2.wait_send()

    @pl.loop(0, q1)
    def _(s):
        for d in range(2):
            hop1(d, s).wait_send()
            fwd1(d, s).wait_send()

    @pl.loop(0, q2)
    def _(s):
        for d in range(2):
            hop2(d, s).wait_send()
            fwd2(d, s).wait_send()

    write(RA - 1).start()
    for row in range(RA):
        write(row).wait()


def sparse(level, x_blocks, index):
    q1, q2 = LEVELS[level]
    blocks = x_blocks.reshape(OWN, B, B)
    vm = lambda *lead: pltpu.VMEM((*lead, B, B), jnp.bfloat16)
    dma = lambda *lead: pltpu.SemaphoreType.DMA(lead)
    out = pl.pallas_call(
        functools.partial(kernel, q1, q2, lax.axis_size("grp"), lax.axis_size("col")),
        out_shape=jax.ShapeDtypeStruct(blocks.shape, jnp.bfloat16),
        in_specs=[
            pl.BlockSpec(memory_space=pltpu.SMEM),
            pl.BlockSpec(memory_space=pl.ANY),
        ],
        out_specs=pl.BlockSpec(memory_space=pl.ANY),
        scratch_shapes=[
            vm(OWN), vm(COLN + 1), vm(4, q1), vm(2, q1), vm(COLN + 1), vm(4, q2), vm(2, q2),
            vm(OWN), vm(OWN),
            dma(2), dma(RA), dma(2, 6),
            dma(2, q1), dma(2, q1), dma(2, q1), dma(2, q1),
            dma(2, q2), dma(2, q2), dma(2, q2), dma(2, q2),
        ],
        compiler_params=pltpu.CompilerParams(
            collective_id=level, has_side_effects=True, vmem_limit_bytes=62 * 1024 * 1024
        ),
        name=f"sign_step_{q1}_{q2}",
    )(index, blocks)
    return out.reshape(x_blocks.shape)


def local(x_blocks, columns, filter_ids):
    grp = lax.axis_index("grp")
    col = lax.axis_index("col")
    need, code, most = list_codes(columns, filter_ids)
    index = tables(columns, filter_ids, need, code, grp, col)
    level = jnp.int32(len(LEVELS))
    for at in reversed(range(len(LEVELS))):
        fits = (most[0] <= LEVELS[at][0]) & (most[1] <= LEVELS[at][1])
        level = jnp.where(fits, at, level)
    branches = [
        functools.partial(lambda at, x, c, f, i: sparse(at, x, i), at)
        for at in range(len(LEVELS))
    ]
    branches.append(lambda x, c, f, i: dense(x, c, f))
    return lax.switch(level, branches, x_blocks, columns, filter_ids, index)


def solution(mesh):
    return jax.shard_map(
        local,
        mesh=mesh,
        in_specs=(P("grp", "col", None, None, None), P(), P()),
        out_specs=P("grp", "col", None, None, None),
        check_vma=False,
    )
```

```python
import functools

import jax
import jax.numpy as jnp
from jax import lax
from jax.experimental import pallas as pl
from jax.experimental.pallas import tpu as pltpu
from jax.sharding import PartitionSpec as P

B = 256
KB = 6
KF = 6
RA = 4
OWN = RA * KB
CR = 2 * RA + 2
COLN = CR * KB
ZERO = COLN
FIRST = 5
LEVELS = ((13, 15), (13, 16), (14, 17), (16, 20))

PICKS = OWN * KB
MESH = pl.DeviceIdType.MESH


def padded(cells, sides, width):
    for axis, dim in sides:
        count = lax.axis_size(axis)
        head = lax.slice_in_dim(cells, 0, width, axis=dim)
        tail = lax.slice_in_dim(cells, cells.shape[dim] - width, cells.shape[dim], axis=dim)
        cells = jnp.concatenate(
            [
                lax.ppermute(tail, axis, [(i, (i + 1) % count) for i in range(count)]),
                cells,
                lax.ppermute(head, axis, [((i + 1) % count, i) for i in range(count)]),
            ],
            axis=dim,
        )
    return cells


def block_terms(
    halo, pos_a, pos_c, row_ids, row_cols, left_blocks, stored_table, wanted, grid_a, grid_c
):
    slot_count = halo.shape[2]
    width = halo.shape[3]
    in_use = row_cols >= 0
    source = jnp.where(in_use, row_cols, 0)
    home_a = row_ids // grid_c
    home_c = row_ids % grid_c
    step_a = (source // grid_c - home_a[:, None] + 1) % grid_a - 1
    step_c = (source % grid_c - home_c[:, None] + 1) % grid_c - 1
    place = (pos_a[:, None] + step_a) * halo.shape[1] + pos_c[:, None] + step_c
    flat = halo.reshape((halo.shape[0] * halo.shape[1] * slot_count, width, width))
    stored = stored_table[source]
    matches = stored[:, :, None, :] == wanted[:, None, :, None]
    present = jnp.any(matches, axis=3) & (wanted[:, None, :] >= 0) & in_use[:, :, None]
    slot_of = jnp.argmax(matches.astype(jnp.int32), axis=3)
    block_index = place[:, :, None] * slot_count + slot_of

    def one_row(inputs):
        index_row, present_row, left_row = inputs
        picked = flat[index_row]
        picked = jnp.where(present_row[:, :, None, None], picked, jnp.zeros((), picked.dtype))
        return jnp.einsum("kab,kfbc->fac", left_row, picked, preferred_element_type=jnp.float32)

    return lax.map(one_row, (block_index, present, left_blocks))


def dense(x_blocks, columns, filter_ids):
    grp_count = lax.axis_size("grp")
    col_count = lax.axis_size("col")
    rows_a = x_blocks.shape[0]
    rows_c = x_blocks.shape[1]
    grid_a = rows_a * grp_count
    grid_c = rows_c * col_count
    col_table = columns.reshape(grid_a * grid_c, KB)
    filt_table = filter_ids.reshape(grid_a * grid_c, KF)
    local_rows = rows_a * rows_c
    offsets = jnp.arange(local_rows, dtype=jnp.int32)
    local_a = offsets // rows_c
    local_c = offsets % rows_c
    row_ids = (
        (lax.axis_index("grp") * rows_a + local_a) * grid_c
        + lax.axis_index("col") * rows_c
        + local_c
    )
    row_cols = col_table[row_ids]
    left_blocks = x_blocks.reshape(local_rows, KB, B, B)
    along_col = padded(x_blocks, (("col", 1),), 1)
    near_x = padded(along_col, (("grp", 0),), 1)
    square = block_terms(
        near_x,
        local_a + 1,
        local_c + 1,
        row_ids,
        row_cols,
        left_blocks,
        col_table,
        filt_table[row_ids],
        grid_a,
        grid_c,
    ).astype(jnp.bfloat16)
    square = square.reshape(rows_a, rows_c, KF, B, B)
    square_along = padded(square, (("col", 1),), 1)
    near_square = padded(square_along, (("grp", 0),), 1)
    cubed = block_terms(
        near_square,
        local_a + 1,
        local_c + 1,
        row_ids,
        row_cols,
        left_blocks,
        filt_table,
        row_cols,
        grid_a,
        grid_c,
    )
    in_use = (row_cols >= 0).astype(jnp.float32)
    result = (1.5 * left_blocks.astype(jnp.float32) - cubed * (0.5 / (KB * B))) * in_use[
        :, :, None, None
    ]
    return result.astype(jnp.bfloat16).reshape(x_blocks.shape)


LANES = 128
LISTS = 8
CODE_ROW = 0
NEAR_ROW = 48
SRC_ROW = 96
TABLE_ROWS = 128


def index_kernel(cols_ref, filt_ref, table_ref, most_ref, own_ref, halo_ref, cols_s, filt_s):
    grp = lax.axis_index("grp")
    col = lax.axis_index("col")
    core = lax.rem(grp, 2)
    grid_c = cols_ref.shape[1]
    grid_a = cols_ref.shape[2]
    chip = 2 * RA

    def lanes_of(x):
        return jnp.concatenate([x] * (LANES // grid_a), axis=1)

    stored, kept = [], []
    for m in range(KB):
        stored.append(lanes_of(cols_ref[m]))
        kept.append(lanes_of(filt_ref[m]))
        cols_s[m] = stored[m]
        filt_s[m] = kept[m]
    shape = (grid_c, LANES)
    lane = lax.broadcasted_iota(jnp.int32, shape, 1)
    ids = lax.rem(lane, grid_a) * grid_c + lax.broadcasted_iota(jnp.int32, shape, 0)
    in_chip = lax.rem(lane, chip)
    first, last = in_chip == 0, in_chip == chip - 1
    false = jnp.zeros(shape, jnp.int32)

    def either(tests):
        got = tests[0]
        for t in tests[1:]:
            got = got | t
        return got

    totals = []
    for d, step_c in enumerate((1, -1)):
        cols_c = [jnp.roll(x, -step_c, 0) for x in stored]
        filt_c = [jnp.roll(x, -step_c, 0) for x in kept]
        found = []
        for step_a in (-1, 0, 1):
            shift = (-step_a) % LANES
            cols_r = [pltpu.roll(x, shift, 1) if shift else x for x in cols_c]
            filt_r = [pltpu.roll(x, shift, 1) if shift else x for x in filt_c]
            member = either([x == ids for x in cols_r])
            one = [either([stored[m] == x for x in filt_r]) & member & (stored[m] >= 0) for m in range(KB)]
            two = [either([kept[m] == x for x in cols_r]) & member for m in range(KB)]
            found.append((one, two))
        up, mid, down = found
        for phase in (0, 1):
            own_row, halo_row = false, false
            for m in range(KB):
                u, c, w = up[phase][m], mid[phase][m], down[phase][m]
                own = (c | (u & ~first) | (w & ~last)).astype(jnp.int32)
                halo = ((u & first) | (w & last)).astype(jnp.int32)
                own_ref[phase, d, m] = own
                halo_ref[phase, d, m] = halo
                own_row = own_row + own
                halo_row = halo_row + halo
            totals.append((phase, own_row, halo_row))

    def summed(x, rule):
        at = lax.broadcasted_iota(jnp.int32, (LANES, LANES), 0)
        to = lax.broadcasted_iota(jnp.int32, (LANES, LANES), 1)
        weight = rule(at, to).astype(jnp.float32).astype(jnp.bfloat16)
        return jnp.dot(
            x.astype(jnp.float32).astype(jnp.bfloat16), weight, preferred_element_type=jnp.float32
        ).astype(jnp.int32)

    def split(n0, n1, total):
        half = (total + 1) // 2
        return half, jnp.maximum(FIRST - n0, 0), jnp.maximum(FIRST - n1, 0)

    own_all = jnp.concatenate([t[1] for t in totals], axis=0)
    halo_all = jnp.concatenate([t[2] for t in totals], axis=0)

    def same_chip(at, to):
        return (at // chip == lax.rem(to, grid_a) // chip) & (at < grid_a)

    def beside(at, to):
        z = lax.rem(to, grid_a) // chip * chip
        above = lax.rem(z + grid_a - 1, grid_a)
        below = lax.rem(z + chip, grid_a)
        return (at == above) | (at == below)

    n0 = summed(own_all, lambda at, to: same_chip(at, to) & (lax.rem(at, chip) < RA))
    n1 = summed(own_all, lambda at, to: same_chip(at, to) & (lax.rem(at, chip) >= RA))
    total = n0 + n1 + summed(halo_all, beside)
    half, gap0, gap1 = split(n0, n1, total)
    rest = total - half
    fill = jnp.maximum(
        half + jnp.where(half > n0, gap0, 0), rest + jnp.where(rest > n1, gap1, 0)
    )
    for p, (phase, _, _) in enumerate(totals):
        most_ref[p] = jnp.max(fill[p * grid_c : (p + 1) * grid_c])

    z = grp // 2
    shift = lax.rem(LANES + 1 - z * chip, LANES)
    west = lax.rem(col + grid_c - 1, grid_c)
    east = lax.rem(col + 1, grid_c)
    row8 = (LISTS, LANES)
    lane8 = lax.broadcasted_iota(jnp.int32, row8, 1)
    rim = (lane8 == 0) | (lane8 == CR - 1)
    lists = [(p, d, c) for p in (0, 1) for d, c in ((0, col), (1, col), (0, west), (1, east))]

    def near(ref_rows):
        return pltpu.roll(jnp.concatenate(ref_rows, axis=0), shift, 1)

    need, in_row = [], []
    run = jnp.zeros(row8, jnp.int32)
    for m in range(KB):
        own = near([own_ref[p, d, m, pl.ds(c, 1), :] for p, d, c in lists])
        halo = near([halo_ref[p, d, m, pl.ds(c, 1), :] for p, d, c in lists])
        flags = jnp.where(lane8 < CR, jnp.where(rim, halo, own), 0)
        need.append(flags)
        in_row.append(run)
        run = run + flags
        rows = [cols_s[m, pl.ds(c, 1), :] for c in (west, col, east)]
        rows += [filt_s[m, pl.ds(c, 1), :] for c in (west, col, east)]
        table_ref[pl.ds(NEAR_ROW + 8 * m, 8), :] = near(rows + rows[:2])
    n0 = summed(run, lambda at, to: (at >= 1) & (at <= RA))
    n1 = summed(run, lambda at, to: (at > RA) & (at <= chip))
    above = summed(run, lambda at, to: at == 0)
    below = summed(run, lambda at, to: at == CR - 1)
    ahead = summed(
        run, lambda at, to: (at < to) & (((at >= 1) & (to <= RA)) | ((at > RA) & (to <= chip)))
    )
    total = n0 + n1 + above + below
    half, gap0, gap1 = split(n0, n1, total)
    of0 = (lane8 >= 1) & (lane8 <= RA)
    of1 = (lane8 > RA) & (lane8 <= chip)
    slots = lax.broadcasted_iota(jnp.int32, (32, LANES), 0) + core * 32
    entry = lax.broadcasted_iota(jnp.int32, (32, LANES), 1) * KB
    source = [jnp.zeros((32, LANES), jnp.int32) for _ in range(4)]
    for m in range(KB):
        place = ahead + in_row[m]
        place = jnp.where(lane8 == 0, n0 + in_row[m], place)
        place = jnp.where(lane8 == CR - 1, n0 + above + in_row[m], place)
        place = jnp.where(of1, total - 1 - place, place)
        turned = total - 1 - place
        slot0 = place + jnp.where(of0, 0, gap0)
        slot1 = turned + jnp.where(of1, 0, gap1)
        code = jnp.where(place < half, slot0, 32 + slot1)
        table_ref[pl.ds(CODE_ROW + 8 * m, 8), :] = code
        sent = jnp.where(need[m] > 0, code, -1)
        for i, at in enumerate((0, 1, 4, 5)):
            same = jnp.broadcast_to(sent[at : at + 1], (32, LANES)) == slots
            source[i] = source[i] + jnp.where(same, entry + m, 0)
    lane32 = lax.broadcasted_iota(jnp.int32, (32, LANES), 1)
    out = jnp.zeros((32, LANES), jnp.int32)
    for i in range(4):
        out = jnp.where(lane32 == i, jnp.sum(source[i], axis=1, keepdims=True), out)
    table_ref[pl.ds(SRC_ROW, 32), :] = out


def list_tables(columns, filter_ids):
    grid_a, grid_c, _ = columns.shape
    ints = lambda *shape: pltpu.VMEM(shape, jnp.int32)
    return pl.pallas_call(
        index_kernel,
        out_shape=(
            jax.ShapeDtypeStruct((TABLE_ROWS, LANES), jnp.int32),
            jax.ShapeDtypeStruct((4,), jnp.int32),
        ),
        in_specs=[pl.BlockSpec(memory_space=pltpu.VMEM)] * 2,
        out_specs=(
            pl.BlockSpec(memory_space=pltpu.VMEM),
            pl.BlockSpec(memory_space=pltpu.SMEM),
        ),
        scratch_shapes=[
            ints(2, 2, KB, grid_c, LANES), ints(2, 2, KB, grid_c, LANES),
            ints(KB, grid_c, LANES), ints(KF, grid_c, LANES),
        ],
        name="block_lists",
    )(columns.transpose(2, 1, 0), filter_ids.transpose(2, 1, 0))


def kernel(q1, q2, grid_a, grid_c, grp_count, col_count, tab, x_hbm, out_hbm, pick, xv, colp1, rcv1, snd1, colp2, rcv2,
           snd2, sown, outv, lsem, osem, zsem, hs1, hr1, fs1, fr1, hs2, hr2, fs2, fr2):
    grp = lax.axis_index("grp")
    col = lax.axis_index("col")
    core = lax.rem(grp, 2)
    partner = (grp + 1 - 2 * core, col)
    zpeer = (lax.rem(grp + grp_count - 1 + 2 * core, grp_count), col)
    right = (grp, lax.rem(col + 1, col_count))
    left = (grp, lax.rem(col + col_count - 1, col_count))
    own0 = (1 + RA * core) * KB
    zout = (RA - 1) * core * KB
    zdst = (CR - 1) * (1 - core) * KB
    zin = (CR - 1) * core * KB

    to_xv = pltpu.make_async_copy(x_hbm, xv, lsem.at[0])
    to_col = pltpu.make_async_copy(x_hbm, colp1.at[pl.ds(own0, OWN)], lsem.at[1])
    to_xv.start()
    to_col.start()

    barrier = pltpu.get_barrier_semaphore()
    for peer in (partner, zpeer, right, left):
        pl.semaphore_signal(barrier, inc=1, device_id=peer, device_id_type=MESH)
    pl.semaphore_wait(barrier, 4)

    def remote(src, dst, send, recv, device):
        return pltpu.make_async_remote_copy(
            src_ref=src, dst_ref=dst, send_sem=send, recv_sem=recv,
            device_id=device, device_id_type=MESH,
        )

    def zsend(src, colp, p):
        return remote(src.at[pl.ds(zout, KB)], colp.at[pl.ds(zdst, KB)],
                      zsem.at[p, 0], zsem.at[p, 1], zpeer)

    def zfwd(colp, p):
        here = colp.at[pl.ds(zin, KB)]
        return remote(here, here, zsem.at[p, 2], zsem.at[p, 3], partner)

    def share(src, colp, p):
        return remote(src, colp.at[pl.ds(own0, OWN)], zsem.at[p, 4], zsem.at[p, 5], partner)

    def hop(snd, rcv, hs, hr, d, s):
        return remote(snd.at[d, s], rcv.at[2 * d + core, s], hs.at[d, s], hr.at[d, s],
                      (right, left)[d])

    def fwd(rcv, fs, fr, d, s):
        here = rcv.at[2 * d + core, s]
        return remote(here, here, fs.at[d, s], fr.at[d, s], partner)

    def right_factor(colp, rcv, v):
        is_col = v < 64
        at_col = jnp.where(is_col, v, ZERO)
        at_rcv = jnp.where(is_col, 0, v - 64)
        slot = jnp.minimum(at_rcv & 31, rcv.shape[1] - 1)
        return jnp.where(is_col, colp[at_col], rcv[(at_rcv >> 5) & 3, slot])

    def product(colp, rcv, phase, row, entry):
        acc = None
        for k in range(KB):
            v = pick[phase * PICKS + entry * KB + k]
            term = jnp.dot(xv[row * KB + k], right_factor(colp, rcv, v),
                           preferred_element_type=jnp.float32)
            acc = term if acc is None else acc + term
        return acc

    def sent(phase, d, s):
        return tab[SRC_ROW + s, 2 * phase + d]

    def list_entry(phase, d, s):
        return jnp.clip(sent(phase, d, s) - own0, 0, OWN - 1)

    def find_factors(at):
        row = at // KB
        k = at - KB * row
        here = 1 + RA * core + row
        source = tab[NEAR_ROW + 8 * k + 1, here]
        in_use = source >= 0
        source = jnp.where(in_use, source, 0)
        step_a = lax.rem(source // grid_c - (grp * RA + row) + 1 + grid_a, grid_a) - 1
        side = lax.rem(lax.rem(source, grid_c) - col + 1 + grid_c, grid_c)
        step_a = jnp.where(in_use, jnp.clip(step_a, -1, 1), 0)
        side = jnp.where(in_use, jnp.minimum(side, 2), 1)
        there = here + step_a
        for phase in range(2):
            held, spot = [], []
            for m in range(KB):
                held.append(tab[NEAR_ROW + 8 * m + side + 3 * phase, there])
                code = tab[CODE_ROW + 8 * m + 4 * phase + jnp.where(side == 0, 2, 3), there]
                far = code + jnp.where(side == 0, 64, 128)
                spot.append(jnp.where(side == 1, there * KB + m, far))
            for f in range(KF):
                wanted = tab[NEAR_ROW + 8 * f + 1 + 3 * (1 - phase), here]
                usable = in_use & (wanted >= 0)
                got = jnp.int32(ZERO)
                for m in range(KB):
                    got = jnp.where(held[m] == wanted, spot[m], got)
                pick[phase * PICKS + (row * KB + f) * KB + k] = jnp.where(usable, got, ZERO)

    zero = jnp.zeros((B, B), jnp.bfloat16)

    to_xv.wait()
    zs1, zf1, sh1 = zsend(xv, colp1, 0), zfwd(colp1, 0), share(xv, colp1, 0)
    zs1.start()
    sh1.start()
    hop1 = functools.partial(hop, snd1, rcv1, hs1, hr1)
    fwd1 = functools.partial(fwd, rcv1, fs1, fr1)

    @pl.loop(0, FIRST)
    def _(s):
        for d in range(2):
            snd1[d, s] = xv[list_entry(0, d, s)]

        @pl.when(s > 0)
        def _():
            for d in range(2):
                hop1(d, s - 1).start()

    colp1[ZERO] = zero
    colp2[ZERO] = zero
    for d in range(2):
        hop1(d, FIRST - 1).start()
    to_col.wait()
    zs1.wait_recv()
    zf1.start()
    sh1.wait_recv()
    zf1.wait_recv()

    @pl.loop(FIRST, q1)
    def _(s):
        for d in range(2):
            snd1[d, s] = colp1[sent(0, d, s)]

        @pl.when(s > FIRST)
        def _():
            for d in range(2):
                hop1(d, s - 1).start()

    for d in range(2):
        hop1(d, q1 - 1).start()

    pl.loop(0, OWN)(find_factors)

    @pl.loop(0, q1)
    def _(s):
        for d in range(2):
            hop1(d, s).wait_recv()
            fwd1(d, s).start()

    @pl.loop(0, q1)
    def _(s):
        for d in range(2):
            fwd1(d, s).wait_recv()

    zs2, zf2, sh2 = zsend(sown, colp2, 1), zfwd(colp2, 1), share(sown, colp2, 1)
    hop2 = functools.partial(hop, snd2, rcv2, hs2, hr2)
    fwd2 = functools.partial(fwd, rcv2, fs2, fr2)

    @pl.loop(0, 2)
    def _(s):
        for d in range(2):
            entry = list_entry(1, d, s)
            snd2[d, s] = product(colp1, rcv1, 0, entry // KB, entry).astype(jnp.bfloat16)

        @pl.when(s > 0)
        def _():
            for d in range(2):
                hop2(d, s - 1).start()

    @pl.loop(0, OWN // 2)
    def _(t):
        step = t // 3
        row = step + core * (RA - 1 - 2 * step)
        for u in range(2):
            entry = row * KB + (t - 3 * step) * 2 + u
            block = product(colp1, rcv1, 0, row, entry).astype(jnp.bfloat16)
            sown[entry] = block
            colp2[own0 + entry] = block

        @pl.when(t == 0)
        def _():
            for d in range(2):
                hop2(d, 1).start()

        @pl.when(t == 3)
        def _():
            zs2.start()

    @pl.loop(2, FIRST)
    def _(s):
        for d in range(2):
            snd2[d, s] = sown[list_entry(1, d, s)]

        @pl.when(s > 2)
        def _():
            for d in range(2):
                hop2(d, s - 1).start()

    sh2.start()
    for d in range(2):
        hop2(d, FIRST - 1).start()
    zs2.wait_recv()
    zf2.start()
    sh2.wait_recv()
    zf2.wait_recv()

    @pl.loop(FIRST, q2)
    def _(s):
        for d in range(2):
            snd2[d, s] = colp2[sent(1, d, s)]

        @pl.when(s > FIRST)
        def _():
            for d in range(2):
                hop2(d, s - 1).start()

    for d in range(2):
        hop2(d, q2 - 1).start()

    @pl.loop(0, q2)
    def _(s):
        for d in range(2):
            hop2(d, s).wait_recv()
            fwd2(d, s).start()

    @pl.loop(0, q2)
    def _(s):
        for d in range(2):
            fwd2(d, s).wait_recv()

    def write(row):
        rows = pl.ds(row * KB, KB)
        return pltpu.make_async_copy(outv.at[rows], out_hbm.at[rows], osem.at[row])

    @pl.loop(0, OWN // 2)
    def _(t):
        row = t // 3
        for u in range(2):
            entry = 2 * t + u
            cubed = product(colp2, rcv2, 1, row, entry)
            in_use = tab[NEAR_ROW + 8 * (entry - row * KB) + 1, 1 + RA * core + row] >= 0
            own = xv[entry].astype(jnp.float32)
            step = 1.5 * own - cubed * (0.5 / (KB * B))
            outv[entry] = jnp.where(in_use, step, 0.0).astype(jnp.bfloat16)

        @pl.when((t > 0) & (t - 3 * row == 0))
        def _():
            write(row - 1).start()

    zs1.wait_send()
    zf1.wait_send()
    sh1.wait_send()
    zs2.wait_send()
    zf2.wait_send()
    sh2.wait_send()

    @pl.loop(0, q1)
    def _(s):
        for d in range(2):
            hop1(d, s).wait_send()
            fwd1(d, s).wait_send()

    @pl.loop(0, q2)
    def _(s):
        for d in range(2):
            hop2(d, s).wait_send()
            fwd2(d, s).wait_send()

    write(RA - 1).start()
    for row in range(RA):
        write(row).wait()


def sparse(level, grid_a, grid_c, x_blocks, table):
    q1, q2 = LEVELS[level]
    blocks = x_blocks.reshape(OWN, B, B)
    vm = lambda *lead: pltpu.VMEM((*lead, B, B), jnp.bfloat16)
    dma = lambda *lead: pltpu.SemaphoreType.DMA(lead)
    out = pl.pallas_call(
        functools.partial(kernel, q1, q2, grid_a, grid_c, lax.axis_size("grp"), lax.axis_size("col")),
        out_shape=jax.ShapeDtypeStruct(blocks.shape, jnp.bfloat16),
        in_specs=[
            pl.BlockSpec(memory_space=pltpu.SMEM),
            pl.BlockSpec(memory_space=pl.ANY),
        ],
        out_specs=pl.BlockSpec(memory_space=pl.ANY),
        scratch_shapes=[
            pltpu.SMEM((2 * PICKS,), jnp.int32),
            vm(OWN), vm(COLN + 1), vm(4, q1), vm(2, q1), vm(COLN + 1), vm(4, q2), vm(2, q2),
            vm(OWN), vm(OWN),
            dma(2), dma(RA), dma(2, 6),
            dma(2, q1), dma(2, q1), dma(2, q1), dma(2, q1),
            dma(2, q2), dma(2, q2), dma(2, q2), dma(2, q2),
        ],
        compiler_params=pltpu.CompilerParams(
            collective_id=level, has_side_effects=True, vmem_limit_bytes=62 * 1024 * 1024
        ),
        name=f"sign_step_{q1}_{q2}",
    )(table, blocks)
    return out.reshape(x_blocks.shape)


def local(x_blocks, columns, filter_ids):
    grid_a, grid_c, _ = columns.shape
    table, most = list_tables(columns, filter_ids)
    most1 = jnp.maximum(most[0], most[2])
    most2 = jnp.maximum(most[1], most[3])
    level = jnp.int32(len(LEVELS))
    for at in reversed(range(len(LEVELS))):
        fits = (most1 <= LEVELS[at][0]) & (most2 <= LEVELS[at][1])
        level = jnp.where(fits, at, level)
    branches = [
        functools.partial(lambda at, x, c, f, t: sparse(at, grid_a, grid_c, x, t), at)
        for at in range(len(LEVELS))
    ]
    branches.append(lambda x, c, f, t: dense(x, c, f))
    return lax.switch(level, branches, x_blocks, columns, filter_ids, table)


def solution(mesh):
    return jax.shard_map(
        local,
        mesh=mesh,
        in_specs=(P("grp", "col", None, None, None), P(), P()),
        out_specs=P("grp", "col", None, None, None),
        check_vma=False,
    )
```

```python
import functools

import jax
import jax.numpy as jnp
from jax import lax
from jax.experimental import pallas as pl
from jax.experimental.pallas import tpu as pltpu
from jax.sharding import PartitionSpec as P

B = 256
KB = 6
KF = 6
RA = 4
OWN = RA * KB
CR = 2 * RA + 2
COLN = CR * KB
ZERO = COLN
FIRST = 5
LEVELS = ((13, 15), (13, 16), (13, 17), (14, 17), (14, 19), (16, 20))

PICKS = OWN * KB
MESH = pl.DeviceIdType.MESH


def padded(cells, sides, width):
    for axis, dim in sides:
        count = lax.axis_size(axis)
        head = lax.slice_in_dim(cells, 0, width, axis=dim)
        tail = lax.slice_in_dim(cells, cells.shape[dim] - width, cells.shape[dim], axis=dim)
        cells = jnp.concatenate(
            [
                lax.ppermute(tail, axis, [(i, (i + 1) % count) for i in range(count)]),
                cells,
                lax.ppermute(head, axis, [((i + 1) % count, i) for i in range(count)]),
            ],
            axis=dim,
        )
    return cells


def block_terms(
    halo, pos_a, pos_c, row_ids, row_cols, left_blocks, stored_table, wanted, grid_a, grid_c
):
    slot_count = halo.shape[2]
    width = halo.shape[3]
    in_use = row_cols >= 0
    source = jnp.where(in_use, row_cols, 0)
    home_a = row_ids // grid_c
    home_c = row_ids % grid_c
    step_a = (source // grid_c - home_a[:, None] + 1) % grid_a - 1
    step_c = (source % grid_c - home_c[:, None] + 1) % grid_c - 1
    place = (pos_a[:, None] + step_a) * halo.shape[1] + pos_c[:, None] + step_c
    flat = halo.reshape((halo.shape[0] * halo.shape[1] * slot_count, width, width))
    stored = stored_table[source]
    matches = stored[:, :, None, :] == wanted[:, None, :, None]
    present = jnp.any(matches, axis=3) & (wanted[:, None, :] >= 0) & in_use[:, :, None]
    slot_of = jnp.argmax(matches.astype(jnp.int32), axis=3)
    block_index = place[:, :, None] * slot_count + slot_of

    def one_row(inputs):
        index_row, present_row, left_row = inputs
        picked = flat[index_row]
        picked = jnp.where(present_row[:, :, None, None], picked, jnp.zeros((), picked.dtype))
        return jnp.einsum("kab,kfbc->fac", left_row, picked, preferred_element_type=jnp.float32)

    return lax.map(one_row, (block_index, present, left_blocks))


def dense(x_blocks, columns, filter_ids):
    grp_count = lax.axis_size("grp")
    col_count = lax.axis_size("col")
    rows_a = x_blocks.shape[0]
    rows_c = x_blocks.shape[1]
    grid_a = rows_a * grp_count
    grid_c = rows_c * col_count
    col_table = columns.reshape(grid_a * grid_c, KB)
    filt_table = filter_ids.reshape(grid_a * grid_c, KF)
    local_rows = rows_a * rows_c
    offsets = jnp.arange(local_rows, dtype=jnp.int32)
    local_a = offsets // rows_c
    local_c = offsets % rows_c
    row_ids = (
        (lax.axis_index("grp") * rows_a + local_a) * grid_c
        + lax.axis_index("col") * rows_c
        + local_c
    )
    row_cols = col_table[row_ids]
    left_blocks = x_blocks.reshape(local_rows, KB, B, B)
    along_col = padded(x_blocks, (("col", 1),), 1)
    near_x = padded(along_col, (("grp", 0),), 1)
    square = block_terms(
        near_x,
        local_a + 1,
        local_c + 1,
        row_ids,
        row_cols,
        left_blocks,
        col_table,
        filt_table[row_ids],
        grid_a,
        grid_c,
    ).astype(jnp.bfloat16)
    square = square.reshape(rows_a, rows_c, KF, B, B)
    square_along = padded(square, (("col", 1),), 1)
    near_square = padded(square_along, (("grp", 0),), 1)
    cubed = block_terms(
        near_square,
        local_a + 1,
        local_c + 1,
        row_ids,
        row_cols,
        left_blocks,
        filt_table,
        row_cols,
        grid_a,
        grid_c,
    )
    in_use = (row_cols >= 0).astype(jnp.float32)
    result = (1.5 * left_blocks.astype(jnp.float32) - cubed * (0.5 / (KB * B))) * in_use[
        :, :, None, None
    ]
    return result.astype(jnp.bfloat16).reshape(x_blocks.shape)


LANES = 128
LISTS = 8
CODE_AT = 0
NEAR_AT = 48
SRC_AT = 96
TABLE_ROWS = 16


def index_kernel(cols_ref, filt_ref, table_ref, level_ref, own_ref, halo_ref, cols_s, filt_s):
    grp = lax.axis_index("grp")
    col = lax.axis_index("col")
    core = lax.rem(grp, 2)
    grid_c = cols_ref.shape[1]
    grid_a = cols_ref.shape[2]
    chip = 2 * RA

    def lanes_of(x):
        return jnp.concatenate([x] * (LANES // grid_a), axis=1)

    stored, kept = [], []
    for m in range(KB):
        stored.append(lanes_of(cols_ref[m]))
        kept.append(lanes_of(filt_ref[m]))
        cols_s[m] = stored[m]
        filt_s[m] = kept[m]
    shape = (grid_c, LANES)
    lane = lax.broadcasted_iota(jnp.int32, shape, 1)
    ids = lax.rem(lane, grid_a) * grid_c + lax.broadcasted_iota(jnp.int32, shape, 0)
    in_chip = lax.rem(lane, chip)
    first, last = in_chip == 0, in_chip == chip - 1
    false = jnp.zeros(shape, jnp.int32)

    def either(tests):
        got = tests[0]
        for t in tests[1:]:
            got = got | t
        return got

    totals = []
    for d, step_c in enumerate((1, -1)):
        cols_c = [jnp.roll(x, -step_c, 0) for x in stored]
        filt_c = [jnp.roll(x, -step_c, 0) for x in kept]
        found = []
        for step_a in (-1, 0, 1):
            shift = (-step_a) % LANES
            cols_r = [pltpu.roll(x, shift, 1) if shift else x for x in cols_c]
            filt_r = [pltpu.roll(x, shift, 1) if shift else x for x in filt_c]
            member = either([x == ids for x in cols_r])
            one = [either([stored[m] == x for x in filt_r]) & member & (stored[m] >= 0) for m in range(KB)]
            two = [either([kept[m] == x for x in cols_r]) & member for m in range(KB)]
            found.append((one, two))
        up, mid, down = found
        for phase in (0, 1):
            own_row, halo_row = false, false
            for m in range(KB):
                u, c, w = up[phase][m], mid[phase][m], down[phase][m]
                own = (c | (u & ~first) | (w & ~last)).astype(jnp.int32)
                halo = ((u & first) | (w & last)).astype(jnp.int32)
                own_ref[phase, d, m] = own
                halo_ref[phase, d, m] = halo
                own_row = own_row + own
                halo_row = halo_row + halo
            totals.append((phase, own_row, halo_row))

    def summed(x, rule):
        at = lax.broadcasted_iota(jnp.int32, (LANES, LANES), 0)
        to = lax.broadcasted_iota(jnp.int32, (LANES, LANES), 1)
        weight = rule(at, to).astype(jnp.float32).astype(jnp.bfloat16)
        return jnp.dot(
            x.astype(jnp.float32).astype(jnp.bfloat16), weight, preferred_element_type=jnp.float32
        ).astype(jnp.int32)

    def split(n0, n1, total):
        half = (total + 1) // 2
        return half, jnp.maximum(FIRST - n0, 0), jnp.maximum(FIRST - n1, 0)

    own_all = jnp.concatenate([t[1] for t in totals], axis=0)
    halo_all = jnp.concatenate([t[2] for t in totals], axis=0)

    def same_chip(at, to):
        return (at // chip == lax.rem(to, grid_a) // chip) & (at < grid_a)

    def beside(at, to):
        z = lax.rem(to, grid_a) // chip * chip
        above = lax.rem(z + grid_a - 1, grid_a)
        below = lax.rem(z + chip, grid_a)
        return (at == above) | (at == below)

    n0 = summed(own_all, lambda at, to: same_chip(at, to) & (lax.rem(at, chip) < RA))
    n1 = summed(own_all, lambda at, to: same_chip(at, to) & (lax.rem(at, chip) >= RA))
    total = n0 + n1 + summed(halo_all, beside)
    half, gap0, gap1 = split(n0, n1, total)
    rest = total - half
    fill = jnp.maximum(
        half + jnp.where(half > n0, gap0, 0), rest + jnp.where(rest > n1, gap1, 0)
    )
    most = [jnp.int32(0), jnp.int32(0)]
    for p, (phase, _, _) in enumerate(totals):
        most[phase] = jnp.maximum(most[phase], jnp.max(fill[p * grid_c : (p + 1) * grid_c]))
    level = jnp.int32(len(LEVELS))
    for at in reversed(range(len(LEVELS))):
        fits = (most[0] <= LEVELS[at][0]) & (most[1] <= LEVELS[at][1])
        level = jnp.where(fits, at, level)
    level_ref[0] = level

    z = grp // 2
    shift = lax.rem(LANES + 1 - z * chip, LANES)
    west = lax.rem(col + grid_c - 1, grid_c)
    east = lax.rem(col + 1, grid_c)
    row8 = (LISTS, LANES)
    lane8 = lax.broadcasted_iota(jnp.int32, row8, 1)
    rim = (lane8 == 0) | (lane8 == CR - 1)
    lists = [(p, d, c) for p in (0, 1) for d, c in ((0, col), (1, col), (0, west), (1, east))]

    def near(ref_rows):
        return pltpu.roll(jnp.concatenate(ref_rows, axis=0), shift, 1)

    need, in_row, stores = [], [], []
    run = jnp.zeros(row8, jnp.int32)
    for m in range(KB):
        own = near([own_ref[p, d, m, pl.ds(c, 1), :] for p, d, c in lists])
        halo = near([halo_ref[p, d, m, pl.ds(c, 1), :] for p, d, c in lists])
        flags = jnp.where(lane8 < CR, jnp.where(rim, halo, own), 0)
        need.append(flags)
        in_row.append(run)
        run = run + flags
        rows = [cols_s[m, pl.ds(c, 1), :] for c in (west, col, east)]
        rows += [filt_s[m, pl.ds(c, 1), :] for c in (west, col, east)]
        stores.append(near(rows + rows[:2]))
    n0 = summed(run, lambda at, to: (at >= 1) & (at <= RA))
    n1 = summed(run, lambda at, to: (at > RA) & (at <= chip))
    above = summed(run, lambda at, to: at == 0)
    below = summed(run, lambda at, to: at == CR - 1)
    ahead = summed(
        run, lambda at, to: (at < to) & (((at >= 1) & (to <= RA)) | ((at > RA) & (to <= chip)))
    )
    total = n0 + n1 + above + below
    half, gap0, gap1 = split(n0, n1, total)
    of0 = (lane8 >= 1) & (lane8 <= RA)
    of1 = (lane8 > RA) & (lane8 <= chip)
    slots = lax.broadcasted_iota(jnp.int32, (32, LANES), 0) + core * 32
    entry = lax.broadcasted_iota(jnp.int32, (32, LANES), 1) * KB
    source = [jnp.zeros((32, LANES), jnp.int32) for _ in range(4)]
    codes = []
    for m in range(KB):
        place = ahead + in_row[m]
        place = jnp.where(lane8 == 0, n0 + in_row[m], place)
        place = jnp.where(lane8 == CR - 1, n0 + above + in_row[m], place)
        place = jnp.where(of1, total - 1 - place, place)
        turned = total - 1 - place
        slot0 = place + jnp.where(of0, 0, gap0)
        slot1 = turned + jnp.where(of1, 0, gap1)
        code = jnp.where(place < half, slot0, 32 + slot1)
        codes.append(code)
        sent = jnp.where(need[m] > 0, code, -1)
        for i, at in enumerate((0, 1, 4, 5)):
            same = jnp.broadcast_to(sent[at : at + 1], (32, LANES)) == slots
            source[i] = source[i] + jnp.where(same, entry + m, 0)
    lane32 = lax.broadcasted_iota(jnp.int32, (32, LANES), 1)
    out = jnp.zeros((32, LANES), jnp.int32)
    for i in range(4):
        out = jnp.where(lane32 == i, jnp.sum(source[i], axis=1, keepdims=True), out)
    table_ref[...] = jnp.concatenate(codes + stores + [out], axis=0).T[:TABLE_ROWS]


def list_tables(columns, filter_ids):
    grid_a, grid_c, _ = columns.shape
    ints = lambda *shape: pltpu.VMEM(shape, jnp.int32)
    return pl.pallas_call(
        index_kernel,
        out_shape=(
            jax.ShapeDtypeStruct((TABLE_ROWS, LANES), jnp.int32),
            jax.ShapeDtypeStruct((1,), jnp.int32),
        ),
        in_specs=[pl.BlockSpec(memory_space=pltpu.VMEM)] * 2,
        out_specs=(
            pl.BlockSpec(memory_space=pltpu.VMEM),
            pl.BlockSpec(memory_space=pltpu.SMEM),
        ),
        scratch_shapes=[
            ints(2, 2, KB, grid_c, LANES), ints(2, 2, KB, grid_c, LANES),
            ints(KB, grid_c, LANES), ints(KF, grid_c, LANES),
        ],
        name="block_lists",
    )(columns.transpose(2, 1, 0), filter_ids.transpose(2, 1, 0))


def kernel(q1, q2, grid_a, grid_c, grp_count, col_count, tab, x_hbm, out_hbm, pick, xv, colp1, rcv1, snd1, colp2, rcv2,
           snd2, sown, outv, lsem, osem, zsem, hs1, hr1, fs1, fr1, hs2, hr2, fs2, fr2):
    grp = lax.axis_index("grp")
    col = lax.axis_index("col")
    core = lax.rem(grp, 2)
    partner = (grp + 1 - 2 * core, col)
    zpeer = (lax.rem(grp + grp_count - 1 + 2 * core, grp_count), col)
    right = (grp, lax.rem(col + 1, col_count))
    left = (grp, lax.rem(col + col_count - 1, col_count))
    own0 = (1 + RA * core) * KB
    zout = (RA - 1) * core * KB
    zdst = (CR - 1) * (1 - core) * KB
    zin = (CR - 1) * core * KB

    to_xv = pltpu.make_async_copy(x_hbm, xv, lsem.at[0])
    to_col = pltpu.make_async_copy(x_hbm, colp1.at[pl.ds(own0, OWN)], lsem.at[1])
    to_xv.start()

    barrier = pltpu.get_barrier_semaphore()
    for peer in (partner, zpeer, right, left):
        pl.semaphore_signal(barrier, inc=1, device_id=peer, device_id_type=MESH)
    pl.semaphore_wait(barrier, 4)

    def remote(src, dst, send, recv, device):
        return pltpu.make_async_remote_copy(
            src_ref=src, dst_ref=dst, send_sem=send, recv_sem=recv,
            device_id=device, device_id_type=MESH,
        )

    def zsend(src, colp, p):
        return remote(src.at[pl.ds(zout, KB)], colp.at[pl.ds(zdst, KB)],
                      zsem.at[p, 0], zsem.at[p, 1], zpeer)

    def zfwd(colp, p):
        here = colp.at[pl.ds(zin, KB)]
        return remote(here, here, zsem.at[p, 2], zsem.at[p, 3], partner)

    def share(src, colp, p):
        return remote(src, colp.at[pl.ds(own0, OWN)], zsem.at[p, 4], zsem.at[p, 5], partner)

    def hop(snd, rcv, hs, hr, d, s):
        return remote(snd.at[d, s], rcv.at[2 * d + core, s], hs.at[d, s], hr.at[d, s],
                      (right, left)[d])

    def fwd(rcv, fs, fr, d, s):
        here = rcv.at[2 * d + core, s]
        return remote(here, here, fs.at[d, s], fr.at[d, s], partner)

    def right_factor(colp, rcv, v):
        is_col = v < 64
        at_col = jnp.where(is_col, v, ZERO)
        at_rcv = jnp.where(is_col, 0, v - 64)
        slot = jnp.minimum(at_rcv & 31, rcv.shape[1] - 1)
        return jnp.where(is_col, colp[at_col], rcv[(at_rcv >> 5) & 3, slot])

    def product(colp, rcv, phase, row, entry):
        acc = None
        for k in range(KB):
            v = pick[phase * PICKS + entry * KB + k]
            term = jnp.dot(xv[row * KB + k], right_factor(colp, rcv, v),
                           preferred_element_type=jnp.float32)
            acc = term if acc is None else acc + term
        return acc

    def sent(phase, d, s):
        return tab[2 * phase + d, SRC_AT + s]

    def list_entry(phase, d, s):
        return jnp.clip(sent(phase, d, s) - own0, 0, OWN - 1)

    def find_factors(at):
        row = at // KB
        k = at - KB * row
        here = 1 + RA * core + row
        source = tab[here, NEAR_AT + 8 * k + 1]
        in_use = source >= 0
        source = jnp.where(in_use, source, 0)
        step_a = lax.rem(source // grid_c - (grp * RA + row) + 1 + grid_a, grid_a) - 1
        side = lax.rem(lax.rem(source, grid_c) - col + 1 + grid_c, grid_c)
        step_a = jnp.where(in_use, jnp.clip(step_a, -1, 1), 0)
        side = jnp.where(in_use, jnp.minimum(side, 2), 1)
        there = here + step_a
        for phase in range(2):
            held, spot = [], []
            for m in range(KB):
                held.append(tab[there, NEAR_AT + 8 * m + side + 3 * phase])
                code = tab[there, CODE_AT + 8 * m + 4 * phase + jnp.where(side == 0, 2, 3)]
                far = code + jnp.where(side == 0, 64, 128)
                spot.append(jnp.where(side == 1, there * KB + m, far))
            for f in range(KF):
                wanted = tab[here, NEAR_AT + 8 * f + 1 + 3 * (1 - phase)]
                usable = in_use & (wanted >= 0)
                got = jnp.int32(ZERO)
                for m in range(KB):
                    got = jnp.where(held[m] == wanted, spot[m], got)
                pick[phase * PICKS + (row * KB + f) * KB + k] = jnp.where(usable, got, ZERO)

    zero = jnp.zeros((B, B), jnp.bfloat16)

    zs1, zf1, sh1 = zsend(xv, colp1, 0), zfwd(colp1, 0), share(xv, colp1, 0)
    to_xv.wait()
    zs1.start()
    to_col.start()
    sh1.start()
    hop1 = functools.partial(hop, snd1, rcv1, hs1, hr1)
    fwd1 = functools.partial(fwd, rcv1, fs1, fr1)

    @pl.loop(0, FIRST)
    def _(s):
        for d in range(2):
            snd1[d, s] = xv[list_entry(0, d, s)]

        @pl.when(s > 0)
        def _():
            for d in range(2):
                hop1(d, s - 1).start()

    colp1[ZERO] = zero
    colp2[ZERO] = zero
    for d in range(2):
        hop1(d, FIRST - 1).start()
    to_col.wait()
    zs1.wait_recv()
    zf1.start()
    sh1.wait_recv()
    zf1.wait_recv()

    @pl.loop(FIRST, q1)
    def _(s):
        for d in range(2):
            snd1[d, s] = colp1[sent(0, d, s)]

        @pl.when(s > FIRST)
        def _():
            for d in range(2):
                hop1(d, s - 1).start()

    for d in range(2):
        hop1(d, q1 - 1).start()

    pl.loop(0, OWN)(find_factors)

    @pl.loop(0, q1)
    def _(s):
        for d in range(2):
            hop1(d, s).wait_recv()
            fwd1(d, s).start()

    @pl.loop(0, q1)
    def _(s):
        for d in range(2):
            fwd1(d, s).wait_recv()

    zs2, zf2, sh2 = zsend(sown, colp2, 1), zfwd(colp2, 1), share(sown, colp2, 1)
    hop2 = functools.partial(hop, snd2, rcv2, hs2, hr2)
    fwd2 = functools.partial(fwd, rcv2, fs2, fr2)

    @pl.loop(0, 2)
    def _(s):
        for d in range(2):
            entry = list_entry(1, d, s)
            snd2[d, s] = product(colp1, rcv1, 0, entry // KB, entry).astype(jnp.bfloat16)

        @pl.when(s > 0)
        def _():
            for d in range(2):
                hop2(d, s - 1).start()

    @pl.loop(0, OWN // 2)
    def _(t):
        step = t // 3
        row = step + core * (RA - 1 - 2 * step)
        for u in range(2):
            entry = row * KB + (t - 3 * step) * 2 + u
            block = product(colp1, rcv1, 0, row, entry).astype(jnp.bfloat16)
            sown[entry] = block
            colp2[own0 + entry] = block

        @pl.when(t == 0)
        def _():
            for d in range(2):
                hop2(d, 1).start()

        @pl.when(t == 3)
        def _():
            zs2.start()

    @pl.loop(2, FIRST)
    def _(s):
        for d in range(2):
            snd2[d, s] = sown[list_entry(1, d, s)]

        @pl.when(s > 2)
        def _():
            for d in range(2):
                hop2(d, s - 1).start()

    sh2.start()
    for d in range(2):
        hop2(d, FIRST - 1).start()
    zs2.wait_recv()
    zf2.start()
    sh2.wait_recv()
    zf2.wait_recv()

    @pl.loop(FIRST, q2)
    def _(s):
        for d in range(2):
            snd2[d, s] = colp2[sent(1, d, s)]

        @pl.when(s > FIRST)
        def _():
            for d in range(2):
                hop2(d, s - 1).start()

    for d in range(2):
        hop2(d, q2 - 1).start()

    @pl.loop(0, q2)
    def _(s):
        for d in range(2):
            hop2(d, s).wait_recv()
            fwd2(d, s).start()

    @pl.loop(0, q2)
    def _(s):
        for d in range(2):
            fwd2(d, s).wait_recv()

    def write(row):
        rows = pl.ds(row * KB, KB)
        return pltpu.make_async_copy(outv.at[rows], out_hbm.at[rows], osem.at[row])

    @pl.loop(0, OWN // 2)
    def _(t):
        row = t // 3
        for u in range(2):
            entry = 2 * t + u
            cubed = product(colp2, rcv2, 1, row, entry)
            in_use = tab[1 + RA * core + row, NEAR_AT + 8 * (entry - row * KB) + 1] >= 0
            own = xv[entry].astype(jnp.float32)
            step = 1.5 * own - cubed * (0.5 / (KB * B))
            outv[entry] = jnp.where(in_use, step, 0.0).astype(jnp.bfloat16)

        @pl.when((t > 0) & (t - 3 * row == 0))
        def _():
            write(row - 1).start()

    zs1.wait_send()
    zf1.wait_send()
    sh1.wait_send()
    zs2.wait_send()
    zf2.wait_send()
    sh2.wait_send()

    @pl.loop(0, q1)
    def _(s):
        for d in range(2):
            hop1(d, s).wait_send()
            fwd1(d, s).wait_send()

    @pl.loop(0, q2)
    def _(s):
        for d in range(2):
            hop2(d, s).wait_send()
            fwd2(d, s).wait_send()

    write(RA - 1).start()
    for row in range(RA):
        write(row).wait()


def sparse(level, grid_a, grid_c, x_blocks, table):
    q1, q2 = LEVELS[level]
    blocks = x_blocks.reshape(OWN, B, B)
    vm = lambda *lead: pltpu.VMEM((*lead, B, B), jnp.bfloat16)
    dma = lambda *lead: pltpu.SemaphoreType.DMA(lead)
    out = pl.pallas_call(
        functools.partial(kernel, q1, q2, grid_a, grid_c, lax.axis_size("grp"), lax.axis_size("col")),
        out_shape=jax.ShapeDtypeStruct(blocks.shape, jnp.bfloat16),
        in_specs=[
            pl.BlockSpec(memory_space=pltpu.SMEM),
            pl.BlockSpec(memory_space=pl.ANY),
        ],
        out_specs=pl.BlockSpec(memory_space=pl.ANY),
        scratch_shapes=[
            pltpu.SMEM((2 * PICKS,), jnp.int32),
            vm(OWN), vm(COLN + 1), vm(4, q1), vm(2, q1), vm(COLN + 1), vm(4, q2), vm(2, q2),
            vm(OWN), vm(OWN),
            dma(2), dma(RA), dma(2, 6),
            dma(2, q1), dma(2, q1), dma(2, q1), dma(2, q1),
            dma(2, q2), dma(2, q2), dma(2, q2), dma(2, q2),
        ],
        compiler_params=pltpu.CompilerParams(
            collective_id=level, has_side_effects=True, vmem_limit_bytes=62 * 1024 * 1024
        ),
        name=f"sign_step_{q1}_{q2}",
    )(table, blocks)
    return out.reshape(x_blocks.shape)


def local(x_blocks, columns, filter_ids):
    grid_a, grid_c, _ = columns.shape
    table, level = list_tables(columns, filter_ids)
    branches = [
        functools.partial(lambda at, x, c, f, t: sparse(at, grid_a, grid_c, x, t), at)
        for at in range(len(LEVELS))
    ]
    branches.append(lambda x, c, f, t: dense(x, c, f))
    return lax.switch(level[0], branches, x_blocks, columns, filter_ids, table)


def solution(mesh):
    return jax.shard_map(
        local,
        mesh=mesh,
        in_specs=(P("grp", "col", None, None, None), P(), P()),
        out_specs=P("grp", "col", None, None, None),
        check_vma=False,
    )
```

```python
import functools

import jax
import jax.numpy as jnp
from jax import lax
from jax.experimental import pallas as pl
from jax.experimental.pallas import tpu as pltpu
from jax.sharding import PartitionSpec as P

B = 256
KB = 6
KF = 6
RA = 4
OWN = RA * KB
CR = 2 * RA + 2
COLN = CR * KB
ZERO = COLN
FIRST = 5
RELAY = 3
LEVELS = ((11, 13), (11, 14), (12, 14), (12, 15), (13, 17), (16, 20))

PICKS = OWN * KB
MESH = pl.DeviceIdType.MESH


def padded(cells, sides, width):
    for axis, dim in sides:
        count = lax.axis_size(axis)
        head = lax.slice_in_dim(cells, 0, width, axis=dim)
        tail = lax.slice_in_dim(cells, cells.shape[dim] - width, cells.shape[dim], axis=dim)
        cells = jnp.concatenate(
            [
                lax.ppermute(tail, axis, [(i, (i + 1) % count) for i in range(count)]),
                cells,
                lax.ppermute(head, axis, [((i + 1) % count, i) for i in range(count)]),
            ],
            axis=dim,
        )
    return cells


def block_terms(
    halo, pos_a, pos_c, row_ids, row_cols, left_blocks, stored_table, wanted, grid_a, grid_c
):
    slot_count = halo.shape[2]
    width = halo.shape[3]
    in_use = row_cols >= 0
    source = jnp.where(in_use, row_cols, 0)
    home_a = row_ids // grid_c
    home_c = row_ids % grid_c
    step_a = (source // grid_c - home_a[:, None] + 1) % grid_a - 1
    step_c = (source % grid_c - home_c[:, None] + 1) % grid_c - 1
    place = (pos_a[:, None] + step_a) * halo.shape[1] + pos_c[:, None] + step_c
    flat = halo.reshape((halo.shape[0] * halo.shape[1] * slot_count, width, width))
    stored = stored_table[source]
    matches = stored[:, :, None, :] == wanted[:, None, :, None]
    present = jnp.any(matches, axis=3) & (wanted[:, None, :] >= 0) & in_use[:, :, None]
    slot_of = jnp.argmax(matches.astype(jnp.int32), axis=3)
    block_index = place[:, :, None] * slot_count + slot_of

    def one_row(inputs):
        index_row, present_row, left_row = inputs
        picked = flat[index_row]
        picked = jnp.where(present_row[:, :, None, None], picked, jnp.zeros((), picked.dtype))
        return jnp.einsum("kab,kfbc->fac", left_row, picked, preferred_element_type=jnp.float32)

    return lax.map(one_row, (block_index, present, left_blocks))


def dense(x_blocks, columns, filter_ids):
    grp_count = lax.axis_size("grp")
    col_count = lax.axis_size("col")
    rows_a = x_blocks.shape[0]
    rows_c = x_blocks.shape[1]
    grid_a = rows_a * grp_count
    grid_c = rows_c * col_count
    col_table = columns.reshape(grid_a * grid_c, KB)
    filt_table = filter_ids.reshape(grid_a * grid_c, KF)
    local_rows = rows_a * rows_c
    offsets = jnp.arange(local_rows, dtype=jnp.int32)
    local_a = offsets // rows_c
    local_c = offsets % rows_c
    row_ids = (
        (lax.axis_index("grp") * rows_a + local_a) * grid_c
        + lax.axis_index("col") * rows_c
        + local_c
    )
    row_cols = col_table[row_ids]
    left_blocks = x_blocks.reshape(local_rows, KB, B, B)
    along_col = padded(x_blocks, (("col", 1),), 1)
    near_x = padded(along_col, (("grp", 0),), 1)
    square = block_terms(
        near_x,
        local_a + 1,
        local_c + 1,
        row_ids,
        row_cols,
        left_blocks,
        col_table,
        filt_table[row_ids],
        grid_a,
        grid_c,
    ).astype(jnp.bfloat16)
    square = square.reshape(rows_a, rows_c, KF, B, B)
    square_along = padded(square, (("col", 1),), 1)
    near_square = padded(square_along, (("grp", 0),), 1)
    cubed = block_terms(
        near_square,
        local_a + 1,
        local_c + 1,
        row_ids,
        row_cols,
        left_blocks,
        filt_table,
        row_cols,
        grid_a,
        grid_c,
    )
    in_use = (row_cols >= 0).astype(jnp.float32)
    result = (1.5 * left_blocks.astype(jnp.float32) - cubed * (0.5 / (KB * B))) * in_use[
        :, :, None, None
    ]
    return result.astype(jnp.bfloat16).reshape(x_blocks.shape)


LANES = 128
LISTS = 8
CODE_AT = 0
NEAR_AT = 48
SRC_AT = 96
TABLE_ROWS = 16


def index_kernel(cols_ref, filt_ref, table_ref, level_ref, own_ref, halo_ref, move_ref,
                 cols_s, filt_s):
    grp = lax.axis_index("grp")
    col = lax.axis_index("col")
    core = lax.rem(grp, 2)
    grid_c = cols_ref.shape[1]
    grid_a = cols_ref.shape[2]
    chip = 2 * RA

    def lanes_of(x):
        return jnp.concatenate([x] * (LANES // grid_a), axis=1)

    stored, kept = [], []
    for m in range(KB):
        stored.append(lanes_of(cols_ref[m]))
        kept.append(lanes_of(filt_ref[m]))
        cols_s[m] = stored[m]
        filt_s[m] = kept[m]
    shape = (grid_c, LANES)
    lane = lax.broadcasted_iota(jnp.int32, shape, 1)
    ids = lax.rem(lane, grid_a) * grid_c + lax.broadcasted_iota(jnp.int32, shape, 0)
    in_chip = lax.rem(lane, chip)
    first, last = in_chip == 0, in_chip == chip - 1
    false = jnp.zeros(shape, jnp.int32)

    def either(tests):
        got = tests[0]
        for t in tests[1:]:
            got = got | t
        return got

    totals = []
    for d, step_c in enumerate((1, -1)):
        cols_c = [jnp.roll(x, -step_c, 0) for x in stored]
        filt_c = [jnp.roll(x, -step_c, 0) for x in kept]
        found = []
        for step_a in (-1, 0, 1):
            shift = (-step_a) % LANES
            cols_r = [pltpu.roll(x, shift, 1) if shift else x for x in cols_c]
            filt_r = [pltpu.roll(x, shift, 1) if shift else x for x in filt_c]
            member = either([x == ids for x in cols_r])
            one = [either([stored[m] == x for x in filt_r]) & member & (stored[m] >= 0) for m in range(KB)]
            two = [either([kept[m] == x for x in cols_r]) & member for m in range(KB)]
            found.append((one, two))
        up, mid, down = found
        for phase in (0, 1):
            own_row, halo_row = false, false
            flags = []
            for m in range(KB):
                u, c, w = up[phase][m], mid[phase][m], down[phase][m]
                own = (c | (u & ~first) | (w & ~last)).astype(jnp.int32)
                halo = ((u & first) | (w & last)).astype(jnp.int32)
                flags.append((own, halo))
                own_row = own_row + own
                halo_row = halo_row + halo
            totals.append((phase, d, flags, own_row, halo_row))

    def summed(x, rule):
        at = lax.broadcasted_iota(jnp.int32, (LANES, LANES), 0)
        to = lax.broadcasted_iota(jnp.int32, (LANES, LANES), 1)
        weight = rule(at, to).astype(jnp.float32).astype(jnp.bfloat16)
        return jnp.dot(
            x.astype(jnp.float32).astype(jnp.bfloat16), weight, preferred_element_type=jnp.float32
        ).astype(jnp.int32)

    def same_chip(at, to):
        return (at // chip == lax.rem(to, grid_a) // chip) & (at < grid_a)

    def beside(at, to):
        z = lax.rem(to, grid_a) // chip * chip
        above = lax.rem(z + grid_a - 1, grid_a)
        below = lax.rem(z + chip, grid_a)
        return (at == above) | (at == below)

    def stack(xs):
        return jnp.concatenate(xs, axis=0)

    loads = summed(stack([t[3] for t in totals]), same_chip) + summed(
        stack([t[4] for t in totals]), beside
    )

    def across(x):
        return jnp.where(last, pltpu.roll(x, LANES - 1, 1), pltpu.roll(x, 1, 1))

    kept_own, kept_halo, got0, got1 = [], [], [], []
    for p, (phase, d, flags, _, _) in enumerate(totals):
        load = loads[p * grid_c : (p + 1) * grid_c]
        lead = jnp.where(last, load - across(load), across(load) - load)
        far = jnp.abs(lead)
        count = jnp.zeros(shape, jnp.int32)
        for step in range(RELAY):
            count = count + (far >= 3 * step + 2).astype(jnp.int32)
        ups = (lead > 0).astype(jnp.int32)
        rim = (first | last).astype(jnp.int32)
        both = [own * halo * rim for own, halo in flags]
        lower = [jnp.where(last, own, halo) for own, halo in flags]
        upper = [jnp.where(last, halo, own) for own, halo in flags]
        single = [
            jnp.where(ups > 0, lower[m], upper[m]) * rim - both[m] for m in range(KB)
        ]
        n_both = sum(both[1:], both[0])
        n_single = sum(single[1:], single[0])
        both_rank = jnp.where(last, 0, across(n_both))
        single_rank = n_both + across(n_both) + jnp.where(last, 0, across(n_single))
        own_row, halo_row, moved_row = false, false, false
        for m in range(KB):
            rank = jnp.where(both[m] > 0, both_rank, single_rank)
            moved = ((both[m] + single[m]) > 0) & (rank < count)
            move = jnp.where(moved, rank + 1 + 8 * ups, 0)
            both_rank = both_rank + both[m]
            single_rank = single_rank + single[m]
            own = jnp.where(moved, 0, flags[m][0])
            halo = jnp.where(moved, 0, flags[m][1])
            own_ref[phase, d, m] = own
            halo_ref[phase, d, m] = halo
            move_ref[phase, d, m] = move
            own_row, halo_row = own_row + own, halo_row + halo
            moved_row = moved_row + moved.astype(jnp.int32)
        moved_row = moved_row + across(moved_row)
        kept_own.append(own_row)
        kept_halo.append(halo_row)
        got0.append(jnp.where(first, moved_row * ups, 0))
        got1.append(jnp.where(last, moved_row * (1 - ups), 0))

    def split(n0, n1, total, extra0, extra1):
        half = jnp.clip((total + extra1 - extra0 + 1) >> 1, 0, total)
        return half, jnp.maximum(FIRST - n0, 0), jnp.maximum(FIRST - n1, 0)

    own_all = stack(kept_own)
    n0 = summed(own_all, lambda at, to: same_chip(at, to) & (lax.rem(at, chip) < RA))
    n1 = summed(own_all, lambda at, to: same_chip(at, to) & (lax.rem(at, chip) >= RA))
    total = n0 + n1 + summed(stack(kept_halo), beside)
    extra0 = summed(stack(got0), same_chip)
    extra1 = summed(stack(got1), same_chip)
    half, gap0, gap1 = split(n0, n1, total, extra0, extra1)
    rest = total - half
    fill = jnp.maximum(
        half + jnp.where(half > n0, gap0, 0) + extra0,
        rest + jnp.where(rest > n1, gap1, 0) + extra1,
    )
    most = [jnp.int32(FIRST + RELAY), jnp.int32(FIRST + RELAY)]
    for p, (phase, _, _, _, _) in enumerate(totals):
        most[phase] = jnp.maximum(most[phase], jnp.max(fill[p * grid_c : (p + 1) * grid_c]))
    level = jnp.int32(len(LEVELS))
    for at in reversed(range(len(LEVELS))):
        fits = (most[0] <= LEVELS[at][0]) & (most[1] <= LEVELS[at][1])
        level = jnp.where(fits, at, level)
    level_ref[0] = level

    z = grp // 2
    shift = lax.rem(LANES + 1 - z * chip, LANES)
    west = lax.rem(col + grid_c - 1, grid_c)
    east = lax.rem(col + 1, grid_c)
    row8 = (LISTS, LANES)
    lane8 = lax.broadcasted_iota(jnp.int32, row8, 1)
    rim = (lane8 == 0) | (lane8 == CR - 1)
    lists = [(p, d, c) for p in (0, 1) for d, c in ((0, col), (1, col), (0, west), (1, east))]

    def near(ref_rows):
        return pltpu.roll(jnp.concatenate(ref_rows, axis=0), shift, 1)

    need, in_row, stores, moves = [], [], [], []
    run = jnp.zeros(row8, jnp.int32)
    relayed = jnp.zeros(row8, jnp.int32)
    low_end = lane8 <= 1
    for m in range(KB):
        own = near([own_ref[p, d, m, pl.ds(c, 1), :] for p, d, c in lists])
        halo = near([halo_ref[p, d, m, pl.ds(c, 1), :] for p, d, c in lists])
        flags = jnp.where(lane8 < CR, jnp.where(rim, halo, own), 0)
        need.append(flags)
        in_row.append(run)
        run = run + flags
        move = near([move_ref[p, d, m, pl.ds(c, 1), :] for p, d, c in lists])
        move = jnp.where((lane8 <= 1) | ((lane8 >= CR - 2) & (lane8 < CR)), move, 0)
        mine = (move > 0) & ((move > 8) == low_end)
        moves.append((move, mine))
        relayed = relayed + mine.astype(jnp.int32)
        rows = [cols_s[m, pl.ds(c, 1), :] for c in (west, col, east)]
        rows += [filt_s[m, pl.ds(c, 1), :] for c in (west, col, east)]
        stores.append(near(rows + rows[:2]))
    n0 = summed(run, lambda at, to: (at >= 1) & (at <= RA))
    n1 = summed(run, lambda at, to: (at > RA) & (at <= chip))
    above = summed(run, lambda at, to: at == 0)
    below = summed(run, lambda at, to: at == CR - 1)
    ahead = summed(
        run, lambda at, to: (at < to) & (((at >= 1) & (to <= RA)) | ((at > RA) & (to <= chip)))
    )
    total = n0 + n1 + above + below
    extra0 = summed(relayed, lambda at, to: at <= 1)
    extra1 = summed(relayed, lambda at, to: at > 1)
    half, gap0, gap1 = split(n0, n1, total, extra0, extra1)
    east_list = lax.rem(lax.broadcasted_iota(jnp.int32, row8, 0), 4) == 3
    of0 = (lane8 >= 1) & (lane8 <= RA)
    of1 = (lane8 > RA) & (lane8 <= chip)
    slots = lax.broadcasted_iota(jnp.int32, (32, LANES), 0) + core * 32
    entry = lax.broadcasted_iota(jnp.int32, (32, LANES), 1) * KB
    source = [jnp.zeros((32, LANES), jnp.int32) for _ in range(4)]
    codes = []
    for m in range(KB):
        place = ahead + in_row[m]
        place = jnp.where(lane8 == 0, n0 + in_row[m], place)
        place = jnp.where(lane8 == CR - 1, n0 + above + in_row[m], place)
        place = jnp.where(of1, total - 1 - place, place)
        turned = total - 1 - place
        slot0 = place + jnp.where(of0, 0, gap0)
        slot1 = turned + jnp.where(of1, 0, gap1)
        slot0 = slot0 + jnp.where(slot0 >= FIRST, extra0, 0)
        slot1 = slot1 + jnp.where(slot1 >= FIRST, extra1, 0)
        code = jnp.where(place < half, slot0, 32 + slot1)
        move, mine = moves[m]
        rank = (move & 7) - 1
        code = jnp.where(mine, jnp.where(low_end, FIRST, 32 + FIRST) + rank, code)
        code = jnp.where((move > 0) & ~mine, jnp.where(east_list, 96, 128) + rank, code)
        codes.append(code)
        sent = jnp.where((need[m] > 0) | mine, code, -1)
        for i, at in enumerate((0, 1, 4, 5)):
            same = jnp.broadcast_to(sent[at : at + 1], (32, LANES)) == slots
            source[i] = source[i] + jnp.where(same, entry + m, 0)
    lane32 = lax.broadcasted_iota(jnp.int32, (32, LANES), 1)
    out = jnp.zeros((32, LANES), jnp.int32)
    for i in range(4):
        out = jnp.where(lane32 == i, jnp.sum(source[i], axis=1, keepdims=True), out)
    table_ref[...] = jnp.concatenate(codes + stores + [out], axis=0).T[:TABLE_ROWS]


def list_tables(columns, filter_ids):
    grid_a, grid_c, _ = columns.shape
    ints = lambda *shape: pltpu.VMEM(shape, jnp.int32)
    return pl.pallas_call(
        index_kernel,
        out_shape=(
            jax.ShapeDtypeStruct((TABLE_ROWS, LANES), jnp.int32),
            jax.ShapeDtypeStruct((1,), jnp.int32),
        ),
        in_specs=[pl.BlockSpec(memory_space=pltpu.VMEM)] * 2,
        out_specs=(
            pl.BlockSpec(memory_space=pltpu.VMEM),
            pl.BlockSpec(memory_space=pltpu.SMEM),
        ),
        scratch_shapes=[
            ints(2, 2, KB, grid_c, LANES), ints(2, 2, KB, grid_c, LANES),
            ints(2, 2, KB, grid_c, LANES),
            ints(KB, grid_c, LANES), ints(KF, grid_c, LANES),
        ],
        name="block_lists",
    )(columns.transpose(2, 1, 0), filter_ids.transpose(2, 1, 0))


def kernel(q1, q2, grid_a, grid_c, grp_count, col_count, tab, x_hbm, out_hbm, pick, xv, colp1, rcv1, snd1, colp2, rcv2,
           snd2, sown, outv, lsem, osem, zsem, hs1, hr1, fs1, fr1, hs2, hr2, fs2, fr2, ysem):
    grp = lax.axis_index("grp")
    col = lax.axis_index("col")
    core = lax.rem(grp, 2)
    partner = (grp + 1 - 2 * core, col)
    zpeer = (lax.rem(grp + grp_count - 1 + 2 * core, grp_count), col)
    right = (grp, lax.rem(col + 1, col_count))
    left = (grp, lax.rem(col + col_count - 1, col_count))
    own0 = (1 + RA * core) * KB
    zout = (RA - 1) * core * KB
    zdst = (CR - 1) * (1 - core) * KB
    zin = (CR - 1) * core * KB

    to_xv = pltpu.make_async_copy(x_hbm, xv, lsem.at[0])
    to_col = pltpu.make_async_copy(x_hbm, colp1.at[pl.ds(own0, OWN)], lsem.at[1])
    to_xv.start()

    barrier = pltpu.get_barrier_semaphore()
    for peer in (partner, zpeer, right, left):
        pl.semaphore_signal(barrier, inc=1, device_id=peer, device_id_type=MESH)
    pl.semaphore_wait(barrier, 4)

    def remote(src, dst, send, recv, device):
        return pltpu.make_async_remote_copy(
            src_ref=src, dst_ref=dst, send_sem=send, recv_sem=recv,
            device_id=device, device_id_type=MESH,
        )

    def zsend(src, colp, p):
        return remote(src.at[pl.ds(zout, KB)], colp.at[pl.ds(zdst, KB)],
                      zsem.at[p, 0], zsem.at[p, 1], zpeer)

    def zfwd(colp, p):
        here = colp.at[pl.ds(zin, KB)]
        return remote(here, here, zsem.at[p, 2], zsem.at[p, 3], partner)

    def share(src, colp, p):
        return remote(src, colp.at[pl.ds(own0, OWN)], zsem.at[p, 4], zsem.at[p, 5], partner)

    def hop(snd, rcv, hs, hr, q, d, s):
        return remote(snd.at[d, s], rcv.at[(2 * d + core) * q + s], hs.at[d, s], hr.at[d, s],
                      (right, left)[d])

    def fwd(rcv, fs, fr, q, d, s):
        here = rcv.at[(2 * d + core) * q + s]
        return remote(here, here, fs.at[d, s], fr.at[d, s], partner)

    def relay(rcv, p, q, d, s):
        rank = s - FIRST
        return remote(rcv.at[(2 * d + core) * q + s], rcv.at[4 * q + d * RELAY + rank],
                      ysem.at[p, 0, d, rank], ysem.at[p, 1, d, rank], zpeer)

    def right_factor(colp, rcv, q, v):
        is_col = v < 64
        at_col = jnp.where(is_col, v, ZERO)
        at_rcv = jnp.where(is_col, 0, v - 64)
        part = at_rcv >> 5
        slot = at_rcv & 31
        direct = jnp.minimum(part, 3) * q + jnp.minimum(slot, q - 1)
        passed = 4 * q + jnp.clip((part - 4) * RELAY + slot, 0, 2 * RELAY - 1)
        return jnp.where(is_col, colp[at_col], rcv[jnp.where(part < 4, direct, passed)])

    def product(colp, rcv, phase, row, entry):
        acc = None
        for k in range(KB):
            v = pick[phase * PICKS + entry * KB + k]
            term = jnp.dot(xv[row * KB + k], right_factor(colp, rcv, (q1, q2)[phase], v),
                           preferred_element_type=jnp.float32)
            acc = term if acc is None else acc + term
        return acc

    def sent(phase, d, s):
        return tab[2 * phase + d, SRC_AT + s]

    def list_entry(phase, d, s):
        return jnp.clip(sent(phase, d, s) - own0, 0, OWN - 1)

    def find_factors(at):
        row = at // KB
        k = at - KB * row
        here = 1 + RA * core + row
        source = tab[here, NEAR_AT + 8 * k + 1]
        in_use = source >= 0
        source = jnp.where(in_use, source, 0)
        step_a = lax.rem(source // grid_c - (grp * RA + row) + 1 + grid_a, grid_a) - 1
        side = lax.rem(lax.rem(source, grid_c) - col + 1 + grid_c, grid_c)
        step_a = jnp.where(in_use, jnp.clip(step_a, -1, 1), 0)
        side = jnp.where(in_use, jnp.minimum(side, 2), 1)
        there = here + step_a
        for phase in range(2):
            held, spot = [], []
            for m in range(KB):
                held.append(tab[there, NEAR_AT + 8 * m + side + 3 * phase])
                code = tab[there, CODE_AT + 8 * m + 4 * phase + jnp.where(side == 0, 2, 3)]
                far = code + jnp.where(side == 0, 64, 128)
                spot.append(jnp.where(side == 1, there * KB + m, far))
            for f in range(KF):
                wanted = tab[here, NEAR_AT + 8 * f + 1 + 3 * (1 - phase)]
                usable = in_use & (wanted >= 0)
                got = jnp.int32(ZERO)
                for m in range(KB):
                    got = jnp.where(held[m] == wanted, spot[m], got)
                pick[phase * PICKS + (row * KB + f) * KB + k] = jnp.where(usable, got, ZERO)

    zero = jnp.zeros((B, B), jnp.bfloat16)

    zs1, zf1, sh1 = zsend(xv, colp1, 0), zfwd(colp1, 0), share(xv, colp1, 0)
    to_xv.wait()
    zs1.start()
    to_col.start()
    sh1.start()
    hop1 = functools.partial(hop, snd1, rcv1, hs1, hr1, q1)
    fwd1 = functools.partial(fwd, rcv1, fs1, fr1, q1)
    pass1 = functools.partial(relay, rcv1, 0, q1)

    @pl.loop(0, FIRST)
    def _(s):
        for d in range(2):
            snd1[d, s] = xv[list_entry(0, d, s)]

        @pl.when(s > 0)
        def _():
            for d in range(2):
                hop1(d, s - 1).start()

    colp1[ZERO] = zero
    colp2[ZERO] = zero
    for d in range(2):
        hop1(d, FIRST - 1).start()
    to_col.wait()
    zs1.wait_recv()
    zf1.start()
    sh1.wait_recv()
    zf1.wait_recv()

    @pl.loop(FIRST, q1)
    def _(s):
        for d in range(2):
            snd1[d, s] = colp1[sent(0, d, s)]

        @pl.when(s > FIRST)
        def _():
            for d in range(2):
                hop1(d, s - 1).start()

    for d in range(2):
        hop1(d, q1 - 1).start()

    pl.loop(0, OWN)(find_factors)

    @pl.loop(0, q1)
    def _(s):
        for d in range(2):
            hop1(d, s).wait_recv()
            fwd1(d, s).start()

        @pl.when((s >= FIRST) & (s < FIRST + RELAY))
        def _():
            for d in range(2):
                pass1(d, s).start()

    @pl.loop(0, q1)
    def _(s):
        for d in range(2):
            fwd1(d, s).wait_recv()

    for s in range(FIRST, FIRST + RELAY):
        for d in range(2):
            pass1(d, s).wait_recv()

    zs2, zf2, sh2 = zsend(sown, colp2, 1), zfwd(colp2, 1), share(sown, colp2, 1)
    hop2 = functools.partial(hop, snd2, rcv2, hs2, hr2, q2)
    fwd2 = functools.partial(fwd, rcv2, fs2, fr2, q2)
    pass2 = functools.partial(relay, rcv2, 1, q2)

    @pl.loop(0, 2)
    def _(s):
        for d in range(2):
            entry = list_entry(1, d, s)
            snd2[d, s] = product(colp1, rcv1, 0, entry // KB, entry).astype(jnp.bfloat16)

        @pl.when(s > 0)
        def _():
            for d in range(2):
                hop2(d, s - 1).start()

    @pl.loop(0, OWN // 2)
    def _(t):
        step = t // 3
        row = step + core * (RA - 1 - 2 * step)
        for u in range(2):
            entry = row * KB + (t - 3 * step) * 2 + u
            block = product(colp1, rcv1, 0, row, entry).astype(jnp.bfloat16)
            sown[entry] = block
            colp2[own0 + entry] = block

        @pl.when(t == 0)
        def _():
            for d in range(2):
                hop2(d, 1).start()

        @pl.when(t == 3)
        def _():
            zs2.start()

    @pl.loop(2, FIRST)
    def _(s):
        for d in range(2):
            snd2[d, s] = sown[list_entry(1, d, s)]

        @pl.when(s > 2)
        def _():
            for d in range(2):
                hop2(d, s - 1).start()

    sh2.start()
    for d in range(2):
        hop2(d, FIRST - 1).start()
    zs2.wait_recv()
    zf2.start()
    sh2.wait_recv()
    zf2.wait_recv()

    @pl.loop(FIRST, q2)
    def _(s):
        for d in range(2):
            snd2[d, s] = colp2[sent(1, d, s)]

        @pl.when(s > FIRST)
        def _():
            for d in range(2):
                hop2(d, s - 1).start()

    for d in range(2):
        hop2(d, q2 - 1).start()

    @pl.loop(0, q2)
    def _(s):
        for d in range(2):
            hop2(d, s).wait_recv()
            fwd2(d, s).start()

        @pl.when((s >= FIRST) & (s < FIRST + RELAY))
        def _():
            for d in range(2):
                pass2(d, s).start()

    @pl.loop(0, q2)
    def _(s):
        for d in range(2):
            fwd2(d, s).wait_recv()

    for s in range(FIRST, FIRST + RELAY):
        for d in range(2):
            pass2(d, s).wait_recv()

    def write(row):
        rows = pl.ds(row * KB, KB)
        return pltpu.make_async_copy(outv.at[rows], out_hbm.at[rows], osem.at[row])

    @pl.loop(0, OWN // 2)
    def _(t):
        row = t // 3
        for u in range(2):
            entry = 2 * t + u
            cubed = product(colp2, rcv2, 1, row, entry)
            in_use = tab[1 + RA * core + row, NEAR_AT + 8 * (entry - row * KB) + 1] >= 0
            own = xv[entry].astype(jnp.float32)
            step = 1.5 * own - cubed * (0.5 / (KB * B))
            outv[entry] = jnp.where(in_use, step, 0.0).astype(jnp.bfloat16)

        @pl.when((t > 0) & (t - 3 * row == 0))
        def _():
            write(row - 1).start()

    for s in range(FIRST, FIRST + RELAY):
        for d in range(2):
            pass1(d, s).wait_send()
            pass2(d, s).wait_send()
    zs1.wait_send()
    zf1.wait_send()
    sh1.wait_send()
    zs2.wait_send()
    zf2.wait_send()
    sh2.wait_send()

    @pl.loop(0, q1)
    def _(s):
        for d in range(2):
            hop1(d, s).wait_send()
            fwd1(d, s).wait_send()

    @pl.loop(0, q2)
    def _(s):
        for d in range(2):
            hop2(d, s).wait_send()
            fwd2(d, s).wait_send()

    write(RA - 1).start()
    for row in range(RA):
        write(row).wait()


def sparse(level, grid_a, grid_c, x_blocks, table):
    q1, q2 = LEVELS[level]
    blocks = x_blocks.reshape(OWN, B, B)
    vm = lambda *lead: pltpu.VMEM((*lead, B, B), jnp.bfloat16)
    dma = lambda *lead: pltpu.SemaphoreType.DMA(lead)
    out = pl.pallas_call(
        functools.partial(kernel, q1, q2, grid_a, grid_c, lax.axis_size("grp"), lax.axis_size("col")),
        out_shape=jax.ShapeDtypeStruct(blocks.shape, jnp.bfloat16),
        in_specs=[
            pl.BlockSpec(memory_space=pltpu.SMEM),
            pl.BlockSpec(memory_space=pl.ANY),
        ],
        out_specs=pl.BlockSpec(memory_space=pl.ANY),
        scratch_shapes=[
            pltpu.SMEM((2 * PICKS,), jnp.int32),
            vm(OWN), vm(COLN + 1), vm(4 * q1 + 2 * RELAY), vm(2, q1), vm(COLN + 1),
            vm(4 * q2 + 2 * RELAY), vm(2, q2),
            vm(OWN), vm(OWN),
            dma(2), dma(RA), dma(2, 6),
            dma(2, q1), dma(2, q1), dma(2, q1), dma(2, q1),
            dma(2, q2), dma(2, q2), dma(2, q2), dma(2, q2), dma(2, 2, 2, RELAY),
        ],
        compiler_params=pltpu.CompilerParams(
            collective_id=level, has_side_effects=True, vmem_limit_bytes=62 * 1024 * 1024
        ),
        name=f"sign_step_{q1}_{q2}",
    )(table, blocks)
    return out.reshape(x_blocks.shape)


def local(x_blocks, columns, filter_ids):
    grid_a, grid_c, _ = columns.shape
    table, level = list_tables(columns, filter_ids)
    branches = [
        functools.partial(lambda at, x, c, f, t: sparse(at, grid_a, grid_c, x, t), at)
        for at in range(len(LEVELS))
    ]
    branches.append(lambda x, c, f, t: dense(x, c, f))
    return lax.switch(level[0], branches, x_blocks, columns, filter_ids, table)


def solution(mesh):
    return jax.shard_map(
        local,
        mesh=mesh,
        in_specs=(P("grp", "col", None, None, None), P(), P()),
        out_specs=P("grp", "col", None, None, None),
        check_vma=False,
    )
```

```python
import functools

import jax
import jax.numpy as jnp
from jax import lax
from jax.experimental import pallas as pl
from jax.experimental.pallas import tpu as pltpu
from jax.sharding import PartitionSpec as P

B = 256
KB = 6
KF = 6
RA = 4
OWN = RA * KB
CR = 2 * RA + 2
COLN = CR * KB
ZERO = COLN
FIRST = 5
RELAY = 4
LEVELS = ((11, 13), (11, 14), (12, 14), (12, 15), (13, 16), (15, 19))

PICKS = OWN * KB
MESH = pl.DeviceIdType.MESH


def padded(cells, sides, width):
    for axis, dim in sides:
        count = lax.axis_size(axis)
        head = lax.slice_in_dim(cells, 0, width, axis=dim)
        tail = lax.slice_in_dim(cells, cells.shape[dim] - width, cells.shape[dim], axis=dim)
        cells = jnp.concatenate(
            [
                lax.ppermute(tail, axis, [(i, (i + 1) % count) for i in range(count)]),
                cells,
                lax.ppermute(head, axis, [((i + 1) % count, i) for i in range(count)]),
            ],
            axis=dim,
        )
    return cells


def block_terms(
    halo, pos_a, pos_c, row_ids, row_cols, left_blocks, stored_table, wanted, grid_a, grid_c
):
    slot_count = halo.shape[2]
    width = halo.shape[3]
    in_use = row_cols >= 0
    source = jnp.where(in_use, row_cols, 0)
    home_a = row_ids // grid_c
    home_c = row_ids % grid_c
    step_a = (source // grid_c - home_a[:, None] + 1) % grid_a - 1
    step_c = (source % grid_c - home_c[:, None] + 1) % grid_c - 1
    place = (pos_a[:, None] + step_a) * halo.shape[1] + pos_c[:, None] + step_c
    flat = halo.reshape((halo.shape[0] * halo.shape[1] * slot_count, width, width))
    stored = stored_table[source]
    matches = stored[:, :, None, :] == wanted[:, None, :, None]
    present = jnp.any(matches, axis=3) & (wanted[:, None, :] >= 0) & in_use[:, :, None]
    slot_of = jnp.argmax(matches.astype(jnp.int32), axis=3)
    block_index = place[:, :, None] * slot_count + slot_of

    def one_row(inputs):
        index_row, present_row, left_row = inputs
        picked = flat[index_row]
        picked = jnp.where(present_row[:, :, None, None], picked, jnp.zeros((), picked.dtype))
        return jnp.einsum("kab,kfbc->fac", left_row, picked, preferred_element_type=jnp.float32)

    return lax.map(one_row, (block_index, present, left_blocks))


def dense(x_blocks, columns, filter_ids):
    grp_count = lax.axis_size("grp")
    col_count = lax.axis_size("col")
    rows_a = x_blocks.shape[0]
    rows_c = x_blocks.shape[1]
    grid_a = rows_a * grp_count
    grid_c = rows_c * col_count
    col_table = columns.reshape(grid_a * grid_c, KB)
    filt_table = filter_ids.reshape(grid_a * grid_c, KF)
    local_rows = rows_a * rows_c
    offsets = jnp.arange(local_rows, dtype=jnp.int32)
    local_a = offsets // rows_c
    local_c = offsets % rows_c
    row_ids = (
        (lax.axis_index("grp") * rows_a + local_a) * grid_c
        + lax.axis_index("col") * rows_c
        + local_c
    )
    row_cols = col_table[row_ids]
    left_blocks = x_blocks.reshape(local_rows, KB, B, B)
    along_col = padded(x_blocks, (("col", 1),), 1)
    near_x = padded(along_col, (("grp", 0),), 1)
    square = block_terms(
        near_x,
        local_a + 1,
        local_c + 1,
        row_ids,
        row_cols,
        left_blocks,
        col_table,
        filt_table[row_ids],
        grid_a,
        grid_c,
    ).astype(jnp.bfloat16)
    square = square.reshape(rows_a, rows_c, KF, B, B)
    square_along = padded(square, (("col", 1),), 1)
    near_square = padded(square_along, (("grp", 0),), 1)
    cubed = block_terms(
        near_square,
        local_a + 1,
        local_c + 1,
        row_ids,
        row_cols,
        left_blocks,
        filt_table,
        row_cols,
        grid_a,
        grid_c,
    )
    in_use = (row_cols >= 0).astype(jnp.float32)
    result = (1.5 * left_blocks.astype(jnp.float32) - cubed * (0.5 / (KB * B))) * in_use[
        :, :, None, None
    ]
    return result.astype(jnp.bfloat16).reshape(x_blocks.shape)


LANES = 128
LISTS = 8
CODE_AT = 0
NEAR_AT = 48
SRC_AT = 96
TABLE_ROWS = 16


def index_kernel(cols_ref, filt_ref, table_ref, level_ref, own_ref, halo_ref, move_ref,
                 cols_s, filt_s):
    grp = lax.axis_index("grp")
    col = lax.axis_index("col")
    core = lax.rem(grp, 2)
    grid_c = cols_ref.shape[1]
    grid_a = cols_ref.shape[2]
    chip = 2 * RA

    def lanes_of(x):
        return jnp.concatenate([x] * (LANES // grid_a), axis=1)

    stored, kept = [], []
    for m in range(KB):
        stored.append(lanes_of(cols_ref[m]))
        kept.append(lanes_of(filt_ref[m]))
        cols_s[m] = stored[m]
        filt_s[m] = kept[m]
    shape = (grid_c, LANES)
    lane = lax.broadcasted_iota(jnp.int32, shape, 1)
    ids = lax.rem(lane, grid_a) * grid_c + lax.broadcasted_iota(jnp.int32, shape, 0)
    in_chip = lax.rem(lane, chip)
    first, last = in_chip == 0, in_chip == chip - 1
    false = jnp.zeros(shape, jnp.int32)

    def either(tests):
        got = tests[0]
        for t in tests[1:]:
            got = got | t
        return got

    totals = []
    for d, step_c in enumerate((1, -1)):
        cols_c = [jnp.roll(x, -step_c, 0) for x in stored]
        filt_c = [jnp.roll(x, -step_c, 0) for x in kept]
        found = []
        for step_a in (-1, 0, 1):
            shift = (-step_a) % LANES
            cols_r = [pltpu.roll(x, shift, 1) if shift else x for x in cols_c]
            filt_r = [pltpu.roll(x, shift, 1) if shift else x for x in filt_c]
            member = either([x == ids for x in cols_r])
            one = [either([stored[m] == x for x in filt_r]) & member & (stored[m] >= 0) for m in range(KB)]
            two = [either([kept[m] == x for x in cols_r]) & member for m in range(KB)]
            found.append((one, two))
        up, mid, down = found
        for phase in (0, 1):
            own_row, halo_row = false, false
            flags = []
            for m in range(KB):
                u, c, w = up[phase][m], mid[phase][m], down[phase][m]
                own = (c | (u & ~first) | (w & ~last)).astype(jnp.int32)
                halo = ((u & first) | (w & last)).astype(jnp.int32)
                flags.append((own, halo))
                own_row = own_row + own
                halo_row = halo_row + halo
            totals.append((phase, d, flags, own_row, halo_row))

    def summed(x, rule):
        at = lax.broadcasted_iota(jnp.int32, (LANES, LANES), 0)
        to = lax.broadcasted_iota(jnp.int32, (LANES, LANES), 1)
        weight = rule(at, to).astype(jnp.float32).astype(jnp.bfloat16)
        return jnp.dot(
            x.astype(jnp.float32).astype(jnp.bfloat16), weight, preferred_element_type=jnp.float32
        ).astype(jnp.int32)

    def same_chip(at, to):
        return (at // chip == lax.rem(to, grid_a) // chip) & (at < grid_a)

    def beside(at, to):
        z = lax.rem(to, grid_a) // chip * chip
        above = lax.rem(z + grid_a - 1, grid_a)
        below = lax.rem(z + chip, grid_a)
        return (at == above) | (at == below)

    def stack(xs):
        return jnp.concatenate(xs, axis=0)

    loads = summed(stack([t[3] for t in totals]), same_chip) + summed(
        stack([t[4] for t in totals]), beside
    )

    def across(x):
        return jnp.where(last, pltpu.roll(x, LANES - 1, 1), pltpu.roll(x, 1, 1))

    kept_own, kept_halo, got0, got1 = [], [], [], []
    for p, (phase, d, flags, _, _) in enumerate(totals):
        load = loads[p * grid_c : (p + 1) * grid_c]
        lead = jnp.where(last, load - across(load), across(load) - load)
        far = jnp.abs(lead)
        count = jnp.zeros(shape, jnp.int32)
        for step in range(RELAY):
            count = count + (far >= 3 * step + 2).astype(jnp.int32)
        ups = (lead > 0).astype(jnp.int32)
        rim = (first | last).astype(jnp.int32)
        both = [own * halo * rim for own, halo in flags]
        lower = [jnp.where(last, own, halo) for own, halo in flags]
        upper = [jnp.where(last, halo, own) for own, halo in flags]
        single = [
            jnp.where(ups > 0, lower[m], upper[m]) * rim - both[m] for m in range(KB)
        ]
        n_both = sum(both[1:], both[0])
        n_single = sum(single[1:], single[0])
        both_rank = jnp.where(last, 0, across(n_both))
        single_rank = n_both + across(n_both) + jnp.where(last, 0, across(n_single))
        own_row, halo_row, moved_row = false, false, false
        for m in range(KB):
            rank = jnp.where(both[m] > 0, both_rank, single_rank)
            moved = ((both[m] + single[m]) > 0) & (rank < count)
            move = jnp.where(moved, rank + 1 + 8 * ups, 0)
            both_rank = both_rank + both[m]
            single_rank = single_rank + single[m]
            own = jnp.where(moved, 0, flags[m][0])
            halo = jnp.where(moved, 0, flags[m][1])
            own_ref[phase, d, m] = own
            halo_ref[phase, d, m] = halo
            move_ref[phase, d, m] = move
            own_row, halo_row = own_row + own, halo_row + halo
            moved_row = moved_row + moved.astype(jnp.int32)
        moved_row = moved_row + across(moved_row)
        kept_own.append(own_row)
        kept_halo.append(halo_row)
        got0.append(jnp.where(first, moved_row * ups, 0))
        got1.append(jnp.where(last, moved_row * (1 - ups), 0))

    def split(n0, n1, total, extra0, extra1):
        half = jnp.clip((total + extra1 - extra0 + 1) >> 1, 0, total)
        return half, jnp.maximum(FIRST - n0, 0), jnp.maximum(FIRST - n1, 0)

    own_all = stack(kept_own)
    n0 = summed(own_all, lambda at, to: same_chip(at, to) & (lax.rem(at, chip) < RA))
    n1 = summed(own_all, lambda at, to: same_chip(at, to) & (lax.rem(at, chip) >= RA))
    total = n0 + n1 + summed(stack(kept_halo), beside)
    extra0 = summed(stack(got0), same_chip)
    extra1 = summed(stack(got1), same_chip)
    half, gap0, gap1 = split(n0, n1, total, extra0, extra1)
    rest = total - half
    fill = jnp.maximum(
        half + jnp.where(half > n0, gap0, 0) + extra0,
        rest + jnp.where(rest > n1, gap1, 0) + extra1,
    )
    most = [jnp.int32(FIRST + RELAY), jnp.int32(FIRST + RELAY)]
    for p, (phase, _, _, _, _) in enumerate(totals):
        most[phase] = jnp.maximum(most[phase], jnp.max(fill[p * grid_c : (p + 1) * grid_c]))
    level = jnp.int32(len(LEVELS))
    for at in reversed(range(len(LEVELS))):
        fits = (most[0] <= LEVELS[at][0]) & (most[1] <= LEVELS[at][1])
        level = jnp.where(fits, at, level)
    level_ref[0] = level

    z = grp // 2
    shift = lax.rem(LANES + 1 - z * chip, LANES)
    west = lax.rem(col + grid_c - 1, grid_c)
    east = lax.rem(col + 1, grid_c)
    row8 = (LISTS, LANES)
    lane8 = lax.broadcasted_iota(jnp.int32, row8, 1)
    rim = (lane8 == 0) | (lane8 == CR - 1)
    lists = [(p, d, c) for p in (0, 1) for d, c in ((0, col), (1, col), (0, west), (1, east))]

    def near(ref_rows):
        return pltpu.roll(jnp.concatenate(ref_rows, axis=0), shift, 1)

    need, in_row, stores, moves = [], [], [], []
    run = jnp.zeros(row8, jnp.int32)
    relayed = jnp.zeros(row8, jnp.int32)
    low_end = lane8 <= 1
    for m in range(KB):
        own = near([own_ref[p, d, m, pl.ds(c, 1), :] for p, d, c in lists])
        halo = near([halo_ref[p, d, m, pl.ds(c, 1), :] for p, d, c in lists])
        flags = jnp.where(lane8 < CR, jnp.where(rim, halo, own), 0)
        need.append(flags)
        in_row.append(run)
        run = run + flags
        move = near([move_ref[p, d, m, pl.ds(c, 1), :] for p, d, c in lists])
        move = jnp.where((lane8 <= 1) | ((lane8 >= CR - 2) & (lane8 < CR)), move, 0)
        mine = (move > 0) & ((move > 8) == low_end)
        moves.append((move, mine))
        relayed = relayed + mine.astype(jnp.int32)
        rows = [cols_s[m, pl.ds(c, 1), :] for c in (west, col, east)]
        rows += [filt_s[m, pl.ds(c, 1), :] for c in (west, col, east)]
        stores.append(near(rows + rows[:2]))
    n0 = summed(run, lambda at, to: (at >= 1) & (at <= RA))
    n1 = summed(run, lambda at, to: (at > RA) & (at <= chip))
    above = summed(run, lambda at, to: at == 0)
    below = summed(run, lambda at, to: at == CR - 1)
    ahead = summed(
        run, lambda at, to: (at < to) & (((at >= 1) & (to <= RA)) | ((at > RA) & (to <= chip)))
    )
    total = n0 + n1 + above + below
    extra0 = summed(relayed, lambda at, to: at <= 1)
    extra1 = summed(relayed, lambda at, to: at > 1)
    half, gap0, gap1 = split(n0, n1, total, extra0, extra1)
    east_list = lax.rem(lax.broadcasted_iota(jnp.int32, row8, 0), 4) == 3
    of0 = (lane8 >= 1) & (lane8 <= RA)
    of1 = (lane8 > RA) & (lane8 <= chip)
    slots = lax.broadcasted_iota(jnp.int32, (32, LANES), 0) + core * 32
    entry = lax.broadcasted_iota(jnp.int32, (32, LANES), 1) * KB
    source = [jnp.zeros((32, LANES), jnp.int32) for _ in range(4)]
    codes = []
    for m in range(KB):
        place = ahead + in_row[m]
        place = jnp.where(lane8 == 0, n0 + in_row[m], place)
        place = jnp.where(lane8 == CR - 1, n0 + above + in_row[m], place)
        place = jnp.where(of1, total - 1 - place, place)
        turned = total - 1 - place
        slot0 = place + jnp.where(of0, 0, gap0)
        slot1 = turned + jnp.where(of1, 0, gap1)
        slot0 = slot0 + jnp.where(slot0 >= FIRST, extra0, 0)
        slot1 = slot1 + jnp.where(slot1 >= FIRST, extra1, 0)
        code = jnp.where(place < half, slot0, 32 + slot1)
        move, mine = moves[m]
        rank = (move & 7) - 1
        code = jnp.where(mine, jnp.where(low_end, FIRST, 32 + FIRST) + rank, code)
        code = jnp.where((move > 0) & ~mine, jnp.where(east_list, 96, 128) + rank, code)
        codes.append(code)
        sent = jnp.where((need[m] > 0) | mine, code, -1)
        for i, at in enumerate((0, 1, 4, 5)):
            same = jnp.broadcast_to(sent[at : at + 1], (32, LANES)) == slots
            source[i] = source[i] + jnp.where(same, entry + m, 0)
    lane32 = lax.broadcasted_iota(jnp.int32, (32, LANES), 1)
    out = jnp.zeros((32, LANES), jnp.int32)
    for i in range(4):
        out = jnp.where(lane32 == i, jnp.sum(source[i], axis=1, keepdims=True), out)
    table_ref[...] = jnp.concatenate(codes + stores + [out], axis=0).T[:TABLE_ROWS]


def list_tables(columns, filter_ids):
    grid_a, grid_c, _ = columns.shape
    ints = lambda *shape: pltpu.VMEM(shape, jnp.int32)
    return pl.pallas_call(
        index_kernel,
        out_shape=(
            jax.ShapeDtypeStruct((TABLE_ROWS, LANES), jnp.int32),
            jax.ShapeDtypeStruct((1,), jnp.int32),
        ),
        in_specs=[pl.BlockSpec(memory_space=pltpu.VMEM)] * 2,
        out_specs=(
            pl.BlockSpec(memory_space=pltpu.VMEM),
            pl.BlockSpec(memory_space=pltpu.SMEM),
        ),
        scratch_shapes=[
            ints(2, 2, KB, grid_c, LANES), ints(2, 2, KB, grid_c, LANES),
            ints(2, 2, KB, grid_c, LANES),
            ints(KB, grid_c, LANES), ints(KF, grid_c, LANES),
        ],
        name="block_lists",
    )(columns.transpose(2, 1, 0), filter_ids.transpose(2, 1, 0))


def kernel(q1, q2, grid_a, grid_c, grp_count, col_count, tab, x_hbm, out_ref, pick, xv, colp1, rcv1, snd1, colp2, rcv2,
           snd2, sown, lsem, zsem, hs1, hr1, fs1, fr1, hs2, hr2, fs2, fr2, ysem):
    grp = lax.axis_index("grp")
    col = lax.axis_index("col")
    core = lax.rem(grp, 2)
    partner = (grp + 1 - 2 * core, col)
    zpeer = (lax.rem(grp + grp_count - 1 + 2 * core, grp_count), col)
    right = (grp, lax.rem(col + 1, col_count))
    left = (grp, lax.rem(col + col_count - 1, col_count))
    own0 = (1 + RA * core) * KB
    zout = (RA - 1) * core * KB
    zdst = (CR - 1) * (1 - core) * KB
    zin = (CR - 1) * core * KB

    to_xv = pltpu.make_async_copy(x_hbm, xv, lsem.at[0])
    to_col = pltpu.make_async_copy(x_hbm, colp1.at[pl.ds(own0, OWN)], lsem.at[1])
    to_xv.start()

    barrier = pltpu.get_barrier_semaphore()
    for peer in (partner, zpeer, right, left):
        pl.semaphore_signal(barrier, inc=1, device_id=peer, device_id_type=MESH)
    pl.semaphore_wait(barrier, 4)

    def remote(src, dst, send, recv, device):
        return pltpu.make_async_remote_copy(
            src_ref=src, dst_ref=dst, send_sem=send, recv_sem=recv,
            device_id=device, device_id_type=MESH,
        )

    def zsend(src, colp, p):
        return remote(src.at[pl.ds(zout, KB)], colp.at[pl.ds(zdst, KB)],
                      zsem.at[p, 0], zsem.at[p, 1], zpeer)

    def zfwd(colp, p):
        here = colp.at[pl.ds(zin, KB)]
        return remote(here, here, zsem.at[p, 2], zsem.at[p, 3], partner)

    def share(src, colp, p):
        return remote(src, colp.at[pl.ds(own0, OWN)], zsem.at[p, 4], zsem.at[p, 5], partner)

    def hop(snd, rcv, hs, hr, q, d, s):
        return remote(snd.at[d, s], rcv.at[(2 * d + core) * q + s], hs.at[d, s], hr.at[d, s],
                      (right, left)[d])

    def fwd(rcv, fs, fr, q, d, s):
        here = rcv.at[(2 * d + core) * q + s]
        return remote(here, here, fs.at[d, s], fr.at[d, s], partner)

    def relay(rcv, p, q, d, s):
        rank = s - FIRST
        return remote(rcv.at[(2 * d + core) * q + s], rcv.at[4 * q + d * RELAY + rank],
                      ysem.at[p, 0, d, rank], ysem.at[p, 1, d, rank], zpeer)

    def right_factor(colp, rcv, q, v):
        is_col = v < 64
        at_col = jnp.where(is_col, v, ZERO)
        at_rcv = jnp.where(is_col, 0, v - 64)
        part = at_rcv >> 5
        slot = at_rcv & 31
        direct = jnp.minimum(part, 3) * q + jnp.minimum(slot, q - 1)
        passed = 4 * q + jnp.clip((part - 4) * RELAY + slot, 0, 2 * RELAY - 1)
        return jnp.where(is_col, colp[at_col], rcv[jnp.where(part < 4, direct, passed)])

    def product(colp, rcv, phase, row, entry):
        acc = None
        for k in range(KB):
            v = pick[phase * PICKS + entry * KB + k]
            term = jnp.dot(xv[row * KB + k], right_factor(colp, rcv, (q1, q2)[phase], v),
                           preferred_element_type=jnp.float32)
            acc = term if acc is None else acc + term
        return acc

    def sent(phase, d, s):
        return tab[2 * phase + d, SRC_AT + s]

    def list_entry(phase, d, s):
        return jnp.clip(sent(phase, d, s) - own0, 0, OWN - 1)

    def find_factors(at):
        row = at // KB
        k = at - KB * row
        here = 1 + RA * core + row
        source = tab[here, NEAR_AT + 8 * k + 1]
        in_use = source >= 0
        source = jnp.where(in_use, source, 0)
        step_a = lax.rem(source // grid_c - (grp * RA + row) + 1 + grid_a, grid_a) - 1
        side = lax.rem(lax.rem(source, grid_c) - col + 1 + grid_c, grid_c)
        step_a = jnp.where(in_use, jnp.clip(step_a, -1, 1), 0)
        side = jnp.where(in_use, jnp.minimum(side, 2), 1)
        there = here + step_a
        for phase in range(2):
            held, spot = [], []
            for m in range(KB):
                held.append(tab[there, NEAR_AT + 8 * m + side + 3 * phase])
                code = tab[there, CODE_AT + 8 * m + 4 * phase + jnp.where(side == 0, 2, 3)]
                far = code + jnp.where(side == 0, 64, 128)
                spot.append(jnp.where(side == 1, there * KB + m, far))
            for f in range(KF):
                wanted = tab[here, NEAR_AT + 8 * f + 1 + 3 * (1 - phase)]
                usable = in_use & (wanted >= 0)
                got = jnp.int32(ZERO)
                for m in range(KB):
                    got = jnp.where(held[m] == wanted, spot[m], got)
                pick[phase * PICKS + (row * KB + f) * KB + k] = jnp.where(usable, got, ZERO)

    zero = jnp.zeros((B, B), jnp.bfloat16)

    zs1, zf1, sh1 = zsend(xv, colp1, 0), zfwd(colp1, 0), share(xv, colp1, 0)
    to_xv.wait()
    zs1.start()
    to_col.start()
    sh1.start()
    hop1 = functools.partial(hop, snd1, rcv1, hs1, hr1, q1)
    fwd1 = functools.partial(fwd, rcv1, fs1, fr1, q1)
    pass1 = functools.partial(relay, rcv1, 0, q1)

    @pl.loop(0, FIRST)
    def _(s):
        for d in range(2):
            snd1[d, s] = xv[list_entry(0, d, s)]

        @pl.when(s > 0)
        def _():
            for d in range(2):
                hop1(d, s - 1).start()

    colp1[ZERO] = zero
    colp2[ZERO] = zero
    for d in range(2):
        hop1(d, FIRST - 1).start()
    to_col.wait()
    zs1.wait_recv()
    zf1.start()
    sh1.wait_recv()
    zf1.wait_recv()

    @pl.loop(FIRST, q1)
    def _(s):
        for d in range(2):
            snd1[d, s] = colp1[sent(0, d, s)]

        @pl.when(s > FIRST)
        def _():
            for d in range(2):
                hop1(d, s - 1).start()

    for d in range(2):
        hop1(d, q1 - 1).start()

    pl.loop(0, OWN)(find_factors)

    @pl.loop(0, q1)
    def _(s):
        for d in range(2):
            hop1(d, s).wait_recv()
            fwd1(d, s).start()

        @pl.when((s >= FIRST) & (s < FIRST + RELAY))
        def _():
            for d in range(2):
                pass1(d, s).start()

    @pl.loop(0, q1)
    def _(s):
        for d in range(2):
            fwd1(d, s).wait_recv()

    for s in range(FIRST, FIRST + RELAY):
        for d in range(2):
            pass1(d, s).wait_recv()

    zs2, zf2, sh2 = zsend(sown, colp2, 1), zfwd(colp2, 1), share(sown, colp2, 1)
    hop2 = functools.partial(hop, snd2, rcv2, hs2, hr2, q2)
    fwd2 = functools.partial(fwd, rcv2, fs2, fr2, q2)
    pass2 = functools.partial(relay, rcv2, 1, q2)

    @pl.loop(0, 2)
    def _(s):
        for d in range(2):
            entry = list_entry(1, d, s)
            snd2[d, s] = product(colp1, rcv1, 0, entry // KB, entry).astype(jnp.bfloat16)

        @pl.when(s > 0)
        def _():
            for d in range(2):
                hop2(d, s - 1).start()

    @pl.loop(0, OWN // 2)
    def _(t):
        step = t // 3
        row = step + core * (RA - 1 - 2 * step)
        for u in range(2):
            entry = row * KB + (t - 3 * step) * 2 + u
            block = product(colp1, rcv1, 0, row, entry).astype(jnp.bfloat16)
            sown[entry] = block
            colp2[own0 + entry] = block

        @pl.when(t == 0)
        def _():
            for d in range(2):
                hop2(d, 1).start()

        @pl.when(t == 3)
        def _():
            zs2.start()

    @pl.loop(2, FIRST)
    def _(s):
        for d in range(2):
            snd2[d, s] = sown[list_entry(1, d, s)]

        @pl.when(s > 2)
        def _():
            for d in range(2):
                hop2(d, s - 1).start()

    sh2.start()
    for d in range(2):
        hop2(d, FIRST - 1).start()
    zs2.wait_recv()
    zf2.start()
    sh2.wait_recv()
    zf2.wait_recv()

    @pl.loop(FIRST, q2)
    def _(s):
        for d in range(2):
            snd2[d, s] = colp2[sent(1, d, s)]

        @pl.when(s > FIRST)
        def _():
            for d in range(2):
                hop2(d, s - 1).start()

    for d in range(2):
        hop2(d, q2 - 1).start()

    @pl.loop(0, q2)
    def _(s):
        for d in range(2):
            hop2(d, s).wait_recv()
            fwd2(d, s).start()

        @pl.when((s >= FIRST) & (s < FIRST + RELAY))
        def _():
            for d in range(2):
                pass2(d, s).start()

    @pl.loop(0, q2)
    def _(s):
        for d in range(2):
            fwd2(d, s).wait_recv()

    for s in range(FIRST, FIRST + RELAY):
        for d in range(2):
            pass2(d, s).wait_recv()

    @pl.loop(0, OWN // 2)
    def _(t):
        row = t // 3
        for u in range(2):
            entry = 2 * t + u
            cubed = product(colp2, rcv2, 1, row, entry)
            in_use = tab[1 + RA * core + row, NEAR_AT + 8 * (entry - row * KB) + 1] >= 0
            own = xv[entry].astype(jnp.float32)
            step = 1.5 * own - cubed * (0.5 / (KB * B))
            out_ref[entry] = jnp.where(in_use, step, 0.0).astype(jnp.bfloat16)

    for s in range(FIRST, FIRST + RELAY):
        for d in range(2):
            pass1(d, s).wait_send()
            pass2(d, s).wait_send()
    zs1.wait_send()
    zf1.wait_send()
    sh1.wait_send()
    zs2.wait_send()
    zf2.wait_send()
    sh2.wait_send()

    @pl.loop(0, q1)
    def _(s):
        for d in range(2):
            hop1(d, s).wait_send()
            fwd1(d, s).wait_send()

    @pl.loop(0, q2)
    def _(s):
        for d in range(2):
            hop2(d, s).wait_send()
            fwd2(d, s).wait_send()


def sparse(level, grid_a, grid_c, x_blocks, table):
    q1, q2 = LEVELS[level]
    blocks = x_blocks.reshape(OWN, B, B)
    vm = lambda *lead: pltpu.VMEM((*lead, B, B), jnp.bfloat16)
    dma = lambda *lead: pltpu.SemaphoreType.DMA(lead)
    out = pl.pallas_call(
        functools.partial(kernel, q1, q2, grid_a, grid_c, lax.axis_size("grp"), lax.axis_size("col")),
        out_shape=pltpu.VMEM(blocks.shape, jnp.bfloat16),
        in_specs=[
            pl.BlockSpec(memory_space=pltpu.SMEM),
            pl.BlockSpec(memory_space=pl.ANY),
        ],
        out_specs=pl.BlockSpec(memory_space=pltpu.VMEM),
        scratch_shapes=[
            pltpu.SMEM((2 * PICKS,), jnp.int32),
            vm(OWN), vm(COLN + 1), vm(4 * q1 + 2 * RELAY), vm(2, q1), vm(COLN + 1),
            vm(4 * q2 + 2 * RELAY), vm(2, q2),
            vm(OWN),
            dma(2), dma(2, 6),
            dma(2, q1), dma(2, q1), dma(2, q1), dma(2, q1),
            dma(2, q2), dma(2, q2), dma(2, q2), dma(2, q2), dma(2, 2, 2, RELAY),
        ],
        compiler_params=pltpu.CompilerParams(
            collective_id=level, has_side_effects=True, vmem_limit_bytes=58 * 1024 * 1024
        ),
        name=f"sign_step_{q1}_{q2}",
    )(table, blocks)
    return written(out).reshape(x_blocks.shape)


def written(blocks):
    def copy(src, dst, sem):
        move = pltpu.make_async_copy(src, dst, sem)
        move.start()
        move.wait()

    return pl.pallas_call(
        copy,
        out_shape=jax.ShapeDtypeStruct(blocks.shape, blocks.dtype),
        in_specs=[pl.BlockSpec(memory_space=pltpu.VMEM)],
        out_specs=pl.BlockSpec(memory_space=pl.ANY),
        scratch_shapes=[pltpu.SemaphoreType.DMA(())],
        compiler_params=pltpu.CompilerParams(vmem_limit_bytes=4 * 1024 * 1024),
        name="write_out",
    )(blocks)


def local(x_blocks, columns, filter_ids):
    grid_a, grid_c, _ = columns.shape
    table, level = list_tables(columns, filter_ids)
    branches = [
        functools.partial(lambda at, x, c, f, t: sparse(at, grid_a, grid_c, x, t), at)
        for at in range(len(LEVELS))
    ]
    branches.append(lambda x, c, f, t: dense(x, c, f))
    return lax.switch(level[0], branches, x_blocks, columns, filter_ids, table)


def solution(mesh):
    return jax.shard_map(
        local,
        mesh=mesh,
        in_specs=(P("grp", "col", None, None, None), P(), P()),
        out_specs=P("grp", "col", None, None, None),
        check_vma=False,
    )
```

```python
import functools

import jax
import jax.numpy as jnp
from jax import lax
from jax.experimental import pallas as pl
from jax.experimental.pallas import tpu as pltpu
from jax.sharding import PartitionSpec as P

B = 256
KB = 6
KF = 6
RA = 4
OWN = RA * KB
CR = 2 * RA + 2
COLN = CR * KB
ZERO = COLN
FIRST = 5
RELAY = 4
LEVELS = ((11, 13), (11, 14), (12, 13), (12, 14), (12, 15), (13, 16), (15, 19))

PICKS = OWN * KB
MESH = pl.DeviceIdType.MESH


def padded(cells, sides, width):
    for axis, dim in sides:
        count = lax.axis_size(axis)
        head = lax.slice_in_dim(cells, 0, width, axis=dim)
        tail = lax.slice_in_dim(cells, cells.shape[dim] - width, cells.shape[dim], axis=dim)
        cells = jnp.concatenate(
            [
                lax.ppermute(tail, axis, [(i, (i + 1) % count) for i in range(count)]),
                cells,
                lax.ppermute(head, axis, [((i + 1) % count, i) for i in range(count)]),
            ],
            axis=dim,
        )
    return cells


def block_terms(
    halo, pos_a, pos_c, row_ids, row_cols, left_blocks, stored_table, wanted, grid_a, grid_c
):
    slot_count = halo.shape[2]
    width = halo.shape[3]
    in_use = row_cols >= 0
    source = jnp.where(in_use, row_cols, 0)
    home_a = row_ids // grid_c
    home_c = row_ids % grid_c
    step_a = (source // grid_c - home_a[:, None] + 1) % grid_a - 1
    step_c = (source % grid_c - home_c[:, None] + 1) % grid_c - 1
    place = (pos_a[:, None] + step_a) * halo.shape[1] + pos_c[:, None] + step_c
    flat = halo.reshape((halo.shape[0] * halo.shape[1] * slot_count, width, width))
    stored = stored_table[source]
    matches = stored[:, :, None, :] == wanted[:, None, :, None]
    present = jnp.any(matches, axis=3) & (wanted[:, None, :] >= 0) & in_use[:, :, None]
    slot_of = jnp.argmax(matches.astype(jnp.int32), axis=3)
    block_index = place[:, :, None] * slot_count + slot_of

    def one_row(inputs):
        index_row, present_row, left_row = inputs
        picked = flat[index_row]
        picked = jnp.where(present_row[:, :, None, None], picked, jnp.zeros((), picked.dtype))
        return jnp.einsum("kab,kfbc->fac", left_row, picked, preferred_element_type=jnp.float32)

    return lax.map(one_row, (block_index, present, left_blocks))


def dense(x_blocks, columns, filter_ids):
    grp_count = lax.axis_size("grp")
    col_count = lax.axis_size("col")
    rows_a = x_blocks.shape[0]
    rows_c = x_blocks.shape[1]
    grid_a = rows_a * grp_count
    grid_c = rows_c * col_count
    col_table = columns.reshape(grid_a * grid_c, KB)
    filt_table = filter_ids.reshape(grid_a * grid_c, KF)
    local_rows = rows_a * rows_c
    offsets = jnp.arange(local_rows, dtype=jnp.int32)
    local_a = offsets // rows_c
    local_c = offsets % rows_c
    row_ids = (
        (lax.axis_index("grp") * rows_a + local_a) * grid_c
        + lax.axis_index("col") * rows_c
        + local_c
    )
    row_cols = col_table[row_ids]
    left_blocks = x_blocks.reshape(local_rows, KB, B, B)
    along_col = padded(x_blocks, (("col", 1),), 1)
    near_x = padded(along_col, (("grp", 0),), 1)
    square = block_terms(
        near_x,
        local_a + 1,
        local_c + 1,
        row_ids,
        row_cols,
        left_blocks,
        col_table,
        filt_table[row_ids],
        grid_a,
        grid_c,
    ).astype(jnp.bfloat16)
    square = square.reshape(rows_a, rows_c, KF, B, B)
    square_along = padded(square, (("col", 1),), 1)
    near_square = padded(square_along, (("grp", 0),), 1)
    cubed = block_terms(
        near_square,
        local_a + 1,
        local_c + 1,
        row_ids,
        row_cols,
        left_blocks,
        filt_table,
        row_cols,
        grid_a,
        grid_c,
    )
    in_use = (row_cols >= 0).astype(jnp.float32)
    result = (1.5 * left_blocks.astype(jnp.float32) - cubed * (0.5 / (KB * B))) * in_use[
        :, :, None, None
    ]
    return result.astype(jnp.bfloat16).reshape(x_blocks.shape)


LANES = 128
LISTS = 8
CODE_AT = 0
NEAR_AT = 48
SRC_AT = 96
TABLE_ROWS = 16


def index_kernel(cols_ref, filt_ref, table_ref, level_ref, own_ref, halo_ref, move_ref,
                 cols_s, filt_s):
    grp = lax.axis_index("grp")
    col = lax.axis_index("col")
    core = lax.rem(grp, 2)
    grid_c = cols_ref.shape[1]
    grid_a = cols_ref.shape[2]
    chip = 2 * RA

    def lanes_of(x):
        return jnp.concatenate([x] * (LANES // grid_a), axis=1)

    stored, kept = [], []
    for m in range(KB):
        stored.append(lanes_of(cols_ref[m]))
        kept.append(lanes_of(filt_ref[m]))
        cols_s[m] = stored[m]
        filt_s[m] = kept[m]
    shape = (grid_c, LANES)
    lane = lax.broadcasted_iota(jnp.int32, shape, 1)
    ids = lax.rem(lane, grid_a) * grid_c + lax.broadcasted_iota(jnp.int32, shape, 0)
    in_chip = lax.rem(lane, chip)
    first, last = in_chip == 0, in_chip == chip - 1
    false = jnp.zeros(shape, jnp.int32)

    def either(tests):
        got = tests[0]
        for t in tests[1:]:
            got = got | t
        return got

    totals = []
    for d, step_c in enumerate((1, -1)):
        cols_c = [jnp.roll(x, -step_c, 0) for x in stored]
        filt_c = [jnp.roll(x, -step_c, 0) for x in kept]
        found = []
        for step_a in (-1, 0, 1):
            shift = (-step_a) % LANES
            cols_r = [pltpu.roll(x, shift, 1) if shift else x for x in cols_c]
            filt_r = [pltpu.roll(x, shift, 1) if shift else x for x in filt_c]
            member = either([x == ids for x in cols_r])
            one = [either([stored[m] == x for x in filt_r]) & member & (stored[m] >= 0) for m in range(KB)]
            two = [either([kept[m] == x for x in cols_r]) & member for m in range(KB)]
            found.append((one, two))
        up, mid, down = found
        for phase in (0, 1):
            own_row, halo_row = false, false
            flags = []
            for m in range(KB):
                u, c, w = up[phase][m], mid[phase][m], down[phase][m]
                own = (c | (u & ~first) | (w & ~last)).astype(jnp.int32)
                halo = ((u & first) | (w & last)).astype(jnp.int32)
                flags.append((own, halo))
                own_row = own_row + own
                halo_row = halo_row + halo
            totals.append((phase, d, flags, own_row, halo_row))

    def summed(x, rule):
        at = lax.broadcasted_iota(jnp.int32, (LANES, LANES), 0)
        to = lax.broadcasted_iota(jnp.int32, (LANES, LANES), 1)
        weight = rule(at, to).astype(jnp.float32).astype(jnp.bfloat16)
        return jnp.dot(
            x.astype(jnp.float32).astype(jnp.bfloat16), weight, preferred_element_type=jnp.float32
        ).astype(jnp.int32)

    def same_chip(at, to):
        return (at // chip == lax.rem(to, grid_a) // chip) & (at < grid_a)

    def beside(at, to):
        z = lax.rem(to, grid_a) // chip * chip
        above = lax.rem(z + grid_a - 1, grid_a)
        below = lax.rem(z + chip, grid_a)
        return (at == above) | (at == below)

    def stack(xs):
        return jnp.concatenate(xs, axis=0)

    loads = summed(stack([t[3] for t in totals]), same_chip) + summed(
        stack([t[4] for t in totals]), beside
    )

    def across(x):
        return jnp.where(last, pltpu.roll(x, LANES - 1, 1), pltpu.roll(x, 1, 1))

    kept_own, kept_halo, got0, got1 = [], [], [], []
    for p, (phase, d, flags, _, _) in enumerate(totals):
        load = loads[p * grid_c : (p + 1) * grid_c]
        lead = jnp.where(last, load - across(load), across(load) - load)
        far = jnp.abs(lead)
        count = jnp.zeros(shape, jnp.int32)
        for step in range(RELAY):
            count = count + (far >= 3 * step + 2).astype(jnp.int32)
        ups = (lead > 0).astype(jnp.int32)
        rim = (first | last).astype(jnp.int32)
        both = [own * halo * rim for own, halo in flags]
        lower = [jnp.where(last, own, halo) for own, halo in flags]
        upper = [jnp.where(last, halo, own) for own, halo in flags]
        single = [
            jnp.where(ups > 0, lower[m], upper[m]) * rim - both[m] for m in range(KB)
        ]
        n_both = sum(both[1:], both[0])
        n_single = sum(single[1:], single[0])
        both_rank = jnp.where(last, 0, across(n_both))
        single_rank = n_both + across(n_both) + jnp.where(last, 0, across(n_single))
        own_row, halo_row, moved_row = false, false, false
        for m in range(KB):
            rank = jnp.where(both[m] > 0, both_rank, single_rank)
            moved = ((both[m] + single[m]) > 0) & (rank < count)
            move = jnp.where(moved, rank + 1 + 8 * ups, 0)
            both_rank = both_rank + both[m]
            single_rank = single_rank + single[m]
            own = jnp.where(moved, 0, flags[m][0])
            halo = jnp.where(moved, 0, flags[m][1])
            own_ref[phase, d, m] = own
            halo_ref[phase, d, m] = halo
            move_ref[phase, d, m] = move
            own_row, halo_row = own_row + own, halo_row + halo
            moved_row = moved_row + moved.astype(jnp.int32)
        moved_row = moved_row + across(moved_row)
        kept_own.append(own_row)
        kept_halo.append(halo_row)
        got0.append(jnp.where(first, moved_row * ups, 0))
        got1.append(jnp.where(last, moved_row * (1 - ups), 0))

    def split(n0, n1, total, extra0, extra1):
        half = jnp.clip((total + extra1 - extra0 + 1) >> 1, 0, total)
        return half, jnp.maximum(FIRST - n0, 0), jnp.maximum(FIRST - n1, 0)

    own_all = stack(kept_own)
    n0 = summed(own_all, lambda at, to: same_chip(at, to) & (lax.rem(at, chip) < RA))
    n1 = summed(own_all, lambda at, to: same_chip(at, to) & (lax.rem(at, chip) >= RA))
    total = n0 + n1 + summed(stack(kept_halo), beside)
    extra0 = summed(stack(got0), same_chip)
    extra1 = summed(stack(got1), same_chip)
    half, gap0, gap1 = split(n0, n1, total, extra0, extra1)
    rest = total - half
    fill = jnp.maximum(
        half + jnp.where(half > n0, gap0, 0) + extra0,
        rest + jnp.where(rest > n1, gap1, 0) + extra1,
    )
    most = [jnp.int32(FIRST + RELAY), jnp.int32(FIRST + RELAY)]
    for p, (phase, _, _, _, _) in enumerate(totals):
        most[phase] = jnp.maximum(most[phase], jnp.max(fill[p * grid_c : (p + 1) * grid_c]))
    level = jnp.int32(len(LEVELS))
    for at in reversed(range(len(LEVELS))):
        fits = (most[0] <= LEVELS[at][0]) & (most[1] <= LEVELS[at][1])
        level = jnp.where(fits, at, level)
    level_ref[0] = level

    z = grp // 2
    shift = lax.rem(LANES + 1 - z * chip, LANES)
    west = lax.rem(col + grid_c - 1, grid_c)
    east = lax.rem(col + 1, grid_c)
    row8 = (LISTS, LANES)
    lane8 = lax.broadcasted_iota(jnp.int32, row8, 1)
    rim = (lane8 == 0) | (lane8 == CR - 1)
    lists = [(p, d, c) for p in (0, 1) for d, c in ((0, col), (1, col), (0, west), (1, east))]

    def near(ref_rows):
        return pltpu.roll(jnp.concatenate(ref_rows, axis=0), shift, 1)

    need, in_row, stores, moves = [], [], [], []
    run = jnp.zeros(row8, jnp.int32)
    relayed = jnp.zeros(row8, jnp.int32)
    low_end = lane8 <= 1
    for m in range(KB):
        own = near([own_ref[p, d, m, pl.ds(c, 1), :] for p, d, c in lists])
        halo = near([halo_ref[p, d, m, pl.ds(c, 1), :] for p, d, c in lists])
        flags = jnp.where(lane8 < CR, jnp.where(rim, halo, own), 0)
        need.append(flags)
        in_row.append(run)
        run = run + flags
        move = near([move_ref[p, d, m, pl.ds(c, 1), :] for p, d, c in lists])
        move = jnp.where((lane8 <= 1) | ((lane8 >= CR - 2) & (lane8 < CR)), move, 0)
        mine = (move > 0) & ((move > 8) == low_end)
        moves.append((move, mine))
        relayed = relayed + mine.astype(jnp.int32)
        rows = [cols_s[m, pl.ds(c, 1), :] for c in (west, col, east)]
        rows += [filt_s[m, pl.ds(c, 1), :] for c in (west, col, east)]
        stores.append(near(rows + rows[:2]))
    n0 = summed(run, lambda at, to: (at >= 1) & (at <= RA))
    n1 = summed(run, lambda at, to: (at > RA) & (at <= chip))
    above = summed(run, lambda at, to: at == 0)
    below = summed(run, lambda at, to: at == CR - 1)
    ahead = summed(
        run, lambda at, to: (at < to) & (((at >= 1) & (to <= RA)) | ((at > RA) & (to <= chip)))
    )
    total = n0 + n1 + above + below
    extra0 = summed(relayed, lambda at, to: at <= 1)
    extra1 = summed(relayed, lambda at, to: at > 1)
    half, gap0, gap1 = split(n0, n1, total, extra0, extra1)
    east_list = lax.rem(lax.broadcasted_iota(jnp.int32, row8, 0), 4) == 3
    of0 = (lane8 >= 1) & (lane8 <= RA)
    of1 = (lane8 > RA) & (lane8 <= chip)
    slots = lax.broadcasted_iota(jnp.int32, (32, LANES), 0) + core * 32
    entry = lax.broadcasted_iota(jnp.int32, (32, LANES), 1) * KB
    source = [jnp.zeros((32, LANES), jnp.int32) for _ in range(4)]
    codes = []
    for m in range(KB):
        place = ahead + in_row[m]
        place = jnp.where(lane8 == 0, n0 + in_row[m], place)
        place = jnp.where(lane8 == CR - 1, n0 + above + in_row[m], place)
        place = jnp.where(of1, total - 1 - place, place)
        turned = total - 1 - place
        slot0 = place + jnp.where(of0, 0, gap0)
        slot1 = turned + jnp.where(of1, 0, gap1)
        slot0 = slot0 + jnp.where(slot0 >= FIRST, extra0, 0)
        slot1 = slot1 + jnp.where(slot1 >= FIRST, extra1, 0)
        code = jnp.where(place < half, slot0, 32 + slot1)
        move, mine = moves[m]
        rank = (move & 7) - 1
        code = jnp.where(mine, jnp.where(low_end, FIRST, 32 + FIRST) + rank, code)
        code = jnp.where((move > 0) & ~mine, jnp.where(east_list, 96, 128) + rank, code)
        codes.append(code)
        sent = jnp.where((need[m] > 0) | mine, code, -1)
        for i, at in enumerate((0, 1, 4, 5)):
            same = jnp.broadcast_to(sent[at : at + 1], (32, LANES)) == slots
            source[i] = source[i] + jnp.where(same, entry + m, 0)
    lane32 = lax.broadcasted_iota(jnp.int32, (32, LANES), 1)
    out = jnp.zeros((32, LANES), jnp.int32)
    for i in range(4):
        out = jnp.where(lane32 == i, jnp.sum(source[i], axis=1, keepdims=True), out)
    table_ref[...] = jnp.concatenate(codes + stores + [out], axis=0).T[:TABLE_ROWS]


def list_tables(columns, filter_ids):
    grid_a, grid_c, _ = columns.shape
    ints = lambda *shape: pltpu.VMEM(shape, jnp.int32)
    return pl.pallas_call(
        index_kernel,
        out_shape=(
            jax.ShapeDtypeStruct((TABLE_ROWS, LANES), jnp.int32),
            jax.ShapeDtypeStruct((1,), jnp.int32),
        ),
        in_specs=[pl.BlockSpec(memory_space=pltpu.VMEM)] * 2,
        out_specs=(
            pl.BlockSpec(memory_space=pltpu.VMEM),
            pl.BlockSpec(memory_space=pltpu.SMEM),
        ),
        scratch_shapes=[
            ints(2, 2, KB, grid_c, LANES), ints(2, 2, KB, grid_c, LANES),
            ints(2, 2, KB, grid_c, LANES),
            ints(KB, grid_c, LANES), ints(KF, grid_c, LANES),
        ],
        name="block_lists",
    )(columns.transpose(2, 1, 0), filter_ids.transpose(2, 1, 0))


def kernel(q1, q2, grid_a, grid_c, grp_count, col_count, tab, x_hbm, out_ref, pick, xv, colp1, rcv1, snd1, colp2, rcv2,
           snd2, sown, lsem, zsem, hs1, hr1, fs1, fr1, hs2, hr2, fs2, fr2, ysem):
    grp = lax.axis_index("grp")
    col = lax.axis_index("col")
    core = lax.rem(grp, 2)
    partner = (grp + 1 - 2 * core, col)
    zpeer = (lax.rem(grp + grp_count - 1 + 2 * core, grp_count), col)
    right = (grp, lax.rem(col + 1, col_count))
    left = (grp, lax.rem(col + col_count - 1, col_count))
    own0 = (1 + RA * core) * KB
    zout = (RA - 1) * core * KB
    zdst = (CR - 1) * (1 - core) * KB
    zin = (CR - 1) * core * KB

    to_xv = pltpu.make_async_copy(x_hbm, xv, lsem.at[0])
    to_col = pltpu.make_async_copy(x_hbm, colp1.at[pl.ds(own0, OWN)], lsem.at[1])
    to_xv.start()

    barrier = pltpu.get_barrier_semaphore()
    for peer in (partner, zpeer, right, left):
        pl.semaphore_signal(barrier, inc=1, device_id=peer, device_id_type=MESH)
    pl.semaphore_wait(barrier, 4)

    def remote(src, dst, send, recv, device):
        return pltpu.make_async_remote_copy(
            src_ref=src, dst_ref=dst, send_sem=send, recv_sem=recv,
            device_id=device, device_id_type=MESH,
        )

    def zsend(src, colp, p):
        return remote(src.at[pl.ds(zout, KB)], colp.at[pl.ds(zdst, KB)],
                      zsem.at[p, 0], zsem.at[p, 1], zpeer)

    def zfwd(colp, p):
        here = colp.at[pl.ds(zin, KB)]
        return remote(here, here, zsem.at[p, 2], zsem.at[p, 3], partner)

    def share(src, colp, p):
        return remote(src, colp.at[pl.ds(own0, OWN)], zsem.at[p, 4], zsem.at[p, 5], partner)

    def hop(snd, rcv, hs, hr, q, d, s):
        return remote(snd.at[d, s], rcv.at[(2 * d + core) * q + s], hs, hr.at[s],
                      (right, left)[d])

    def fwd(rcv, fs, fr, q, d, s):
        here = rcv.at[(2 * d + core) * q + s]
        return remote(here, here, fs, fr, partner)

    def relay(rcv, p, q, d, s):
        rank = s - FIRST
        return remote(rcv.at[(2 * d + core) * q + s], rcv.at[4 * q + d * RELAY + rank],
                      ysem.at[p, 0], ysem.at[p, 1], zpeer)

    def wait_all(like, sem):
        pltpu.make_async_copy(like, like, sem).wait()

    def right_factor(colp, rcv, q, v):
        is_col = v < 64
        at_col = jnp.where(is_col, v, ZERO)
        at_rcv = jnp.where(is_col, 0, v - 64)
        part = at_rcv >> 5
        slot = at_rcv & 31
        direct = jnp.minimum(part, 3) * q + jnp.minimum(slot, q - 1)
        passed = 4 * q + jnp.clip((part - 4) * RELAY + slot, 0, 2 * RELAY - 1)
        return jnp.where(is_col, colp[at_col], rcv[jnp.where(part < 4, direct, passed)])

    def product(colp, rcv, phase, row, entry):
        acc = None
        for k in range(KB):
            v = pick[phase * PICKS + entry * KB + k]
            term = jnp.dot(xv[row * KB + k], right_factor(colp, rcv, (q1, q2)[phase], v),
                           preferred_element_type=jnp.float32)
            acc = term if acc is None else acc + term
        return acc

    def sent(phase, d, s):
        return tab[2 * phase + d, SRC_AT + s]

    def list_entry(phase, d, s):
        return jnp.clip(sent(phase, d, s) - own0, 0, OWN - 1)

    def find_factors(at):
        row = at // KB
        k = at - KB * row
        here = 1 + RA * core + row
        source = tab[here, NEAR_AT + 8 * k + 1]
        in_use = source >= 0
        source = jnp.where(in_use, source, 0)
        step_a = lax.rem(source // grid_c - (grp * RA + row) + 1 + grid_a, grid_a) - 1
        side = lax.rem(lax.rem(source, grid_c) - col + 1 + grid_c, grid_c)
        step_a = jnp.where(in_use, jnp.clip(step_a, -1, 1), 0)
        side = jnp.where(in_use, jnp.minimum(side, 2), 1)
        there = here + step_a
        for phase in range(2):
            held, spot = [], []
            for m in range(KB):
                held.append(tab[there, NEAR_AT + 8 * m + side + 3 * phase])
                code = tab[there, CODE_AT + 8 * m + 4 * phase + jnp.where(side == 0, 2, 3)]
                far = code + jnp.where(side == 0, 64, 128)
                spot.append(jnp.where(side == 1, there * KB + m, far))
            for f in range(KF):
                wanted = tab[here, NEAR_AT + 8 * f + 1 + 3 * (1 - phase)]
                usable = in_use & (wanted >= 0)
                got = jnp.int32(ZERO)
                for m in range(KB):
                    got = jnp.where(held[m] == wanted, spot[m], got)
                pick[phase * PICKS + (row * KB + f) * KB + k] = jnp.where(usable, got, ZERO)

    zero = jnp.zeros((B, B), jnp.bfloat16)

    zs1, zf1, sh1 = zsend(xv, colp1, 0), zfwd(colp1, 0), share(xv, colp1, 0)
    to_xv.wait()
    zs1.start()
    to_col.start()
    sh1.start()
    hop1 = functools.partial(hop, snd1, rcv1, hs1, hr1, q1)
    fwd1 = functools.partial(fwd, rcv1, fs1, fr1, q1)
    pass1 = functools.partial(relay, rcv1, 0, q1)

    @pl.loop(0, FIRST)
    def _(s):
        for d in range(2):
            snd1[d, s] = xv[list_entry(0, d, s)]

        @pl.when(s > 0)
        def _():
            for d in range(2):
                hop1(d, s - 1).start()

    colp1[ZERO] = zero
    colp2[ZERO] = zero
    for d in range(2):
        hop1(d, FIRST - 1).start()
    to_col.wait()
    zs1.wait_recv()
    zf1.start()
    sh1.wait_recv()
    zf1.wait_recv()

    @pl.loop(FIRST, q1)
    def _(s):
        for d in range(2):
            snd1[d, s] = colp1[sent(0, d, s)]

        @pl.when(s > FIRST)
        def _():
            for d in range(2):
                hop1(d, s - 1).start()

    for d in range(2):
        hop1(d, q1 - 1).start()

    pl.loop(0, OWN)(find_factors)

    @pl.loop(0, q1)
    def _(s):
        wait_all(rcv1.at[pl.ds(0, 2)], hr1.at[s])
        for d in range(2):
            fwd1(d, s).start()

        @pl.when((s >= FIRST) & (s < FIRST + RELAY))
        def _():
            for d in range(2):
                pass1(d, s).start()

    wait_all(snd1, fr1)
    wait_all(rcv1.at[pl.ds(0, 2 * RELAY)], ysem.at[0, 1])

    zs2, zf2, sh2 = zsend(sown, colp2, 1), zfwd(colp2, 1), share(sown, colp2, 1)
    hop2 = functools.partial(hop, snd2, rcv2, hs2, hr2, q2)
    fwd2 = functools.partial(fwd, rcv2, fs2, fr2, q2)
    pass2 = functools.partial(relay, rcv2, 1, q2)

    @pl.loop(0, 2)
    def _(s):
        for d in range(2):
            entry = list_entry(1, d, s)
            snd2[d, s] = product(colp1, rcv1, 0, entry // KB, entry).astype(jnp.bfloat16)
        hop2(0, s).start()

        @pl.when(s > 0)
        def _():
            hop2(1, s - 1).start()

    @pl.loop(0, OWN // 2)
    def _(t):
        step = t // 3
        row = step + core * (RA - 1 - 2 * step)
        for u in range(2):
            entry = row * KB + (t - 3 * step) * 2 + u
            block = product(colp1, rcv1, 0, row, entry).astype(jnp.bfloat16)
            sown[entry] = block
            colp2[own0 + entry] = block

        @pl.when(t == 0)
        def _():
            hop2(1, 1).start()

        @pl.when(t == 3)
        def _():
            zs2.start()

    @pl.loop(2, FIRST)
    def _(s):
        for d in range(2):
            snd2[d, s] = sown[list_entry(1, d, s)]

        @pl.when(s > 2)
        def _():
            for d in range(2):
                hop2(d, s - 1).start()

    sh2.start()
    for d in range(2):
        hop2(d, FIRST - 1).start()
    zs2.wait_recv()
    zf2.start()
    sh2.wait_recv()
    zf2.wait_recv()

    @pl.loop(FIRST, q2)
    def _(s):
        for d in range(2):
            snd2[d, s] = colp2[sent(1, d, s)]

        @pl.when(s > FIRST)
        def _():
            for d in range(2):
                hop2(d, s - 1).start()

    for d in range(2):
        hop2(d, q2 - 1).start()

    @pl.loop(0, q2)
    def _(s):
        wait_all(rcv2.at[pl.ds(0, 2)], hr2.at[s])
        for d in range(2):
            fwd2(d, s).start()

        @pl.when((s >= FIRST) & (s < FIRST + RELAY))
        def _():
            for d in range(2):
                pass2(d, s).start()

    wait_all(snd2, fr2)
    wait_all(rcv2.at[pl.ds(0, 2 * RELAY)], ysem.at[1, 1])

    @pl.loop(0, OWN // 2)
    def _(t):
        row = t // 3
        for u in range(2):
            entry = 2 * t + u
            cubed = product(colp2, rcv2, 1, row, entry)
            in_use = tab[1 + RA * core + row, NEAR_AT + 8 * (entry - row * KB) + 1] >= 0
            own = xv[entry].astype(jnp.float32)
            step = 1.5 * own - cubed * (0.5 / (KB * B))
            out_ref[entry] = jnp.where(in_use, step, 0.0).astype(jnp.bfloat16)

    zs1.wait_send()
    zf1.wait_send()
    sh1.wait_send()
    zs2.wait_send()
    zf2.wait_send()
    sh2.wait_send()
    for snd, rcv, hs, fs, p in ((snd1, rcv1, hs1, fs1, 0), (snd2, rcv2, hs2, fs2, 1)):
        wait_all(snd, hs)
        wait_all(snd, fs)
        wait_all(rcv.at[pl.ds(0, 2 * RELAY)], ysem.at[p, 0])


def sparse(level, grid_a, grid_c, x_blocks, table):
    q1, q2 = LEVELS[level]
    blocks = x_blocks.reshape(OWN, B, B)
    vm = lambda *lead: pltpu.VMEM((*lead, B, B), jnp.bfloat16)
    dma = lambda *lead: pltpu.SemaphoreType.DMA(lead)
    out = pl.pallas_call(
        functools.partial(kernel, q1, q2, grid_a, grid_c, lax.axis_size("grp"), lax.axis_size("col")),
        out_shape=pltpu.VMEM(blocks.shape, jnp.bfloat16),
        in_specs=[
            pl.BlockSpec(memory_space=pltpu.SMEM),
            pl.BlockSpec(memory_space=pl.ANY),
        ],
        out_specs=pl.BlockSpec(memory_space=pltpu.VMEM),
        scratch_shapes=[
            pltpu.SMEM((2 * PICKS,), jnp.int32),
            vm(OWN), vm(COLN + 1), vm(4 * q1 + 2 * RELAY), vm(2, q1), vm(COLN + 1),
            vm(4 * q2 + 2 * RELAY), vm(2, q2),
            vm(OWN),
            dma(2), dma(2, 6),
            dma(), dma(q1), dma(), dma(), dma(), dma(q2), dma(), dma(), dma(2, 2),
        ],
        compiler_params=pltpu.CompilerParams(
            collective_id=level, has_side_effects=True, vmem_limit_bytes=58 * 1024 * 1024
        ),
        name=f"sign_step_{q1}_{q2}",
    )(table, blocks)
    return written(out).reshape(x_blocks.shape)


def written(blocks):
    def copy(src, dst, sem):
        move = pltpu.make_async_copy(src, dst, sem)
        move.start()
        move.wait()

    return pl.pallas_call(
        copy,
        out_shape=jax.ShapeDtypeStruct(blocks.shape, blocks.dtype),
        in_specs=[pl.BlockSpec(memory_space=pltpu.VMEM)],
        out_specs=pl.BlockSpec(memory_space=pl.ANY),
        scratch_shapes=[pltpu.SemaphoreType.DMA(())],
        compiler_params=pltpu.CompilerParams(vmem_limit_bytes=4 * 1024 * 1024),
        name="write_out",
    )(blocks)


def local(x_blocks, columns, filter_ids):
    grid_a, grid_c, _ = columns.shape
    table, level = list_tables(columns, filter_ids)
    branches = [
        functools.partial(lambda at, x, c, f, t: sparse(at, grid_a, grid_c, x, t), at)
        for at in range(len(LEVELS))
    ]
    branches.append(lambda x, c, f, t: dense(x, c, f))
    return lax.switch(level[0], branches, x_blocks, columns, filter_ids, table)


def solution(mesh):
    return jax.shard_map(
        local,
        mesh=mesh,
        in_specs=(P("grp", "col", None, None, None), P(), P()),
        out_specs=P("grp", "col", None, None, None),
        check_vma=False,
    )
```

```python
import functools

import jax
import jax.numpy as jnp
from jax import lax
from jax.experimental import pallas as pl
from jax.experimental.pallas import tpu as pltpu
from jax.sharding import PartitionSpec as P

B = 256
KB = 6
KF = 6
RA = 4
OWN = RA * KB
CR = 2 * RA + 2
COLN = CR * KB
ZERO = COLN
FIRST = 5
LATE = 2
RELAY = 4
LEVELS = ((11, 13), (11, 14), (12, 14), (12, 15), (13, 16), (15, 18))

PICKS = OWN * KB
MESH = pl.DeviceIdType.MESH


def padded(cells, sides, width):
    for axis, dim in sides:
        count = lax.axis_size(axis)
        head = lax.slice_in_dim(cells, 0, width, axis=dim)
        tail = lax.slice_in_dim(cells, cells.shape[dim] - width, cells.shape[dim], axis=dim)
        cells = jnp.concatenate(
            [
                lax.ppermute(tail, axis, [(i, (i + 1) % count) for i in range(count)]),
                cells,
                lax.ppermute(head, axis, [((i + 1) % count, i) for i in range(count)]),
            ],
            axis=dim,
        )
    return cells


def block_terms(
    halo, pos_a, pos_c, row_ids, row_cols, left_blocks, stored_table, wanted, grid_a, grid_c
):
    slot_count = halo.shape[2]
    width = halo.shape[3]
    in_use = row_cols >= 0
    source = jnp.where(in_use, row_cols, 0)
    home_a = row_ids // grid_c
    home_c = row_ids % grid_c
    step_a = (source // grid_c - home_a[:, None] + 1) % grid_a - 1
    step_c = (source % grid_c - home_c[:, None] + 1) % grid_c - 1
    place = (pos_a[:, None] + step_a) * halo.shape[1] + pos_c[:, None] + step_c
    flat = halo.reshape((halo.shape[0] * halo.shape[1] * slot_count, width, width))
    stored = stored_table[source]
    matches = stored[:, :, None, :] == wanted[:, None, :, None]
    present = jnp.any(matches, axis=3) & (wanted[:, None, :] >= 0) & in_use[:, :, None]
    slot_of = jnp.argmax(matches.astype(jnp.int32), axis=3)
    block_index = place[:, :, None] * slot_count + slot_of

    def one_row(inputs):
        index_row, present_row, left_row = inputs
        picked = flat[index_row]
        picked = jnp.where(present_row[:, :, None, None], picked, jnp.zeros((), picked.dtype))
        return jnp.einsum("kab,kfbc->fac", left_row, picked, preferred_element_type=jnp.float32)

    return lax.map(one_row, (block_index, present, left_blocks))


def dense(x_blocks, columns, filter_ids):
    grp_count = lax.axis_size("grp")
    col_count = lax.axis_size("col")
    rows_a = x_blocks.shape[0]
    rows_c = x_blocks.shape[1]
    grid_a = rows_a * grp_count
    grid_c = rows_c * col_count
    col_table = columns.reshape(grid_a * grid_c, KB)
    filt_table = filter_ids.reshape(grid_a * grid_c, KF)
    local_rows = rows_a * rows_c
    offsets = jnp.arange(local_rows, dtype=jnp.int32)
    local_a = offsets // rows_c
    local_c = offsets % rows_c
    row_ids = (
        (lax.axis_index("grp") * rows_a + local_a) * grid_c
        + lax.axis_index("col") * rows_c
        + local_c
    )
    row_cols = col_table[row_ids]
    left_blocks = x_blocks.reshape(local_rows, KB, B, B)
    along_col = padded(x_blocks, (("col", 1),), 1)
    near_x = padded(along_col, (("grp", 0),), 1)
    square = block_terms(
        near_x,
        local_a + 1,
        local_c + 1,
        row_ids,
        row_cols,
        left_blocks,
        col_table,
        filt_table[row_ids],
        grid_a,
        grid_c,
    ).astype(jnp.bfloat16)
    square = square.reshape(rows_a, rows_c, KF, B, B)
    square_along = padded(square, (("col", 1),), 1)
    near_square = padded(square_along, (("grp", 0),), 1)
    cubed = block_terms(
        near_square,
        local_a + 1,
        local_c + 1,
        row_ids,
        row_cols,
        left_blocks,
        filt_table,
        row_cols,
        grid_a,
        grid_c,
    )
    in_use = (row_cols >= 0).astype(jnp.float32)
    result = (1.5 * left_blocks.astype(jnp.float32) - cubed * (0.5 / (KB * B))) * in_use[
        :, :, None, None
    ]
    return result.astype(jnp.bfloat16).reshape(x_blocks.shape)


LANES = 128
LISTS = 8
CODE_AT = 0
NEAR_AT = 48
SRC_AT = 96
TABLE_ROWS = 16


def index_kernel(cols_ref, filt_ref, table_ref, level_ref, own_ref, halo_ref, move_ref,
                 cols_s, filt_s):
    grp = lax.axis_index("grp")
    col = lax.axis_index("col")
    core = lax.rem(grp, 2)
    grid_c = cols_ref.shape[1]
    grid_a = cols_ref.shape[2]
    chip = 2 * RA

    def lanes_of(x):
        return jnp.concatenate([x] * (LANES // grid_a), axis=1)

    stored, kept = [], []
    for m in range(KB):
        stored.append(lanes_of(cols_ref[m]))
        kept.append(lanes_of(filt_ref[m]))
        cols_s[m] = stored[m]
        filt_s[m] = kept[m]
    shape = (grid_c, LANES)
    lane = lax.broadcasted_iota(jnp.int32, shape, 1)
    ids = lax.rem(lane, grid_a) * grid_c + lax.broadcasted_iota(jnp.int32, shape, 0)
    in_chip = lax.rem(lane, chip)
    first, last = in_chip == 0, in_chip == chip - 1
    false = jnp.zeros(shape, jnp.int32)

    def either(tests):
        got = tests[0]
        for t in tests[1:]:
            got = got | t
        return got

    totals = []
    for d, step_c in enumerate((1, -1)):
        cols_c = [jnp.roll(x, -step_c, 0) for x in stored]
        filt_c = [jnp.roll(x, -step_c, 0) for x in kept]
        found = []
        for step_a in (-1, 0, 1):
            shift = (-step_a) % LANES
            cols_r = [pltpu.roll(x, shift, 1) if shift else x for x in cols_c]
            filt_r = [pltpu.roll(x, shift, 1) if shift else x for x in filt_c]
            member = either([x == ids for x in cols_r])
            one = [either([stored[m] == x for x in filt_r]) & member & (stored[m] >= 0) for m in range(KB)]
            two = [either([kept[m] == x for x in cols_r]) & member for m in range(KB)]
            found.append((one, two))
        up, mid, down = found
        for phase in (0, 1):
            own_row, halo_row = false, false
            flags = []
            for m in range(KB):
                u, c, w = up[phase][m], mid[phase][m], down[phase][m]
                own = (c | (u & ~first) | (w & ~last)).astype(jnp.int32)
                halo = ((u & first) | (w & last)).astype(jnp.int32)
                flags.append((own, halo))
                own_row = own_row + own
                halo_row = halo_row + halo
            totals.append((phase, d, flags, own_row, halo_row))

    def summed(x, rule):
        at = lax.broadcasted_iota(jnp.int32, (LANES, LANES), 0)
        to = lax.broadcasted_iota(jnp.int32, (LANES, LANES), 1)
        weight = rule(at, to).astype(jnp.float32).astype(jnp.bfloat16)
        return jnp.dot(
            x.astype(jnp.float32).astype(jnp.bfloat16), weight, preferred_element_type=jnp.float32
        ).astype(jnp.int32)

    def same_chip(at, to):
        return (at // chip == lax.rem(to, grid_a) // chip) & (at < grid_a)

    def beside(at, to):
        z = lax.rem(to, grid_a) // chip * chip
        above = lax.rem(z + grid_a - 1, grid_a)
        below = lax.rem(z + chip, grid_a)
        return (at == above) | (at == below)

    def stack(xs):
        return jnp.concatenate(xs, axis=0)

    loads = summed(stack([t[3] for t in totals]), same_chip) + summed(
        stack([t[4] for t in totals]), beside
    )

    def across(x):
        return jnp.where(last, pltpu.roll(x, LANES - 1, 1), pltpu.roll(x, 1, 1))

    kept_own, kept_halo, got0, got1 = [], [], [], []
    for p, (phase, d, flags, _, _) in enumerate(totals):
        load = loads[p * grid_c : (p + 1) * grid_c]
        lead = jnp.where(last, load - across(load), across(load) - load)
        far = jnp.abs(lead)
        count = jnp.zeros(shape, jnp.int32)
        for step in range(RELAY):
            count = count + (far >= 3 * step + 2).astype(jnp.int32)
        ups = (lead > 0).astype(jnp.int32)
        rim = (first | last).astype(jnp.int32)
        both = [own * halo * rim for own, halo in flags]
        lower = [jnp.where(last, own, halo) for own, halo in flags]
        upper = [jnp.where(last, halo, own) for own, halo in flags]
        single = [
            jnp.where(ups > 0, lower[m], upper[m]) * rim - both[m] for m in range(KB)
        ]
        n_both = sum(both[1:], both[0])
        n_single = sum(single[1:], single[0])
        both_rank = jnp.where(last, 0, across(n_both))
        single_rank = n_both + across(n_both) + jnp.where(last, 0, across(n_single))
        own_row, halo_row, moved_row = false, false, false
        for m in range(KB):
            rank = jnp.where(both[m] > 0, both_rank, single_rank)
            moved = ((both[m] + single[m]) > 0) & (rank < count)
            move = jnp.where(moved, rank + 1 + 8 * ups, 0)
            both_rank = both_rank + both[m]
            single_rank = single_rank + single[m]
            own = jnp.where(moved, 0, flags[m][0])
            halo = jnp.where(moved, 0, flags[m][1])
            own_ref[phase, d, m] = own
            halo_ref[phase, d, m] = halo
            move_ref[phase, d, m] = move
            own_row, halo_row = own_row + own, halo_row + halo
            moved_row = moved_row + moved.astype(jnp.int32)
        moved_row = moved_row + across(moved_row)
        kept_own.append(own_row)
        kept_halo.append(halo_row)
        got0.append(jnp.where(first, moved_row * ups, 0))
        got1.append(jnp.where(last, moved_row * (1 - ups), 0))

    def split(n0, n1, total, extra0, extra1):
        half = jnp.clip((total + extra1 - extra0 + 1) >> 1, 0, total)
        return half, jnp.maximum(FIRST - n0, 0), jnp.maximum(FIRST - n1, 0)

    own_all = stack(kept_own)
    n0 = summed(own_all, lambda at, to: same_chip(at, to) & (lax.rem(at, chip) < RA))
    n1 = summed(own_all, lambda at, to: same_chip(at, to) & (lax.rem(at, chip) >= RA))
    total = n0 + n1 + summed(stack(kept_halo), beside)
    extra0 = summed(stack(got0), same_chip)
    extra1 = summed(stack(got1), same_chip)
    half, gap0, gap1 = split(n0, n1, total, extra0, extra1)
    rest = total - half
    fill = jnp.maximum(
        half + jnp.where(half > n0, gap0, 0) + extra0,
        rest + jnp.where(rest > n1, gap1, 0) + extra1,
    )
    most = [jnp.int32(FIRST + RELAY), jnp.int32(FIRST + RELAY)]
    for p, (phase, _, _, _, _) in enumerate(totals):
        most[phase] = jnp.maximum(most[phase], jnp.max(fill[p * grid_c : (p + 1) * grid_c]))
    level = jnp.int32(len(LEVELS))
    for at in reversed(range(len(LEVELS))):
        fits = (most[0] <= LEVELS[at][0]) & (most[1] <= LEVELS[at][1])
        level = jnp.where(fits, at, level)
    level_ref[0] = level

    z = grp // 2
    shift = lax.rem(LANES + 1 - z * chip, LANES)
    west = lax.rem(col + grid_c - 1, grid_c)
    east = lax.rem(col + 1, grid_c)
    row8 = (LISTS, LANES)
    lane8 = lax.broadcasted_iota(jnp.int32, row8, 1)
    rim = (lane8 == 0) | (lane8 == CR - 1)
    lists = [(p, d, c) for p in (0, 1) for d, c in ((0, col), (1, col), (0, west), (1, east))]

    def near(ref_rows):
        return pltpu.roll(jnp.concatenate(ref_rows, axis=0), shift, 1)

    need, in_row, stores, moves = [], [], [], []
    run = jnp.zeros(row8, jnp.int32)
    relayed = jnp.zeros(row8, jnp.int32)
    low_end = lane8 <= 1
    for m in range(KB):
        own = near([own_ref[p, d, m, pl.ds(c, 1), :] for p, d, c in lists])
        halo = near([halo_ref[p, d, m, pl.ds(c, 1), :] for p, d, c in lists])
        flags = jnp.where(lane8 < CR, jnp.where(rim, halo, own), 0)
        need.append(flags)
        in_row.append(run)
        run = run + flags
        move = near([move_ref[p, d, m, pl.ds(c, 1), :] for p, d, c in lists])
        move = jnp.where((lane8 <= 1) | ((lane8 >= CR - 2) & (lane8 < CR)), move, 0)
        mine = (move > 0) & ((move > 8) == low_end)
        moves.append((move, mine))
        relayed = relayed + mine.astype(jnp.int32)
        rows = [cols_s[m, pl.ds(c, 1), :] for c in (west, col, east)]
        rows += [filt_s[m, pl.ds(c, 1), :] for c in (west, col, east)]
        stores.append(near(rows + rows[:2]))
    n0 = summed(run, lambda at, to: (at >= 1) & (at <= RA))
    n1 = summed(run, lambda at, to: (at > RA) & (at <= chip))
    above = summed(run, lambda at, to: at == 0)
    below = summed(run, lambda at, to: at == CR - 1)
    ahead = summed(
        run, lambda at, to: (at < to) & (((at >= 1) & (to <= RA)) | ((at > RA) & (to <= chip)))
    )
    total = n0 + n1 + above + below
    extra0 = summed(relayed, lambda at, to: at <= 1)
    extra1 = summed(relayed, lambda at, to: at > 1)
    half, gap0, gap1 = split(n0, n1, total, extra0, extra1)
    east_list = lax.rem(lax.broadcasted_iota(jnp.int32, row8, 0), 4) == 3
    of0 = (lane8 >= 1) & (lane8 <= RA)
    of1 = (lane8 > RA) & (lane8 <= chip)
    slots = lax.broadcasted_iota(jnp.int32, (32, LANES), 0) + core * 32
    entry = lax.broadcasted_iota(jnp.int32, (32, LANES), 1) * KB
    source = [jnp.zeros((32, LANES), jnp.int32) for _ in range(4)]
    codes = []
    for m in range(KB):
        place = ahead + in_row[m]
        place = jnp.where(lane8 == 0, n0 + in_row[m], place)
        place = jnp.where(lane8 == CR - 1, n0 + above + in_row[m], place)
        place = jnp.where(of1, total - 1 - place, place)
        turned = total - 1 - place
        slot0 = place + jnp.where(of0, 0, gap0)
        slot1 = turned + jnp.where(of1, 0, gap1)
        slot0 = slot0 + jnp.where(slot0 >= FIRST, extra0, 0)
        slot1 = slot1 + jnp.where(slot1 >= FIRST, extra1, 0)
        code = jnp.where(place < half, slot0, 32 + slot1)
        move, mine = moves[m]
        rank = (move & 7) - 1
        code = jnp.where(mine, jnp.where(low_end, FIRST, 32 + FIRST) + rank, code)
        code = jnp.where((move > 0) & ~mine, jnp.where(east_list, 96, 128) + rank, code)
        codes.append(code)
        sent = jnp.where((need[m] > 0) | mine, code, -1)
        for i, at in enumerate((0, 1, 4, 5)):
            same = jnp.broadcast_to(sent[at : at + 1], (32, LANES)) == slots
            source[i] = source[i] + jnp.where(same, entry + m, 0)
    lane32 = lax.broadcasted_iota(jnp.int32, (32, LANES), 1)
    out = jnp.zeros((32, LANES), jnp.int32)
    for i in range(4):
        out = jnp.where(lane32 == i, jnp.sum(source[i], axis=1, keepdims=True), out)
    table_ref[...] = jnp.concatenate(codes + stores + [out], axis=0).T[:TABLE_ROWS]


def list_tables(columns, filter_ids):
    grid_a, grid_c, _ = columns.shape
    ints = lambda *shape: pltpu.VMEM(shape, jnp.int32)
    return pl.pallas_call(
        index_kernel,
        out_shape=(
            jax.ShapeDtypeStruct((TABLE_ROWS, LANES), jnp.int32),
            jax.ShapeDtypeStruct((1,), jnp.int32),
        ),
        in_specs=[pl.BlockSpec(memory_space=pltpu.VMEM)] * 2,
        out_specs=(
            pl.BlockSpec(memory_space=pltpu.VMEM),
            pl.BlockSpec(memory_space=pltpu.SMEM),
        ),
        scratch_shapes=[
            ints(2, 2, KB, grid_c, LANES), ints(2, 2, KB, grid_c, LANES),
            ints(2, 2, KB, grid_c, LANES),
            ints(KB, grid_c, LANES), ints(KF, grid_c, LANES),
        ],
        name="block_lists",
    )(columns.transpose(2, 1, 0), filter_ids.transpose(2, 1, 0))


def kernel(q1, q2, grid_a, grid_c, grp_count, col_count, tab, x_hbm, out_ref, acc_ref, late, xv, todo, pick, colp1, rcv1, snd1, colp2, rcv2,
           snd2, sown, lsem, zsem, hs1, hr1, fs1, fr1, hs2, hr2, fs2, fr2, lr2, ysem):
    grp = lax.axis_index("grp")
    col = lax.axis_index("col")
    core = lax.rem(grp, 2)
    partner = (grp + 1 - 2 * core, col)
    zpeer = (lax.rem(grp + grp_count - 1 + 2 * core, grp_count), col)
    right = (grp, lax.rem(col + 1, col_count))
    left = (grp, lax.rem(col + col_count - 1, col_count))
    own0 = (1 + RA * core) * KB
    zout = (RA - 1) * core * KB
    zdst = (CR - 1) * (1 - core) * KB
    zin = (CR - 1) * core * KB

    to_xv = pltpu.make_async_copy(x_hbm, xv, lsem.at[0])
    to_col = pltpu.make_async_copy(x_hbm, colp1.at[pl.ds(own0, OWN)], lsem.at[1])
    to_xv.start()

    barrier = pltpu.get_barrier_semaphore()
    for peer in (partner, zpeer, right, left):
        pl.semaphore_signal(barrier, inc=1, device_id=peer, device_id_type=MESH)
    pl.semaphore_wait(barrier, 4)

    def remote(src, dst, send, recv, device):
        return pltpu.make_async_remote_copy(
            src_ref=src, dst_ref=dst, send_sem=send, recv_sem=recv,
            device_id=device, device_id_type=MESH,
        )

    def zsend(src, colp, p):
        return remote(src.at[pl.ds(zout, KB)], colp.at[pl.ds(zdst, KB)],
                      zsem.at[p, 0], zsem.at[p, 1], zpeer)

    def zfwd(colp, p):
        here = colp.at[pl.ds(zin, KB)]
        return remote(here, here, zsem.at[p, 2], zsem.at[p, 3], partner)

    def share(src, colp, p):
        return remote(src, colp.at[pl.ds(own0, OWN)], zsem.at[p, 4], zsem.at[p, 5], partner)

    def hop(snd, rcv, hs, hr, q, d, s):
        return remote(snd.at[d, s], rcv.at[(2 * d + core) * q + s], hs, hr.at[s],
                      (right, left)[d])

    def fwd(rcv, fs, fr, q, d, s):
        here = rcv.at[(2 * d + core) * q + s]
        return remote(here, here, fs, fr, partner)

    def late_hop(d, i):
        s = q2 - LATE + i
        return remote(snd2.at[d, s], late.at[(2 * d + core) * LATE + i], hs2, hr2.at[s],
                      (right, left)[d])

    def late_fwd(d, i):
        here = late.at[(2 * d + core) * LATE + i]
        return remote(here, here, fs2, lr2, partner)

    def relay(rcv, p, q, d, s):
        rank = s - FIRST
        return remote(rcv.at[(2 * d + core) * q + s], rcv.at[4 * q + d * RELAY + rank],
                      ysem.at[p, 0], ysem.at[p, 1], zpeer)

    def wait_all(like, sem):
        pltpu.make_async_copy(like, like, sem).wait()

    def right_factor(colp, rcv, q, v):
        is_col = v < 64
        at_col = jnp.where(is_col, v, ZERO)
        at_rcv = jnp.where(is_col, 0, v - 64)
        part = at_rcv >> 5
        slot = at_rcv & 31
        direct = jnp.minimum(part, 3) * q + jnp.minimum(slot, q - 1)
        passed = 4 * q + jnp.clip((part - 4) * RELAY + slot, 0, 2 * RELAY - 1)
        return jnp.where(is_col, colp[at_col], rcv[jnp.where(part < 4, direct, passed)])

    def product(colp, rcv, phase, row, entry):
        acc = None
        for k in range(KB):
            v = pick[phase * PICKS + entry * KB + k]
            term = jnp.dot(xv[row * KB + k], right_factor(colp, rcv, (q1, q2 - LATE)[phase], v),
                           preferred_element_type=jnp.float32)
            acc = term if acc is None else acc + term
        return acc

    def sent(phase, d, s):
        return tab[2 * phase + d, SRC_AT + s]

    def list_entry(phase, d, s):
        return jnp.clip(sent(phase, d, s) - own0, 0, OWN - 1)

    def find_factors(at):
        row = at // KB
        k = at - KB * row
        here = 1 + RA * core + row
        source = tab[here, NEAR_AT + 8 * k + 1]
        in_use = source >= 0
        source = jnp.where(in_use, source, 0)
        step_a = lax.rem(source // grid_c - (grp * RA + row) + 1 + grid_a, grid_a) - 1
        side = lax.rem(lax.rem(source, grid_c) - col + 1 + grid_c, grid_c)
        step_a = jnp.where(in_use, jnp.clip(step_a, -1, 1), 0)
        side = jnp.where(in_use, jnp.minimum(side, 2), 1)
        there = here + step_a
        mark_row = lax.broadcasted_iota(jnp.int32, (8, LANES), 0)
        there_at = lax.broadcasted_iota(jnp.int32, (8, LANES), 1) == at
        marks = todo[...]
        for phase in range(2):
            held, spot = [], []
            for m in range(KB):
                held.append(tab[there, NEAR_AT + 8 * m + side + 3 * phase])
                code = tab[there, CODE_AT + 8 * m + 4 * phase + jnp.where(side == 0, 2, 3)]
                far = code + jnp.where(side == 0, 64, 128)
                spot.append(jnp.where(side == 1, there * KB + m, far))
            for f in range(KF):
                wanted = tab[here, NEAR_AT + 8 * f + 1 + 3 * (1 - phase)]
                usable = in_use & (wanted >= 0)
                got = jnp.int32(ZERO)
                for m in range(KB):
                    got = jnp.where(held[m] == wanted, spot[m], got)
                got = jnp.where(usable, got, ZERO)
                if phase:
                    part, slot = (got - 64) >> 5, (got - 64) & 31
                    waits = (got >= 64) & (part < 4) & (slot >= q2 - LATE)
                    code = jnp.clip(part * LATE + slot - (q2 - LATE), 0, 4 * LATE - 1)
                    marks = jnp.where(there_at & (mark_row == f), jnp.where(waits, code, -1), marks)
                    got = jnp.where(waits, ZERO, got)
                pick[phase * PICKS + (row * KB + f) * KB + k] = got
        todo[...] = marks

    zero = jnp.zeros((B, B), jnp.bfloat16)

    zs1, zf1, sh1 = zsend(xv, colp1, 0), zfwd(colp1, 0), share(xv, colp1, 0)
    to_xv.wait()
    zs1.start()
    to_col.start()
    sh1.start()
    hop1 = functools.partial(hop, snd1, rcv1, hs1, hr1, q1)
    fwd1 = functools.partial(fwd, rcv1, fs1, fr1, q1)
    pass1 = functools.partial(relay, rcv1, 0, q1)

    @pl.loop(0, FIRST)
    def _(s):
        for d in range(2):
            snd1[d, s] = xv[list_entry(0, d, s)]

        @pl.when(s > 0)
        def _():
            for d in range(2):
                hop1(d, s - 1).start()

    colp1[ZERO] = zero
    colp2[ZERO] = zero
    for d in range(2):
        hop1(d, FIRST - 1).start()
    to_col.wait()
    zs1.wait_recv()
    zf1.start()
    sh1.wait_recv()
    zf1.wait_recv()

    @pl.loop(FIRST, q1)
    def _(s):
        for d in range(2):
            snd1[d, s] = colp1[sent(0, d, s)]

        @pl.when(s > FIRST)
        def _():
            for d in range(2):
                hop1(d, s - 1).start()

    for d in range(2):
        hop1(d, q1 - 1).start()

    todo[...] = jnp.full((8, LANES), -1, jnp.int32)
    pl.loop(0, OWN)(find_factors)

    @pl.loop(0, q1)
    def _(s):
        wait_all(rcv1.at[pl.ds(0, 2)], hr1.at[s])
        for d in range(2):
            fwd1(d, s).start()

        @pl.when((s >= FIRST) & (s < FIRST + RELAY))
        def _():
            for d in range(2):
                pass1(d, s).start()

    wait_all(snd1, fr1)
    wait_all(rcv1.at[pl.ds(0, 2 * RELAY)], ysem.at[0, 1])

    zs2, zf2, sh2 = zsend(sown, colp2, 1), zfwd(colp2, 1), share(sown, colp2, 1)
    hop2 = functools.partial(hop, snd2, rcv2, hs2, hr2, q2 - LATE)
    fwd2 = functools.partial(fwd, rcv2, fs2, fr2, q2 - LATE)
    pass2 = functools.partial(relay, rcv2, 1, q2 - LATE)

    @pl.loop(0, 2)
    def _(s):
        for d in range(2):
            entry = list_entry(1, d, s)
            snd2[d, s] = product(colp1, rcv1, 0, entry // KB, entry).astype(jnp.bfloat16)
        hop2(0, s).start()

        @pl.when(s > 0)
        def _():
            hop2(1, s - 1).start()

    @pl.loop(0, OWN // 2)
    def _(t):
        step = t // 3
        row = step + core * (RA - 1 - 2 * step)
        for u in range(2):
            entry = row * KB + (t - 3 * step) * 2 + u
            block = product(colp1, rcv1, 0, row, entry).astype(jnp.bfloat16)
            sown[entry] = block
            colp2[own0 + entry] = block

        @pl.when(t == 0)
        def _():
            hop2(1, 1).start()

        @pl.when(t == 3)
        def _():
            zs2.start()

    @pl.loop(2, FIRST)
    def _(s):
        for d in range(2):
            snd2[d, s] = sown[list_entry(1, d, s)]

        @pl.when(s > 2)
        def _():
            for d in range(2):
                hop2(d, s - 1).start()

    sh2.start()
    for d in range(2):
        hop2(d, FIRST - 1).start()
    zs2.wait_recv()
    zf2.start()
    sh2.wait_recv()
    zf2.wait_recv()

    @pl.loop(FIRST, q2 - LATE)
    def _(s):
        for d in range(2):
            snd2[d, s] = colp2[sent(1, d, s)]

        @pl.when(s > FIRST)
        def _():
            for d in range(2):
                hop2(d, s - 1).start()

    for i in range(LATE):
        s = q2 - LATE + i
        for d in range(2):
            snd2[d, s] = colp2[sent(1, d, s)]
        for d in range(2):
            (late_hop(d, i - 1) if i else hop2(d, s - 1)).start()
    for d in range(2):
        late_hop(d, LATE - 1).start()

    @pl.loop(0, q2 - LATE)
    def _(s):
        wait_all(rcv2.at[pl.ds(0, 2)], hr2.at[s])
        for d in range(2):
            fwd2(d, s).start()

        @pl.when((s >= FIRST) & (s < FIRST + RELAY))
        def _():
            for d in range(2):
                pass2(d, s).start()

    wait_all(rcv2.at[pl.ds(0, 2 * (q2 - LATE))], fr2)
    wait_all(rcv2.at[pl.ds(0, 2 * RELAY)], ysem.at[1, 1])

    @pl.loop(0, OWN // 2)
    def _(t):
        row = t // 3
        for u in range(2):
            entry = 2 * t + u
            cubed = product(colp2, rcv2, 1, row, entry)
            in_use = tab[1 + RA * core + row, NEAR_AT + 8 * (entry - row * KB) + 1] >= 0
            own = xv[entry].astype(jnp.float32)
            step = 1.5 * own - cubed * (0.5 / (KB * B))
            out_ref[entry] = jnp.where(in_use, step, 0.0).astype(jnp.bfloat16)
            acc_ref[entry] = cubed

        for i, when in enumerate((5, 10)):

            @pl.when(t == when)
            def _():
                wait_all(rcv2.at[pl.ds(0, 2)], hr2.at[q2 - LATE + i])
                for d in range(2):
                    late_fwd(d, i).start()

    wait_all(late.at[pl.ds(0, 2 * LATE)], lr2)
    zs1.wait_send()
    zf1.wait_send()
    sh1.wait_send()
    zs2.wait_send()
    zf2.wait_send()
    sh2.wait_send()
    for snd, rcv, hs, fs, p in ((snd1, rcv1, hs1, fs1, 0), (snd2, rcv2, hs2, fs2, 1)):
        wait_all(snd, hs)
        wait_all(snd, fs)
        wait_all(rcv.at[pl.ds(0, 2 * RELAY)], ysem.at[p, 0])


def sparse(level, grid_a, grid_c, x_blocks, table):
    q1, q2 = LEVELS[level]
    blocks = x_blocks.reshape(OWN, B, B)
    vm = lambda *lead: pltpu.VMEM((*lead, B, B), jnp.bfloat16)
    dma = lambda *lead: pltpu.SemaphoreType.DMA(lead)
    held = OWN + 2 * COLN + 2 + 6 * (q1 + q2) + 4 * RELAY + 16
    out, acc, late, xv, todo = pl.pallas_call(
        functools.partial(kernel, q1, q2, grid_a, grid_c, lax.axis_size("grp"), lax.axis_size("col")),
        out_shape=(
            pltpu.VMEM(blocks.shape, jnp.bfloat16),
            pltpu.VMEM(blocks.shape, jnp.float32),
            pltpu.VMEM((4 * LATE, B, B), jnp.bfloat16),
            pltpu.VMEM(blocks.shape, jnp.bfloat16),
            pltpu.VMEM((8, LANES), jnp.int32),
        ),
        in_specs=[
            pl.BlockSpec(memory_space=pltpu.SMEM),
            pl.BlockSpec(memory_space=pl.ANY),
        ],
        out_specs=tuple(pl.BlockSpec(memory_space=pltpu.VMEM) for _ in range(5)),
        scratch_shapes=[
            pltpu.SMEM((2 * PICKS,), jnp.int32),
            vm(COLN + 1), vm(4 * q1 + 2 * RELAY), vm(2, q1), vm(COLN + 1),
            vm(4 * (q2 - LATE) + 2 * RELAY), vm(2, q2), vm(OWN),
            dma(2), dma(2, 6),
            dma(), dma(q1), dma(), dma(), dma(), dma(q2), dma(), dma(), dma(), dma(2, 2),
        ],
        compiler_params=pltpu.CompilerParams(
            collective_id=level, has_side_effects=True, vmem_limit_bytes=held * B * B * 2
        ),
        name=f"sign_step_{q1}_{q2}",
    )(table, blocks)
    return finished(todo, out, acc, late, xv).reshape(x_blocks.shape)


def finish_kernel(todo, out_ref, acc_ref, late, xv, res, total, fixed, sem):
    def waits(entry):
        row, f = entry // KB, entry % KB
        codes = [todo[f, row * KB + k] for k in range(KB)]
        any_late = codes[0]
        for c in codes[1:]:
            any_late = jnp.maximum(any_late, c)
        return row, codes, any_late >= 0

    def write(src, entry):
        return pltpu.make_async_copy(src.at[entry], res.at[entry], sem)

    @pl.loop(0, OWN)
    def _(entry):
        @pl.when(~waits(entry)[2])
        def _():
            write(out_ref, entry).start()

    @pl.loop(0, OWN)
    def _(entry):
        row, codes, some = waits(entry)

        @pl.when(some)
        def _():
            total[...] = acc_ref[entry]
            for k in range(KB):

                @pl.when(codes[k] >= 0)
                def _():
                    total[...] += jnp.dot(
                        xv[row * KB + k],
                        late[jnp.clip(codes[k], 0, 4 * LATE - 1)],
                        preferred_element_type=jnp.float32,
                    )

            own = xv[entry].astype(jnp.float32)
            fixed[entry] = (1.5 * own - total[...] * (0.5 / (KB * B))).astype(jnp.bfloat16)

    @pl.loop(0, OWN)
    def _(entry):
        @pl.when(waits(entry)[2])
        def _():
            write(fixed, entry).start()

    pltpu.make_async_copy(out_ref, res, sem).wait()


def finished(todo, out, acc, late, xv):
    return pl.pallas_call(
        finish_kernel,
        out_shape=jax.ShapeDtypeStruct(out.shape, out.dtype),
        in_specs=[pl.BlockSpec(memory_space=pltpu.SMEM)]
        + [pl.BlockSpec(memory_space=pltpu.VMEM)] * 4,
        out_specs=pl.BlockSpec(memory_space=pl.ANY),
        scratch_shapes=[
            pltpu.VMEM((B, B), jnp.float32),
            pltpu.VMEM(out.shape, out.dtype),
            pltpu.SemaphoreType.DMA(()),
        ],
        compiler_params=pltpu.CompilerParams(vmem_limit_bytes=20 * 1024 * 1024),
        name="finish",
    )(todo, out, acc, late, xv)


def local(x_blocks, columns, filter_ids):
    grid_a, grid_c, _ = columns.shape
    table, level = list_tables(columns, filter_ids)
    branches = [
        functools.partial(lambda at, x, c, f, t: sparse(at, grid_a, grid_c, x, t), at)
        for at in range(len(LEVELS))
    ]
    branches.append(lambda x, c, f, t: dense(x, c, f))
    return lax.switch(level[0], branches, x_blocks, columns, filter_ids, table)


def solution(mesh):
    return jax.shard_map(
        local,
        mesh=mesh,
        in_specs=(P("grp", "col", None, None, None), P(), P()),
        out_specs=P("grp", "col", None, None, None),
        check_vma=False,
    )
```

```python
import functools

import jax
import jax.numpy as jnp
from jax import lax
from jax.experimental import pallas as pl
from jax.experimental.pallas import tpu as pltpu
from jax.sharding import PartitionSpec as P

B = 256
KB = 6
KF = 6
RA = 4
OWN = RA * KB
CR = 2 * RA + 2
COLN = CR * KB
ZERO = COLN
FIRST = 5
LATE = 3
RELAY = 4
LEVELS = ((11, 13), (12, 13), (11, 14), (12, 14), (13, 15), (15, 18))

PICKS = OWN * KB
MESH = pl.DeviceIdType.MESH


def padded(cells, sides, width):
    for axis, dim in sides:
        count = lax.axis_size(axis)
        head = lax.slice_in_dim(cells, 0, width, axis=dim)
        tail = lax.slice_in_dim(cells, cells.shape[dim] - width, cells.shape[dim], axis=dim)
        cells = jnp.concatenate(
            [
                lax.ppermute(tail, axis, [(i, (i + 1) % count) for i in range(count)]),
                cells,
                lax.ppermute(head, axis, [((i + 1) % count, i) for i in range(count)]),
            ],
            axis=dim,
        )
    return cells


def block_terms(
    halo, pos_a, pos_c, row_ids, row_cols, left_blocks, stored_table, wanted, grid_a, grid_c
):
    slot_count = halo.shape[2]
    width = halo.shape[3]
    in_use = row_cols >= 0
    source = jnp.where(in_use, row_cols, 0)
    home_a = row_ids // grid_c
    home_c = row_ids % grid_c
    step_a = (source // grid_c - home_a[:, None] + 1) % grid_a - 1
    step_c = (source % grid_c - home_c[:, None] + 1) % grid_c - 1
    place = (pos_a[:, None] + step_a) * halo.shape[1] + pos_c[:, None] + step_c
    flat = halo.reshape((halo.shape[0] * halo.shape[1] * slot_count, width, width))
    stored = stored_table[source]
    matches = stored[:, :, None, :] == wanted[:, None, :, None]
    present = jnp.any(matches, axis=3) & (wanted[:, None, :] >= 0) & in_use[:, :, None]
    slot_of = jnp.argmax(matches.astype(jnp.int32), axis=3)
    block_index = place[:, :, None] * slot_count + slot_of

    def one_row(inputs):
        index_row, present_row, left_row = inputs
        picked = flat[index_row]
        picked = jnp.where(present_row[:, :, None, None], picked, jnp.zeros((), picked.dtype))
        return jnp.einsum("kab,kfbc->fac", left_row, picked, preferred_element_type=jnp.float32)

    return lax.map(one_row, (block_index, present, left_blocks))


def dense(x_blocks, columns, filter_ids):
    grp_count = lax.axis_size("grp")
    col_count = lax.axis_size("col")
    rows_a = x_blocks.shape[0]
    rows_c = x_blocks.shape[1]
    grid_a = rows_a * grp_count
    grid_c = rows_c * col_count
    col_table = columns.reshape(grid_a * grid_c, KB)
    filt_table = filter_ids.reshape(grid_a * grid_c, KF)
    local_rows = rows_a * rows_c
    offsets = jnp.arange(local_rows, dtype=jnp.int32)
    local_a = offsets // rows_c
    local_c = offsets % rows_c
    row_ids = (
        (lax.axis_index("grp") * rows_a + local_a) * grid_c
        + lax.axis_index("col") * rows_c
        + local_c
    )
    row_cols = col_table[row_ids]
    left_blocks = x_blocks.reshape(local_rows, KB, B, B)
    along_col = padded(x_blocks, (("col", 1),), 1)
    near_x = padded(along_col, (("grp", 0),), 1)
    square = block_terms(
        near_x,
        local_a + 1,
        local_c + 1,
        row_ids,
        row_cols,
        left_blocks,
        col_table,
        filt_table[row_ids],
        grid_a,
        grid_c,
    ).astype(jnp.bfloat16)
    square = square.reshape(rows_a, rows_c, KF, B, B)
    square_along = padded(square, (("col", 1),), 1)
    near_square = padded(square_along, (("grp", 0),), 1)
    cubed = block_terms(
        near_square,
        local_a + 1,
        local_c + 1,
        row_ids,
        row_cols,
        left_blocks,
        filt_table,
        row_cols,
        grid_a,
        grid_c,
    )
    in_use = (row_cols >= 0).astype(jnp.float32)
    result = (1.5 * left_blocks.astype(jnp.float32) - cubed * (0.5 / (KB * B))) * in_use[
        :, :, None, None
    ]
    return result.astype(jnp.bfloat16).reshape(x_blocks.shape)


LANES = 128
LISTS = 8
CODE_AT = 0
NEAR_AT = 48
SRC_AT = 96
TABLE_ROWS = 16


def index_kernel(cols_ref, filt_ref, table_ref, level_ref, own_ref, halo_ref, move_ref,
                 cols_s, filt_s):
    grp = lax.axis_index("grp")
    col = lax.axis_index("col")
    core = lax.rem(grp, 2)
    grid_c = cols_ref.shape[1]
    grid_a = cols_ref.shape[2]
    chip = 2 * RA

    def lanes_of(x):
        return jnp.concatenate([x] * (LANES // grid_a), axis=1)

    stored, kept = [], []
    for m in range(KB):
        stored.append(lanes_of(cols_ref[m]))
        kept.append(lanes_of(filt_ref[m]))
        cols_s[m] = stored[m]
        filt_s[m] = kept[m]
    shape = (grid_c, LANES)
    lane = lax.broadcasted_iota(jnp.int32, shape, 1)
    ids = lax.rem(lane, grid_a) * grid_c + lax.broadcasted_iota(jnp.int32, shape, 0)
    in_chip = lax.rem(lane, chip)
    first, last = in_chip == 0, in_chip == chip - 1
    false = jnp.zeros(shape, jnp.int32)

    def either(tests):
        got = tests[0]
        for t in tests[1:]:
            got = got | t
        return got

    totals = []
    for d, step_c in enumerate((1, -1)):
        cols_c = [jnp.roll(x, -step_c, 0) for x in stored]
        filt_c = [jnp.roll(x, -step_c, 0) for x in kept]
        found = []
        for step_a in (-1, 0, 1):
            shift = (-step_a) % LANES
            cols_r = [pltpu.roll(x, shift, 1) if shift else x for x in cols_c]
            filt_r = [pltpu.roll(x, shift, 1) if shift else x for x in filt_c]
            member = either([x == ids for x in cols_r])
            one = [either([stored[m] == x for x in filt_r]) & member & (stored[m] >= 0) for m in range(KB)]
            two = [either([kept[m] == x for x in cols_r]) & member for m in range(KB)]
            found.append((one, two))
        up, mid, down = found
        for phase in (0, 1):
            own_row, halo_row = false, false
            flags = []
            for m in range(KB):
                u, c, w = up[phase][m], mid[phase][m], down[phase][m]
                own = (c | (u & ~first) | (w & ~last)).astype(jnp.int32)
                halo = ((u & first) | (w & last)).astype(jnp.int32)
                flags.append((own, halo))
                own_row = own_row + own
                halo_row = halo_row + halo
            totals.append((phase, d, flags, own_row, halo_row))

    def summed(x, rule):
        at = lax.broadcasted_iota(jnp.int32, (LANES, LANES), 0)
        to = lax.broadcasted_iota(jnp.int32, (LANES, LANES), 1)
        weight = rule(at, to).astype(jnp.float32).astype(jnp.bfloat16)
        return jnp.dot(
            x.astype(jnp.float32).astype(jnp.bfloat16), weight, preferred_element_type=jnp.float32
        ).astype(jnp.int32)

    def same_chip(at, to):
        return (at // chip == lax.rem(to, grid_a) // chip) & (at < grid_a)

    def beside(at, to):
        z = lax.rem(to, grid_a) // chip * chip
        above = lax.rem(z + grid_a - 1, grid_a)
        below = lax.rem(z + chip, grid_a)
        return (at == above) | (at == below)

    def stack(xs):
        return jnp.concatenate(xs, axis=0)

    loads = summed(stack([t[3] for t in totals]), same_chip) + summed(
        stack([t[4] for t in totals]), beside
    )

    def across(x):
        return jnp.where(last, pltpu.roll(x, LANES - 1, 1), pltpu.roll(x, 1, 1))

    kept_own, kept_halo, got0, got1 = [], [], [], []
    for p, (phase, d, flags, _, _) in enumerate(totals):
        load = loads[p * grid_c : (p + 1) * grid_c]
        lead = jnp.where(last, load - across(load), across(load) - load)
        far = jnp.abs(lead)
        count = jnp.zeros(shape, jnp.int32)
        for step in range(RELAY):
            count = count + (far >= 3 * step + 2).astype(jnp.int32)
        ups = (lead > 0).astype(jnp.int32)
        rim = (first | last).astype(jnp.int32)
        both = [own * halo * rim for own, halo in flags]
        lower = [jnp.where(last, own, halo) for own, halo in flags]
        upper = [jnp.where(last, halo, own) for own, halo in flags]
        single = [
            jnp.where(ups > 0, lower[m], upper[m]) * rim - both[m] for m in range(KB)
        ]
        n_both = sum(both[1:], both[0])
        n_single = sum(single[1:], single[0])
        both_rank = jnp.where(last, 0, across(n_both))
        single_rank = n_both + across(n_both) + jnp.where(last, 0, across(n_single))
        own_row, halo_row, moved_row = false, false, false
        for m in range(KB):
            rank = jnp.where(both[m] > 0, both_rank, single_rank)
            moved = ((both[m] + single[m]) > 0) & (rank < count)
            move = jnp.where(moved, rank + 1 + 8 * ups, 0)
            both_rank = both_rank + both[m]
            single_rank = single_rank + single[m]
            own = jnp.where(moved, 0, flags[m][0])
            halo = jnp.where(moved, 0, flags[m][1])
            own_ref[phase, d, m] = own
            halo_ref[phase, d, m] = halo
            move_ref[phase, d, m] = move
            own_row, halo_row = own_row + own, halo_row + halo
            moved_row = moved_row + moved.astype(jnp.int32)
        moved_row = moved_row + across(moved_row)
        kept_own.append(own_row)
        kept_halo.append(halo_row)
        got0.append(jnp.where(first, moved_row * ups, 0))
        got1.append(jnp.where(last, moved_row * (1 - ups), 0))

    def split(n0, n1, total, extra0, extra1):
        half = jnp.clip((total + extra1 - extra0 + 1) >> 1, 0, total)
        return half, jnp.maximum(FIRST - n0, 0), jnp.maximum(FIRST - n1, 0)

    own_all = stack(kept_own)
    n0 = summed(own_all, lambda at, to: same_chip(at, to) & (lax.rem(at, chip) < RA))
    n1 = summed(own_all, lambda at, to: same_chip(at, to) & (lax.rem(at, chip) >= RA))
    total = n0 + n1 + summed(stack(kept_halo), beside)
    extra0 = summed(stack(got0), same_chip)
    extra1 = summed(stack(got1), same_chip)
    half, gap0, gap1 = split(n0, n1, total, extra0, extra1)
    rest = total - half
    fill = jnp.maximum(
        half + jnp.where(half > n0, gap0, 0) + extra0,
        rest + jnp.where(rest > n1, gap1, 0) + extra1,
    )
    most = [jnp.int32(FIRST + RELAY), jnp.int32(FIRST + RELAY)]
    for p, (phase, _, _, _, _) in enumerate(totals):
        most[phase] = jnp.maximum(most[phase], jnp.max(fill[p * grid_c : (p + 1) * grid_c]))
    level = jnp.int32(len(LEVELS))
    for at in reversed(range(len(LEVELS))):
        fits = (most[0] <= LEVELS[at][0]) & (most[1] <= LEVELS[at][1])
        level = jnp.where(fits, at, level)
    level_ref[0] = level

    z = grp // 2
    shift = lax.rem(LANES + 1 - z * chip, LANES)
    west = lax.rem(col + grid_c - 1, grid_c)
    east = lax.rem(col + 1, grid_c)
    row8 = (LISTS, LANES)
    lane8 = lax.broadcasted_iota(jnp.int32, row8, 1)
    rim = (lane8 == 0) | (lane8 == CR - 1)
    lists = [(p, d, c) for p in (0, 1) for d, c in ((0, col), (1, col), (0, west), (1, east))]

    def near(ref_rows):
        return pltpu.roll(jnp.concatenate(ref_rows, axis=0), shift, 1)

    need, in_row, stores, moves = [], [], [], []
    run = jnp.zeros(row8, jnp.int32)
    relayed = jnp.zeros(row8, jnp.int32)
    low_end = lane8 <= 1
    for m in range(KB):
        own = near([own_ref[p, d, m, pl.ds(c, 1), :] for p, d, c in lists])
        halo = near([halo_ref[p, d, m, pl.ds(c, 1), :] for p, d, c in lists])
        flags = jnp.where(lane8 < CR, jnp.where(rim, halo, own), 0)
        need.append(flags)
        in_row.append(run)
        run = run + flags
        move = near([move_ref[p, d, m, pl.ds(c, 1), :] for p, d, c in lists])
        move = jnp.where((lane8 <= 1) | ((lane8 >= CR - 2) & (lane8 < CR)), move, 0)
        mine = (move > 0) & ((move > 8) == low_end)
        moves.append((move, mine))
        relayed = relayed + mine.astype(jnp.int32)
        rows = [cols_s[m, pl.ds(c, 1), :] for c in (west, col, east)]
        rows += [filt_s[m, pl.ds(c, 1), :] for c in (west, col, east)]
        stores.append(near(rows + rows[:2]))
    n0 = summed(run, lambda at, to: (at >= 1) & (at <= RA))
    n1 = summed(run, lambda at, to: (at > RA) & (at <= chip))
    above = summed(run, lambda at, to: at == 0)
    below = summed(run, lambda at, to: at == CR - 1)
    ahead = summed(
        run, lambda at, to: (at < to) & (((at >= 1) & (to <= RA)) | ((at > RA) & (to <= chip)))
    )
    total = n0 + n1 + above + below
    extra0 = summed(relayed, lambda at, to: at <= 1)
    extra1 = summed(relayed, lambda at, to: at > 1)
    half, gap0, gap1 = split(n0, n1, total, extra0, extra1)
    east_list = lax.rem(lax.broadcasted_iota(jnp.int32, row8, 0), 4) == 3
    of0 = (lane8 >= 1) & (lane8 <= RA)
    of1 = (lane8 > RA) & (lane8 <= chip)
    slots = lax.broadcasted_iota(jnp.int32, (32, LANES), 0) + core * 32
    entry = lax.broadcasted_iota(jnp.int32, (32, LANES), 1) * KB
    source = [jnp.zeros((32, LANES), jnp.int32) for _ in range(4)]
    codes = []
    for m in range(KB):
        place = ahead + in_row[m]
        place = jnp.where(lane8 == 0, n0 + in_row[m], place)
        place = jnp.where(lane8 == CR - 1, n0 + above + in_row[m], place)
        place = jnp.where(of1, total - 1 - place, place)
        turned = total - 1 - place
        slot0 = place + jnp.where(of0, 0, gap0)
        slot1 = turned + jnp.where(of1, 0, gap1)
        slot0 = slot0 + jnp.where(slot0 >= FIRST, extra0, 0)
        slot1 = slot1 + jnp.where(slot1 >= FIRST, extra1, 0)
        code = jnp.where(place < half, slot0, 32 + slot1)
        move, mine = moves[m]
        rank = (move & 7) - 1
        code = jnp.where(mine, jnp.where(low_end, FIRST, 32 + FIRST) + rank, code)
        code = jnp.where((move > 0) & ~mine, jnp.where(east_list, 96, 128) + rank, code)
        codes.append(code)
        sent = jnp.where((need[m] > 0) | mine, code, -1)
        for i, at in enumerate((0, 1, 4, 5)):
            same = jnp.broadcast_to(sent[at : at + 1], (32, LANES)) == slots
            source[i] = source[i] + jnp.where(same, entry + m, 0)
    lane32 = lax.broadcasted_iota(jnp.int32, (32, LANES), 1)
    out = jnp.zeros((32, LANES), jnp.int32)
    for i in range(4):
        out = jnp.where(lane32 == i, jnp.sum(source[i], axis=1, keepdims=True), out)
    table_ref[...] = jnp.concatenate(codes + stores + [out], axis=0).T[:TABLE_ROWS]


def list_tables(columns, filter_ids):
    grid_a, grid_c, _ = columns.shape
    ints = lambda *shape: pltpu.VMEM(shape, jnp.int32)
    return pl.pallas_call(
        index_kernel,
        out_shape=(
            jax.ShapeDtypeStruct((TABLE_ROWS, LANES), jnp.int32),
            jax.ShapeDtypeStruct((1,), jnp.int32),
        ),
        in_specs=[pl.BlockSpec(memory_space=pltpu.VMEM)] * 2,
        out_specs=(
            pl.BlockSpec(memory_space=pltpu.VMEM),
            pl.BlockSpec(memory_space=pltpu.SMEM),
        ),
        scratch_shapes=[
            ints(2, 2, KB, grid_c, LANES), ints(2, 2, KB, grid_c, LANES),
            ints(2, 2, KB, grid_c, LANES),
            ints(KB, grid_c, LANES), ints(KF, grid_c, LANES),
        ],
        name="block_lists",
    )(columns.transpose(2, 1, 0), filter_ids.transpose(2, 1, 0))


def kernel(q1, q2, grid_a, grid_c, grp_count, col_count, tab, x_hbm, out_ref, acc_ref, late, xv, todo, pick, colp1, rcv1, snd1, colp2, rcv2,
           snd2, sown, lsem, zsem, hs1, hr1, fs1, fr1, hs2, hr2, fs2, fr2, lr2, ysem):
    grp = lax.axis_index("grp")
    col = lax.axis_index("col")
    core = lax.rem(grp, 2)
    partner = (grp + 1 - 2 * core, col)
    zpeer = (lax.rem(grp + grp_count - 1 + 2 * core, grp_count), col)
    right = (grp, lax.rem(col + 1, col_count))
    left = (grp, lax.rem(col + col_count - 1, col_count))
    own0 = (1 + RA * core) * KB
    zout = (RA - 1) * core * KB
    zdst = (CR - 1) * (1 - core) * KB
    zin = (CR - 1) * core * KB

    to_xv = pltpu.make_async_copy(x_hbm, xv, lsem.at[0])
    to_col = pltpu.make_async_copy(x_hbm, colp1.at[pl.ds(own0, OWN)], lsem.at[1])
    to_xv.start()

    barrier = pltpu.get_barrier_semaphore()
    for peer in (partner, zpeer, right, left):
        pl.semaphore_signal(barrier, inc=1, device_id=peer, device_id_type=MESH)
    pl.semaphore_wait(barrier, 4)

    def remote(src, dst, send, recv, device):
        return pltpu.make_async_remote_copy(
            src_ref=src, dst_ref=dst, send_sem=send, recv_sem=recv,
            device_id=device, device_id_type=MESH,
        )

    def zsend(src, colp, p):
        return remote(src.at[pl.ds(zout, KB)], colp.at[pl.ds(zdst, KB)],
                      zsem.at[p, 0], zsem.at[p, 1], zpeer)

    def zfwd(colp, p):
        here = colp.at[pl.ds(zin, KB)]
        return remote(here, here, zsem.at[p, 2], zsem.at[p, 3], partner)

    def share(src, colp, p):
        return remote(src, colp.at[pl.ds(own0, OWN)], zsem.at[p, 4], zsem.at[p, 5], partner)

    def hop(snd, rcv, hs, hr, q, d, s):
        return remote(snd.at[d, s], rcv.at[(2 * d + core) * q + s], hs, hr.at[s],
                      (right, left)[d])

    def fwd(rcv, fs, fr, q, d, s):
        here = rcv.at[(2 * d + core) * q + s]
        return remote(here, here, fs, fr, partner)

    def late_hop(d, i):
        s = q2 - LATE + i
        return remote(snd2.at[d, s], late.at[(2 * d + core) * LATE + i], hs2, hr2.at[s],
                      (right, left)[d])

    def late_fwd(d, i):
        here = late.at[(2 * d + core) * LATE + i]
        return remote(here, here, fs2, lr2, partner)

    def relay(rcv, p, q, d, s):
        rank = s - FIRST
        return remote(rcv.at[(2 * d + core) * q + s], rcv.at[4 * q + d * RELAY + rank],
                      ysem.at[p, 0], ysem.at[p, 1], zpeer)

    def wait_all(like, sem):
        pltpu.make_async_copy(like, like, sem).wait()

    def right_factor(colp, rcv, q, v):
        is_col = v < 64
        at_col = jnp.where(is_col, v, ZERO)
        at_rcv = jnp.where(is_col, 0, v - 64)
        part = at_rcv >> 5
        slot = at_rcv & 31
        direct = jnp.minimum(part, 3) * q + jnp.minimum(slot, q - 1)
        passed = 4 * q + jnp.clip((part - 4) * RELAY + slot, 0, 2 * RELAY - 1)
        return jnp.where(is_col, colp[at_col], rcv[jnp.where(part < 4, direct, passed)])

    def product(colp, rcv, phase, row, entry):
        acc = None
        for k in range(KB):
            v = pick[phase * PICKS + entry * KB + k]
            term = jnp.dot(xv[row * KB + k], right_factor(colp, rcv, (q1, q2 - LATE)[phase], v),
                           preferred_element_type=jnp.float32)
            acc = term if acc is None else acc + term
        return acc

    def sent(phase, d, s):
        return tab[2 * phase + d, SRC_AT + s]

    def list_entry(phase, d, s):
        return jnp.clip(sent(phase, d, s) - own0, 0, OWN - 1)

    def find_factors(at):
        row = at // KB
        k = at - KB * row
        here = 1 + RA * core + row
        source = tab[here, NEAR_AT + 8 * k + 1]
        in_use = source >= 0
        source = jnp.where(in_use, source, 0)
        step_a = lax.rem(source // grid_c - (grp * RA + row) + 1 + grid_a, grid_a) - 1
        side = lax.rem(lax.rem(source, grid_c) - col + 1 + grid_c, grid_c)
        step_a = jnp.where(in_use, jnp.clip(step_a, -1, 1), 0)
        side = jnp.where(in_use, jnp.minimum(side, 2), 1)
        there = here + step_a
        mark_row = lax.broadcasted_iota(jnp.int32, (8, LANES), 0)
        there_at = lax.broadcasted_iota(jnp.int32, (8, LANES), 1) == at
        marks = todo[...]
        for phase in range(2):
            held, spot = [], []
            for m in range(KB):
                held.append(tab[there, NEAR_AT + 8 * m + side + 3 * phase])
                code = tab[there, CODE_AT + 8 * m + 4 * phase + jnp.where(side == 0, 2, 3)]
                far = code + jnp.where(side == 0, 64, 128)
                spot.append(jnp.where(side == 1, there * KB + m, far))
            for f in range(KF):
                wanted = tab[here, NEAR_AT + 8 * f + 1 + 3 * (1 - phase)]
                usable = in_use & (wanted >= 0)
                got = jnp.int32(ZERO)
                for m in range(KB):
                    got = jnp.where(held[m] == wanted, spot[m], got)
                got = jnp.where(usable, got, ZERO)
                if phase:
                    part, slot = (got - 64) >> 5, (got - 64) & 31
                    waits = (got >= 64) & (part < 4) & (slot >= q2 - LATE)
                    code = jnp.clip(part * LATE + slot - (q2 - LATE), 0, 4 * LATE - 1)
                    marks = jnp.where(there_at & (mark_row == f), jnp.where(waits, code, -1), marks)
                    got = jnp.where(waits, ZERO, got)
                pick[phase * PICKS + (row * KB + f) * KB + k] = got
        todo[...] = marks

    zero = jnp.zeros((B, B), jnp.bfloat16)

    zs1, zf1, sh1 = zsend(xv, colp1, 0), zfwd(colp1, 0), share(xv, colp1, 0)
    to_xv.wait()
    zs1.start()
    to_col.start()
    sh1.start()
    hop1 = functools.partial(hop, snd1, rcv1, hs1, hr1, q1)
    fwd1 = functools.partial(fwd, rcv1, fs1, fr1, q1)
    pass1 = functools.partial(relay, rcv1, 0, q1)

    @pl.loop(0, FIRST)
    def _(s):
        for d in range(2):
            snd1[d, s] = xv[list_entry(0, d, s)]

        @pl.when(s > 0)
        def _():
            for d in range(2):
                hop1(d, s - 1).start()

    colp1[ZERO] = zero
    colp2[ZERO] = zero
    for d in range(2):
        hop1(d, FIRST - 1).start()
    to_col.wait()
    zs1.wait_recv()
    zf1.start()
    sh1.wait_recv()
    zf1.wait_recv()

    @pl.loop(FIRST, q1)
    def _(s):
        for d in range(2):
            snd1[d, s] = colp1[sent(0, d, s)]

        @pl.when(s > FIRST)
        def _():
            for d in range(2):
                hop1(d, s - 1).start()

    for d in range(2):
        hop1(d, q1 - 1).start()

    todo[...] = jnp.full((8, LANES), -1, jnp.int32)
    pl.loop(0, OWN)(find_factors)

    @pl.loop(0, q1)
    def _(s):
        wait_all(rcv1.at[pl.ds(0, 2)], hr1.at[s])
        for d in range(2):
            fwd1(d, s).start()

        @pl.when((s >= FIRST) & (s < FIRST + RELAY))
        def _():
            for d in range(2):
                pass1(d, s).start()

    wait_all(snd1, fr1)
    wait_all(rcv1.at[pl.ds(0, 2 * RELAY)], ysem.at[0, 1])

    zs2, zf2, sh2 = zsend(sown, colp2, 1), zfwd(colp2, 1), share(sown, colp2, 1)
    hop2 = functools.partial(hop, snd2, rcv2, hs2, hr2, q2 - LATE)
    fwd2 = functools.partial(fwd, rcv2, fs2, fr2, q2 - LATE)
    pass2 = functools.partial(relay, rcv2, 1, q2 - LATE)

    @pl.loop(0, 2 + OWN // 2)
    def _(t):
        listed = t < 2
        slot = jnp.where(listed, t, 0)
        at = jnp.where(listed, 0, t - 2)
        step = at // 3
        row = step + core * (RA - 1 - 2 * step)
        for d in range(2):
            own_entry = row * KB + (at - 3 * step) * 2 + d
            entry = jnp.where(listed, list_entry(1, d, slot), own_entry)
            block = product(colp1, rcv1, 0, entry // KB, entry).astype(jnp.bfloat16)

            @pl.when(listed)
            def _():
                snd2[d, slot] = block

            @pl.when(~listed)
            def _():
                sown[own_entry] = block
                colp2[own0 + own_entry] = block

        @pl.when(listed)
        def _():
            hop2(0, slot).start()

        @pl.when((t > 0) & (t < 3))
        def _():
            hop2(1, t - 1).start()

        @pl.when(t == 5)
        def _():
            zs2.start()

    @pl.loop(2, FIRST)
    def _(s):
        for d in range(2):
            snd2[d, s] = sown[list_entry(1, d, s)]

        @pl.when(s > 2)
        def _():
            for d in range(2):
                hop2(d, s - 1).start()

    sh2.start()
    for d in range(2):
        hop2(d, FIRST - 1).start()
    zs2.wait_recv()
    zf2.start()
    sh2.wait_recv()
    zf2.wait_recv()

    @pl.loop(FIRST, q2 - LATE)
    def _(s):
        for d in range(2):
            snd2[d, s] = colp2[sent(1, d, s)]

        @pl.when(s > FIRST)
        def _():
            for d in range(2):
                hop2(d, s - 1).start()

    for i in range(LATE):
        s = q2 - LATE + i
        for d in range(2):
            snd2[d, s] = colp2[sent(1, d, s)]
        for d in range(2):
            (late_hop(d, i - 1) if i else hop2(d, s - 1)).start()
    for d in range(2):
        late_hop(d, LATE - 1).start()

    @pl.loop(0, q2 - LATE)
    def _(s):
        wait_all(rcv2.at[pl.ds(0, 2)], hr2.at[s])
        for d in range(2):
            fwd2(d, s).start()

        @pl.when((s >= FIRST) & (s < FIRST + RELAY))
        def _():
            for d in range(2):
                pass2(d, s).start()

    wait_all(rcv2.at[pl.ds(0, 2 * (q2 - LATE))], fr2)
    wait_all(rcv2.at[pl.ds(0, 2 * RELAY)], ysem.at[1, 1])

    def pass_late(i):
        wait_all(rcv2.at[pl.ds(0, 2)], hr2.at[q2 - LATE + i])
        for d in range(2):
            late_fwd(d, i).start()

    @pl.loop(0, OWN // 2)
    def _(t):
        row = t // 3
        for u in range(2):
            entry = 2 * t + u
            cubed = product(colp2, rcv2, 1, row, entry)
            in_use = tab[1 + RA * core + row, NEAR_AT + 8 * (entry - row * KB) + 1] >= 0
            own = xv[entry].astype(jnp.float32)
            step = 1.5 * own - cubed * (0.5 / (KB * B))
            out_ref[entry] = jnp.where(in_use, step, 0.0).astype(jnp.bfloat16)
            acc_ref[entry] = cubed

        for i, when in enumerate((5, 11)):

            @pl.when(t == when)
            def _():
                pass_late(i)

    pass_late(2)

    wait_all(late.at[pl.ds(0, 2 * LATE)], lr2)
    zs1.wait_send()
    zf1.wait_send()
    sh1.wait_send()
    zs2.wait_send()
    zf2.wait_send()
    sh2.wait_send()
    for snd, rcv, hs, fs, p in ((snd1, rcv1, hs1, fs1, 0), (snd2, rcv2, hs2, fs2, 1)):
        wait_all(snd, hs)
        wait_all(snd, fs)
        wait_all(rcv.at[pl.ds(0, 2 * RELAY)], ysem.at[p, 0])


def sparse(level, grid_a, grid_c, x_blocks, table):
    q1, q2 = LEVELS[level]
    blocks = x_blocks.reshape(OWN, B, B)
    vm = lambda *lead: pltpu.VMEM((*lead, B, B), jnp.bfloat16)
    dma = lambda *lead: pltpu.SemaphoreType.DMA(lead)
    held = OWN + 2 * COLN + 2 + 6 * (q1 + q2) + 4 * RELAY + 16
    out, acc, late, xv, todo = pl.pallas_call(
        functools.partial(kernel, q1, q2, grid_a, grid_c, lax.axis_size("grp"), lax.axis_size("col")),
        out_shape=(
            pltpu.VMEM(blocks.shape, jnp.bfloat16),
            pltpu.VMEM(blocks.shape, jnp.float32),
            pltpu.VMEM((4 * LATE, B, B), jnp.bfloat16),
            pltpu.VMEM(blocks.shape, jnp.bfloat16),
            pltpu.VMEM((8, LANES), jnp.int32),
        ),
        in_specs=[
            pl.BlockSpec(memory_space=pltpu.SMEM),
            pl.BlockSpec(memory_space=pl.ANY),
        ],
        out_specs=tuple(pl.BlockSpec(memory_space=pltpu.VMEM) for _ in range(5)),
        scratch_shapes=[
            pltpu.SMEM((2 * PICKS,), jnp.int32),
            vm(COLN + 1), vm(4 * q1 + 2 * RELAY), vm(2, q1), vm(COLN + 1),
            vm(4 * (q2 - LATE) + 2 * RELAY), vm(2, q2), vm(OWN),
            dma(2), dma(2, 6),
            dma(), dma(q1), dma(), dma(), dma(), dma(q2), dma(), dma(), dma(), dma(2, 2),
        ],
        compiler_params=pltpu.CompilerParams(
            collective_id=level, has_side_effects=True, vmem_limit_bytes=held * B * B * 2
        ),
        name=f"sign_step_{q1}_{q2}",
    )(table, blocks)
    return finished(todo, out, acc, late, xv).reshape(x_blocks.shape)


def finish_kernel(todo, out_ref, acc_ref, late, xv, res, some, total, fixed, sem):
    def write(src, entry):
        return pltpu.make_async_copy(src.at[entry], res.at[entry], sem)

    @pl.loop(0, KF)
    def _(f):
        for row in range(RA):
            entry = row * KB + f
            latest = todo[f, row * KB]
            for k in range(1, KB):
                latest = jnp.maximum(latest, todo[f, row * KB + k])
            some[entry] = latest

            @pl.when(latest < 0)
            def _():
                write(out_ref, entry).start()

    @pl.loop(0, OWN)
    def _(entry):
        @pl.when(some[entry] >= 0)
        def _():
            row, f = entry // KB, entry % KB
            total[...] = acc_ref[entry]
            for k in range(KB):
                code = todo[f, row * KB + k]

                @pl.when(code >= 0)
                def _():
                    total[...] += jnp.dot(
                        xv[row * KB + k],
                        late[jnp.clip(code, 0, 4 * LATE - 1)],
                        preferred_element_type=jnp.float32,
                    )

            own = xv[entry].astype(jnp.float32)
            fixed[entry] = (1.5 * own - total[...] * (0.5 / (KB * B))).astype(jnp.bfloat16)

    @pl.loop(0, OWN)
    def _(entry):
        @pl.when(some[entry] >= 0)
        def _():
            write(fixed, entry).start()

    pltpu.make_async_copy(out_ref, res, sem).wait()


def finished(todo, out, acc, late, xv):
    return pl.pallas_call(
        finish_kernel,
        out_shape=jax.ShapeDtypeStruct(out.shape, out.dtype),
        in_specs=[pl.BlockSpec(memory_space=pltpu.SMEM)]
        + [pl.BlockSpec(memory_space=pltpu.VMEM)] * 4,
        out_specs=pl.BlockSpec(memory_space=pl.ANY),
        scratch_shapes=[
            pltpu.SMEM((OWN,), jnp.int32),
            pltpu.VMEM((B, B), jnp.float32),
            pltpu.VMEM(out.shape, out.dtype),
            pltpu.SemaphoreType.DMA(()),
        ],
        compiler_params=pltpu.CompilerParams(vmem_limit_bytes=20 * 1024 * 1024),
        name="finish",
    )(todo, out, acc, late, xv)


def local(x_blocks, columns, filter_ids):
    grid_a, grid_c, _ = columns.shape
    table, level = list_tables(columns, filter_ids)
    branches = [
        functools.partial(lambda at, x, c, f, t: sparse(at, grid_a, grid_c, x, t), at)
        for at in range(len(LEVELS))
    ]
    branches.append(lambda x, c, f, t: dense(x, c, f))
    return lax.switch(level[0], branches, x_blocks, columns, filter_ids, table)


def solution(mesh):
    return jax.shard_map(
        local,
        mesh=mesh,
        in_specs=(P("grp", "col", None, None, None), P(), P()),
        out_specs=P("grp", "col", None, None, None),
        check_vma=False,
    )
```

```python
import functools

import jax
import jax.numpy as jnp
from jax import lax
from jax.experimental import pallas as pl
from jax.experimental.pallas import tpu as pltpu
from jax.sharding import PartitionSpec as P

B = 256
KB = 6
KF = 6
RA = 4
OWN = RA * KB
CR = 2 * RA + 2
COLN = CR * KB
ZERO = COLN
FIRST = 5
LATE = 3
RELAY = 4
LEVELS = ((11, 13), (12, 13), (11, 14), (12, 14), (13, 15), (15, 18))

PICKS = OWN * KB
MESH = pl.DeviceIdType.MESH


def padded(cells, sides, width):
    for axis, dim in sides:
        count = lax.axis_size(axis)
        head = lax.slice_in_dim(cells, 0, width, axis=dim)
        tail = lax.slice_in_dim(cells, cells.shape[dim] - width, cells.shape[dim], axis=dim)
        cells = jnp.concatenate(
            [
                lax.ppermute(tail, axis, [(i, (i + 1) % count) for i in range(count)]),
                cells,
                lax.ppermute(head, axis, [((i + 1) % count, i) for i in range(count)]),
            ],
            axis=dim,
        )
    return cells


def block_terms(
    halo, pos_a, pos_c, row_ids, row_cols, left_blocks, stored_table, wanted, grid_a, grid_c
):
    slot_count = halo.shape[2]
    width = halo.shape[3]
    in_use = row_cols >= 0
    source = jnp.where(in_use, row_cols, 0)
    home_a = row_ids // grid_c
    home_c = row_ids % grid_c
    step_a = (source // grid_c - home_a[:, None] + 1) % grid_a - 1
    step_c = (source % grid_c - home_c[:, None] + 1) % grid_c - 1
    place = (pos_a[:, None] + step_a) * halo.shape[1] + pos_c[:, None] + step_c
    flat = halo.reshape((halo.shape[0] * halo.shape[1] * slot_count, width, width))
    stored = stored_table[source]
    matches = stored[:, :, None, :] == wanted[:, None, :, None]
    present = jnp.any(matches, axis=3) & (wanted[:, None, :] >= 0) & in_use[:, :, None]
    slot_of = jnp.argmax(matches.astype(jnp.int32), axis=3)
    block_index = place[:, :, None] * slot_count + slot_of

    def one_row(inputs):
        index_row, present_row, left_row = inputs
        picked = flat[index_row]
        picked = jnp.where(present_row[:, :, None, None], picked, jnp.zeros((), picked.dtype))
        return jnp.einsum("kab,kfbc->fac", left_row, picked, preferred_element_type=jnp.float32)

    return lax.map(one_row, (block_index, present, left_blocks))


def dense(x_blocks, columns, filter_ids):
    grp_count = lax.axis_size("grp")
    col_count = lax.axis_size("col")
    rows_a = x_blocks.shape[0]
    rows_c = x_blocks.shape[1]
    grid_a = rows_a * grp_count
    grid_c = rows_c * col_count
    col_table = columns.reshape(grid_a * grid_c, KB)
    filt_table = filter_ids.reshape(grid_a * grid_c, KF)
    local_rows = rows_a * rows_c
    offsets = jnp.arange(local_rows, dtype=jnp.int32)
    local_a = offsets // rows_c
    local_c = offsets % rows_c
    row_ids = (
        (lax.axis_index("grp") * rows_a + local_a) * grid_c
        + lax.axis_index("col") * rows_c
        + local_c
    )
    row_cols = col_table[row_ids]
    left_blocks = x_blocks.reshape(local_rows, KB, B, B)
    along_col = padded(x_blocks, (("col", 1),), 1)
    near_x = padded(along_col, (("grp", 0),), 1)
    square = block_terms(
        near_x,
        local_a + 1,
        local_c + 1,
        row_ids,
        row_cols,
        left_blocks,
        col_table,
        filt_table[row_ids],
        grid_a,
        grid_c,
    ).astype(jnp.bfloat16)
    square = square.reshape(rows_a, rows_c, KF, B, B)
    square_along = padded(square, (("col", 1),), 1)
    near_square = padded(square_along, (("grp", 0),), 1)
    cubed = block_terms(
        near_square,
        local_a + 1,
        local_c + 1,
        row_ids,
        row_cols,
        left_blocks,
        filt_table,
        row_cols,
        grid_a,
        grid_c,
    )
    in_use = (row_cols >= 0).astype(jnp.float32)
    result = (1.5 * left_blocks.astype(jnp.float32) - cubed * (0.5 / (KB * B))) * in_use[
        :, :, None, None
    ]
    return result.astype(jnp.bfloat16).reshape(x_blocks.shape)


LANES = 128
LISTS = 8
CODE_AT = 0
NEAR_AT = 48
SRC_AT = 96
TABLE_ROWS = 16


def index_kernel(cols_ref, filt_ref, table_ref, level_ref, own_ref, halo_ref, move_ref,
                 cols_s, filt_s):
    grp = lax.axis_index("grp")
    col = lax.axis_index("col")
    core = lax.rem(grp, 2)
    grid_c = cols_ref.shape[1]
    grid_a = cols_ref.shape[2]
    chip = 2 * RA

    def lanes_of(x):
        return jnp.concatenate([x] * (LANES // grid_a), axis=1)

    stored, kept = [], []
    for m in range(KB):
        stored.append(lanes_of(cols_ref[m]))
        kept.append(lanes_of(filt_ref[m]))
        cols_s[m] = stored[m]
        filt_s[m] = kept[m]
    shape = (grid_c, LANES)
    lane = lax.broadcasted_iota(jnp.int32, shape, 1)
    ids = lax.rem(lane, grid_a) * grid_c + lax.broadcasted_iota(jnp.int32, shape, 0)
    in_chip = lax.rem(lane, chip)
    first, last = in_chip == 0, in_chip == chip - 1
    false = jnp.zeros(shape, jnp.int32)

    def either(tests):
        got = tests[0]
        for t in tests[1:]:
            got = got | t
        return got

    totals = []
    for d, step_c in enumerate((1, -1)):
        cols_c = [jnp.roll(x, -step_c, 0) for x in stored]
        filt_c = [jnp.roll(x, -step_c, 0) for x in kept]
        found = []
        for step_a in (-1, 0, 1):
            shift = (-step_a) % LANES
            cols_r = [pltpu.roll(x, shift, 1) if shift else x for x in cols_c]
            filt_r = [pltpu.roll(x, shift, 1) if shift else x for x in filt_c]
            member = either([x == ids for x in cols_r])
            one = [either([stored[m] == x for x in filt_r]) & member & (stored[m] >= 0) for m in range(KB)]
            two = [either([kept[m] == x for x in cols_r]) & member for m in range(KB)]
            found.append((one, two))
        up, mid, down = found
        for phase in (0, 1):
            own_row, halo_row = false, false
            flags = []
            for m in range(KB):
                u, c, w = up[phase][m], mid[phase][m], down[phase][m]
                own = (c | (u & ~first) | (w & ~last)).astype(jnp.int32)
                halo = ((u & first) | (w & last)).astype(jnp.int32)
                flags.append((own, halo))
                own_row = own_row + own
                halo_row = halo_row + halo
            totals.append((phase, d, flags, own_row, halo_row))

    def summed(x, rule):
        at = lax.broadcasted_iota(jnp.int32, (LANES, LANES), 0)
        to = lax.broadcasted_iota(jnp.int32, (LANES, LANES), 1)
        weight = rule(at, to).astype(jnp.float32).astype(jnp.bfloat16)
        return jnp.dot(
            x.astype(jnp.float32).astype(jnp.bfloat16), weight, preferred_element_type=jnp.float32
        ).astype(jnp.int32)

    def same_chip(at, to):
        return (at // chip == lax.rem(to, grid_a) // chip) & (at < grid_a)

    def beside(at, to):
        z = lax.rem(to, grid_a) // chip * chip
        above = lax.rem(z + grid_a - 1, grid_a)
        below = lax.rem(z + chip, grid_a)
        return (at == above) | (at == below)

    def stack(xs):
        return jnp.concatenate(xs, axis=0)

    loads = summed(stack([t[3] for t in totals]), same_chip) + summed(
        stack([t[4] for t in totals]), beside
    )

    def across(x):
        return jnp.where(last, pltpu.roll(x, LANES - 1, 1), pltpu.roll(x, 1, 1))

    kept_own, kept_halo, got0, got1 = [], [], [], []
    for p, (phase, d, flags, _, _) in enumerate(totals):
        load = loads[p * grid_c : (p + 1) * grid_c]
        lead = jnp.where(last, load - across(load), across(load) - load)
        far = jnp.abs(lead)
        count = jnp.zeros(shape, jnp.int32)
        for step in range(RELAY):
            count = count + (far >= 3 * step + 2).astype(jnp.int32)
        ups = (lead > 0).astype(jnp.int32)
        rim = (first | last).astype(jnp.int32)
        both = [own * halo * rim for own, halo in flags]
        lower = [jnp.where(last, own, halo) for own, halo in flags]
        upper = [jnp.where(last, halo, own) for own, halo in flags]
        single = [
            jnp.where(ups > 0, lower[m], upper[m]) * rim - both[m] for m in range(KB)
        ]
        n_both = sum(both[1:], both[0])
        n_single = sum(single[1:], single[0])
        both_rank = jnp.where(last, 0, across(n_both))
        single_rank = n_both + across(n_both) + jnp.where(last, 0, across(n_single))
        own_row, halo_row, moved_row = false, false, false
        for m in range(KB):
            rank = jnp.where(both[m] > 0, both_rank, single_rank)
            moved = ((both[m] + single[m]) > 0) & (rank < count)
            move = jnp.where(moved, rank + 1 + 8 * ups, 0)
            both_rank = both_rank + both[m]
            single_rank = single_rank + single[m]
            own = jnp.where(moved, 0, flags[m][0])
            halo = jnp.where(moved, 0, flags[m][1])
            own_ref[phase, d, m] = own
            halo_ref[phase, d, m] = halo
            move_ref[phase, d, m] = move
            own_row, halo_row = own_row + own, halo_row + halo
            moved_row = moved_row + moved.astype(jnp.int32)
        moved_row = moved_row + across(moved_row)
        kept_own.append(own_row)
        kept_halo.append(halo_row)
        got0.append(jnp.where(first, moved_row * ups, 0))
        got1.append(jnp.where(last, moved_row * (1 - ups), 0))

    def split(n0, n1, total, extra0, extra1):
        half = jnp.clip((total + extra1 - extra0 + 1) >> 1, 0, total)
        return half, jnp.maximum(FIRST - n0, 0), jnp.maximum(FIRST - n1, 0)

    own_all = stack(kept_own)
    n0 = summed(own_all, lambda at, to: same_chip(at, to) & (lax.rem(at, chip) < RA))
    n1 = summed(own_all, lambda at, to: same_chip(at, to) & (lax.rem(at, chip) >= RA))
    total = n0 + n1 + summed(stack(kept_halo), beside)
    extra0 = summed(stack(got0), same_chip)
    extra1 = summed(stack(got1), same_chip)
    half, gap0, gap1 = split(n0, n1, total, extra0, extra1)
    rest = total - half
    fill = jnp.maximum(
        half + jnp.where(half > n0, gap0, 0) + extra0,
        rest + jnp.where(rest > n1, gap1, 0) + extra1,
    )
    most = [jnp.int32(FIRST + RELAY), jnp.int32(FIRST + RELAY)]
    for p, (phase, _, _, _, _) in enumerate(totals):
        most[phase] = jnp.maximum(most[phase], jnp.max(fill[p * grid_c : (p + 1) * grid_c]))
    level = jnp.int32(len(LEVELS))
    for at in reversed(range(len(LEVELS))):
        fits = (most[0] <= LEVELS[at][0]) & (most[1] <= LEVELS[at][1])
        level = jnp.where(fits, at, level)
    level_ref[0] = level

    z = grp // 2
    shift = lax.rem(LANES + 1 - z * chip, LANES)
    west = lax.rem(col + grid_c - 1, grid_c)
    east = lax.rem(col + 1, grid_c)
    row8 = (LISTS, LANES)
    lane8 = lax.broadcasted_iota(jnp.int32, row8, 1)
    rim = (lane8 == 0) | (lane8 == CR - 1)
    lists = [(p, d, c) for p in (0, 1) for d, c in ((0, col), (1, col), (0, west), (1, east))]

    def near(ref_rows):
        return pltpu.roll(jnp.concatenate(ref_rows, axis=0), shift, 1)

    need, in_row, stores, moves = [], [], [], []
    run = jnp.zeros(row8, jnp.int32)
    relayed = jnp.zeros(row8, jnp.int32)
    low_end = lane8 <= 1
    for m in range(KB):
        own = near([own_ref[p, d, m, pl.ds(c, 1), :] for p, d, c in lists])
        halo = near([halo_ref[p, d, m, pl.ds(c, 1), :] for p, d, c in lists])
        flags = jnp.where(lane8 < CR, jnp.where(rim, halo, own), 0)
        need.append(flags)
        in_row.append(run)
        run = run + flags
        move = near([move_ref[p, d, m, pl.ds(c, 1), :] for p, d, c in lists])
        move = jnp.where((lane8 <= 1) | ((lane8 >= CR - 2) & (lane8 < CR)), move, 0)
        mine = (move > 0) & ((move > 8) == low_end)
        moves.append((move, mine))
        relayed = relayed + mine.astype(jnp.int32)
        rows = [cols_s[m, pl.ds(c, 1), :] for c in (west, col, east)]
        rows += [filt_s[m, pl.ds(c, 1), :] for c in (west, col, east)]
        stores.append(near(rows + rows[:2]))
    n0 = summed(run, lambda at, to: (at >= 1) & (at <= RA))
    n1 = summed(run, lambda at, to: (at > RA) & (at <= chip))
    above = summed(run, lambda at, to: at == 0)
    below = summed(run, lambda at, to: at == CR - 1)
    ahead = summed(
        run, lambda at, to: (at < to) & (((at >= 1) & (to <= RA)) | ((at > RA) & (to <= chip)))
    )
    total = n0 + n1 + above + below
    extra0 = summed(relayed, lambda at, to: at <= 1)
    extra1 = summed(relayed, lambda at, to: at > 1)
    half, gap0, gap1 = split(n0, n1, total, extra0, extra1)
    east_list = lax.rem(lax.broadcasted_iota(jnp.int32, row8, 0), 4) == 3
    of0 = (lane8 >= 1) & (lane8 <= RA)
    of1 = (lane8 > RA) & (lane8 <= chip)
    slots = lax.broadcasted_iota(jnp.int32, (32, LANES), 0) + core * 32
    entry = lax.broadcasted_iota(jnp.int32, (32, LANES), 1) * KB
    source = [jnp.zeros((32, LANES), jnp.int32) for _ in range(4)]
    codes = []
    for m in range(KB):
        place = ahead + in_row[m]
        place = jnp.where(lane8 == 0, n0 + in_row[m], place)
        place = jnp.where(lane8 == CR - 1, n0 + above + in_row[m], place)
        place = jnp.where(of1, total - 1 - place, place)
        turned = total - 1 - place
        slot0 = place + jnp.where(of0, 0, gap0)
        slot1 = turned + jnp.where(of1, 0, gap1)
        slot0 = slot0 + jnp.where(slot0 >= FIRST, extra0, 0)
        slot1 = slot1 + jnp.where(slot1 >= FIRST, extra1, 0)
        code = jnp.where(place < half, slot0, 32 + slot1)
        move, mine = moves[m]
        rank = (move & 7) - 1
        code = jnp.where(mine, jnp.where(low_end, FIRST, 32 + FIRST) + rank, code)
        code = jnp.where((move > 0) & ~mine, jnp.where(east_list, 96, 128) + rank, code)
        codes.append(code)
        sent = jnp.where((need[m] > 0) | mine, code, -1)
        for i, at in enumerate((0, 1, 4, 5)):
            same = jnp.broadcast_to(sent[at : at + 1], (32, LANES)) == slots
            source[i] = source[i] + jnp.where(same, entry + m, 0)
    lane32 = lax.broadcasted_iota(jnp.int32, (32, LANES), 1)
    out = jnp.zeros((32, LANES), jnp.int32)
    for i in range(4):
        out = jnp.where(lane32 == i, jnp.sum(source[i], axis=1, keepdims=True), out)
    table_ref[...] = jnp.concatenate(codes + stores + [out], axis=0).T[:TABLE_ROWS]


def list_tables(columns, filter_ids):
    grid_a, grid_c, _ = columns.shape
    ints = lambda *shape: pltpu.VMEM(shape, jnp.int32)
    return pl.pallas_call(
        index_kernel,
        out_shape=(
            jax.ShapeDtypeStruct((TABLE_ROWS, LANES), jnp.int32),
            jax.ShapeDtypeStruct((1,), jnp.int32),
        ),
        in_specs=[pl.BlockSpec(memory_space=pltpu.VMEM)] * 2,
        out_specs=(
            pl.BlockSpec(memory_space=pltpu.VMEM),
            pl.BlockSpec(memory_space=pltpu.SMEM),
        ),
        scratch_shapes=[
            ints(2, 2, KB, grid_c, LANES), ints(2, 2, KB, grid_c, LANES),
            ints(2, 2, KB, grid_c, LANES),
            ints(KB, grid_c, LANES), ints(KF, grid_c, LANES),
        ],
        name="block_lists",
    )(columns.transpose(2, 1, 0), filter_ids.transpose(2, 1, 0))


def kernel(q1, q2, grid_a, grid_c, grp_count, col_count, tab, x_hbm, out_ref, acc_ref, late, xv, todo, pick, colp1, rcv1, snd1, colp2, rcv2,
           snd2, sown, lsem, zsem, hs1, hr1, fs1, fr1, hs2, hr2, fs2, fr2, lr2, ysem):
    grp = lax.axis_index("grp")
    col = lax.axis_index("col")
    core = lax.rem(grp, 2)
    partner = (grp + 1 - 2 * core, col)
    zpeer = (lax.rem(grp + grp_count - 1 + 2 * core, grp_count), col)
    right = (grp, lax.rem(col + 1, col_count))
    left = (grp, lax.rem(col + col_count - 1, col_count))
    own0 = (1 + RA * core) * KB
    zout = (RA - 1) * core * KB
    zdst = (CR - 1) * (1 - core) * KB
    zin = (CR - 1) * core * KB

    to_xv = pltpu.make_async_copy(x_hbm, xv, lsem.at[0])
    to_col = pltpu.make_async_copy(x_hbm, colp1.at[pl.ds(own0, OWN)], lsem.at[1])
    to_xv.start()

    barrier = pltpu.get_barrier_semaphore()
    for peer in (partner, zpeer, right, left):
        pl.semaphore_signal(barrier, inc=1, device_id=peer, device_id_type=MESH)
    pl.semaphore_wait(barrier, 4)

    def remote(src, dst, send, recv, device):
        return pltpu.make_async_remote_copy(
            src_ref=src, dst_ref=dst, send_sem=send, recv_sem=recv,
            device_id=device, device_id_type=MESH,
        )

    def zsend(src, colp, p):
        return remote(src.at[pl.ds(zout, KB)], colp.at[pl.ds(zdst, KB)],
                      zsem.at[p, 0], zsem.at[p, 1], zpeer)

    def zfwd(colp, p):
        here = colp.at[pl.ds(zin, KB)]
        return remote(here, here, zsem.at[p, 2], zsem.at[p, 3], partner)

    def share(src, colp, p):
        return remote(src, colp.at[pl.ds(own0, OWN)], zsem.at[p, 4], zsem.at[p, 5], partner)

    def hop(snd, rcv, hs, hr, q, d, s):
        return remote(snd.at[d, s], rcv.at[(2 * d + core) * q + s], hs, hr.at[s],
                      (right, left)[d])

    def fwd(rcv, fs, fr, q, d, s):
        here = rcv.at[(2 * d + core) * q + s]
        return remote(here, here, fs, fr, partner)

    def late_hop(d, i):
        s = q2 - LATE + i
        return remote(snd2.at[d, s], late.at[(2 * d + core) * LATE + i], hs2, hr2.at[s],
                      (right, left)[d])

    def late_fwd(d, i):
        here = late.at[(2 * d + core) * LATE + i]
        return remote(here, here, fs2, lr2, partner)

    def relay(rcv, p, q, d, s):
        rank = s - FIRST
        return remote(rcv.at[(2 * d + core) * q + s], rcv.at[4 * q + d * RELAY + rank],
                      ysem.at[p, 0], ysem.at[p, 1], zpeer)

    def wait_all(like, sem):
        pltpu.make_async_copy(like, like, sem).wait()

    def right_factor(colp, rcv, q, v):
        is_col = v < 64
        at_col = jnp.where(is_col, v, ZERO)
        at_rcv = jnp.where(is_col, 0, v - 64)
        part = at_rcv >> 5
        slot = at_rcv & 31
        direct = jnp.minimum(part, 3) * q + jnp.minimum(slot, q - 1)
        passed = 4 * q + jnp.clip((part - 4) * RELAY + slot, 0, 2 * RELAY - 1)
        return jnp.where(is_col, colp[at_col], rcv[jnp.where(part < 4, direct, passed)])

    def product(colp, rcv, phase, row, entry):
        acc = None
        for k in range(KB):
            v = pick[phase * PICKS + entry * KB + k]
            term = jnp.dot(xv[row * KB + k], right_factor(colp, rcv, (q1, q2 - LATE)[phase], v),
                           preferred_element_type=jnp.float32)
            acc = term if acc is None else acc + term
        return acc

    def sent(phase, d, s):
        return tab[2 * phase + d, SRC_AT + s]

    def list_entry(phase, d, s):
        return jnp.clip(sent(phase, d, s) - own0, 0, OWN - 1)

    def find_factors(at):
        row = at // KB
        k = at - KB * row
        here = 1 + RA * core + row
        source = tab[here, NEAR_AT + 8 * k + 1]
        in_use = source >= 0
        source = jnp.where(in_use, source, 0)
        step_a = lax.rem(source // grid_c - (grp * RA + row) + 1 + grid_a, grid_a) - 1
        side = lax.rem(lax.rem(source, grid_c) - col + 1 + grid_c, grid_c)
        step_a = jnp.where(in_use, jnp.clip(step_a, -1, 1), 0)
        side = jnp.where(in_use, jnp.minimum(side, 2), 1)
        there = here + step_a
        mark_row = lax.broadcasted_iota(jnp.int32, (8, LANES), 0)
        there_at = lax.broadcasted_iota(jnp.int32, (8, LANES), 1) == at
        marks = todo[...]
        for phase in range(2):
            held, spot = [], []
            for m in range(KB):
                held.append(tab[there, NEAR_AT + 8 * m + side + 3 * phase])
                code = tab[there, CODE_AT + 8 * m + 4 * phase + jnp.where(side == 0, 2, 3)]
                far = code + jnp.where(side == 0, 64, 128)
                spot.append(jnp.where(side == 1, there * KB + m, far))
            for f in range(KF):
                wanted = tab[here, NEAR_AT + 8 * f + 1 + 3 * (1 - phase)]
                usable = in_use & (wanted >= 0)
                got = jnp.int32(ZERO)
                for m in range(KB):
                    got = jnp.where(held[m] == wanted, spot[m], got)
                got = jnp.where(usable, got, ZERO)
                if phase:
                    part, slot = (got - 64) >> 5, (got - 64) & 31
                    waits = (got >= 64) & (part < 4) & (slot >= q2 - LATE)
                    code = jnp.clip(part * LATE + slot - (q2 - LATE), 0, 4 * LATE - 1)
                    marks = jnp.where(there_at & (mark_row == f), jnp.where(waits, code, -1), marks)
                    got = jnp.where(waits, ZERO, got)
                pick[phase * PICKS + (row * KB + f) * KB + k] = got
        todo[...] = marks

    zero = jnp.zeros((B, B), jnp.bfloat16)

    zs1, zf1, sh1 = zsend(xv, colp1, 0), zfwd(colp1, 0), share(xv, colp1, 0)
    to_xv.wait()
    zs1.start()
    to_col.start()
    sh1.start()
    hop1 = functools.partial(hop, snd1, rcv1, hs1, hr1, q1)
    fwd1 = functools.partial(fwd, rcv1, fs1, fr1, q1)
    pass1 = functools.partial(relay, rcv1, 0, q1)

    @pl.loop(0, FIRST)
    def _(s):
        for d in range(2):
            snd1[d, s] = xv[list_entry(0, d, s)]

        @pl.when(s > 0)
        def _():
            for d in range(2):
                hop1(d, s - 1).start()

    colp1[ZERO] = zero
    colp2[ZERO] = zero
    for d in range(2):
        hop1(d, FIRST - 1).start()
    to_col.wait()
    zs1.wait_recv()
    zf1.start()
    sh1.wait_recv()
    zf1.wait_recv()

    @pl.loop(FIRST, q1)
    def _(s):
        for d in range(2):
            snd1[d, s] = colp1[sent(0, d, s)]

        @pl.when(s > FIRST)
        def _():
            for d in range(2):
                hop1(d, s - 1).start()

    for d in range(2):
        hop1(d, q1 - 1).start()

    todo[...] = jnp.full((8, LANES), -1, jnp.int32)
    pl.loop(0, OWN)(find_factors)

    @pl.loop(0, q1)
    def _(s):
        wait_all(rcv1.at[pl.ds(0, 2)], hr1.at[s])
        for d in range(2):
            fwd1(d, s).start()

        @pl.when((s >= FIRST) & (s < FIRST + RELAY))
        def _():
            for d in range(2):
                pass1(d, s).start()

    wait_all(snd1, fr1)
    wait_all(rcv1.at[pl.ds(0, 2 * RELAY)], ysem.at[0, 1])

    zs2, zf2, sh2 = zsend(sown, colp2, 1), zfwd(colp2, 1), share(sown, colp2, 1)
    hop2 = functools.partial(hop, snd2, rcv2, hs2, hr2, q2 - LATE)
    fwd2 = functools.partial(fwd, rcv2, fs2, fr2, q2 - LATE)
    pass2 = functools.partial(relay, rcv2, 1, q2 - LATE)

    @pl.loop(0, 3 + OWN // 2)
    def _(t):
        listed = (t == 0) | (t == 4) | (t == 5)
        slot = jnp.where(listed, jnp.maximum(t - 3, 0), 0)
        at = jnp.where(listed, 3, jnp.where(t < 4, t - 1, t - 3))
        step = at // 3

        @pl.when(t == 4)
        def _():
            zs2.start()

        row = step + core * (RA - 1 - 2 * step)
        for d in range(2):
            own_entry = row * KB + (at - 3 * step) * 2 + d
            entry = jnp.where(listed, list_entry(1, d, slot), own_entry)
            block = product(colp1, rcv1, 0, entry // KB, entry).astype(jnp.bfloat16)
            snd2[d, jnp.where(listed, slot, q2 - 1)] = block
            sown[own_entry] = block
            colp2[own0 + own_entry] = block

        @pl.when(listed)
        def _():
            hop2(0, slot).start()

        @pl.when(t == 1)
        def _():
            hop2(1, 0).start()

        @pl.when((t == 5) | (t == 6))
        def _():
            hop2(1, t - 4).start()

    @pl.loop(3, FIRST)
    def _(s):
        for d in range(2):
            snd2[d, s] = sown[list_entry(1, d, s)]

        @pl.when(s > 3)
        def _():
            for d in range(2):
                hop2(d, s - 1).start()

    sh2.start()
    for d in range(2):
        hop2(d, FIRST - 1).start()
    zs2.wait_recv()
    zf2.start()
    sh2.wait_recv()
    zf2.wait_recv()

    @pl.loop(FIRST, q2 - LATE)
    def _(s):
        for d in range(2):
            snd2[d, s] = colp2[sent(1, d, s)]

        @pl.when(s > FIRST)
        def _():
            for d in range(2):
                hop2(d, s - 1).start()

    for i in range(LATE):
        s = q2 - LATE + i
        for d in range(2):
            snd2[d, s] = colp2[sent(1, d, s)]
        for d in range(2):
            (late_hop(d, i - 1) if i else hop2(d, s - 1)).start()
    for d in range(2):
        late_hop(d, LATE - 1).start()

    @pl.loop(0, q2 - LATE)
    def _(s):
        wait_all(rcv2.at[pl.ds(0, 2)], hr2.at[s])
        for d in range(2):
            fwd2(d, s).start()

        @pl.when((s >= FIRST) & (s < FIRST + RELAY))
        def _():
            for d in range(2):
                pass2(d, s).start()

    wait_all(rcv2.at[pl.ds(0, 2 * (q2 - LATE))], fr2)
    wait_all(rcv2.at[pl.ds(0, 2 * RELAY)], ysem.at[1, 1])

    def pass_late(i):
        wait_all(rcv2.at[pl.ds(0, 2)], hr2.at[q2 - LATE + i])
        for d in range(2):
            late_fwd(d, i).start()

    @pl.loop(0, OWN // 2)
    def _(t):
        row = t // 3
        for u in range(2):
            entry = 2 * t + u
            cubed = product(colp2, rcv2, 1, row, entry)
            in_use = tab[1 + RA * core + row, NEAR_AT + 8 * (entry - row * KB) + 1] >= 0
            own = xv[entry].astype(jnp.float32)
            step = 1.5 * own - cubed * (0.5 / (KB * B))
            out_ref[entry] = jnp.where(in_use, step, 0.0).astype(jnp.bfloat16)
            acc_ref[entry] = cubed

        for i, when in enumerate((5, 11)):

            @pl.when(t == when)
            def _():
                pass_late(i)

    pass_late(2)

    wait_all(late.at[pl.ds(0, 2 * LATE)], lr2)
    zs1.wait_send()
    zf1.wait_send()
    sh1.wait_send()
    zs2.wait_send()
    zf2.wait_send()
    sh2.wait_send()
    for snd, rcv, hs, fs, p in ((snd1, rcv1, hs1, fs1, 0), (snd2, rcv2, hs2, fs2, 1)):
        wait_all(snd, hs)
        wait_all(snd, fs)
        wait_all(rcv.at[pl.ds(0, 2 * RELAY)], ysem.at[p, 0])


def sparse(level, grid_a, grid_c, x_blocks, table):
    q1, q2 = LEVELS[level]
    blocks = x_blocks.reshape(OWN, B, B)
    vm = lambda *lead: pltpu.VMEM((*lead, B, B), jnp.bfloat16)
    dma = lambda *lead: pltpu.SemaphoreType.DMA(lead)
    held = OWN + 2 * COLN + 2 + 6 * (q1 + q2) + 4 * RELAY + 16
    out, acc, late, xv, todo = pl.pallas_call(
        functools.partial(kernel, q1, q2, grid_a, grid_c, lax.axis_size("grp"), lax.axis_size("col")),
        out_shape=(
            pltpu.VMEM(blocks.shape, jnp.bfloat16),
            pltpu.VMEM(blocks.shape, jnp.float32),
            pltpu.VMEM((4 * LATE, B, B), jnp.bfloat16),
            pltpu.VMEM(blocks.shape, jnp.bfloat16),
            pltpu.VMEM((8, LANES), jnp.int32),
        ),
        in_specs=[
            pl.BlockSpec(memory_space=pltpu.SMEM),
            pl.BlockSpec(memory_space=pl.ANY),
        ],
        out_specs=tuple(pl.BlockSpec(memory_space=pltpu.VMEM) for _ in range(5)),
        scratch_shapes=[
            pltpu.SMEM((2 * PICKS,), jnp.int32),
            vm(COLN + 1), vm(4 * q1 + 2 * RELAY), vm(2, q1), vm(COLN + 1),
            vm(4 * (q2 - LATE) + 2 * RELAY), vm(2, q2), vm(OWN),
            dma(2), dma(2, 6),
            dma(), dma(q1), dma(), dma(), dma(), dma(q2), dma(), dma(), dma(), dma(2, 2),
        ],
        compiler_params=pltpu.CompilerParams(
            collective_id=level, has_side_effects=True, vmem_limit_bytes=held * B * B * 2
        ),
        name=f"sign_step_{q1}_{q2}",
    )(table, blocks)
    return finished(todo, out, acc, late, xv).reshape(x_blocks.shape)


def finish_kernel(todo, out_ref, acc_ref, late, xv, res, some, total, fixed, sem):
    def write(src, entry):
        return pltpu.make_async_copy(src.at[entry], res.at[entry], sem)

    @pl.loop(0, KF)
    def _(f):
        for row in range(RA):
            entry = row * KB + f
            latest = todo[f, row * KB]
            for k in range(1, KB):
                latest = jnp.maximum(latest, todo[f, row * KB + k])
            some[entry] = latest

            @pl.when(latest < 0)
            def _():
                write(out_ref, entry).start()

    @pl.loop(0, OWN)
    def _(entry):
        @pl.when(some[entry] >= 0)
        def _():
            row, f = entry // KB, entry % KB
            total[...] = acc_ref[entry]
            for k in range(KB):
                code = todo[f, row * KB + k]

                @pl.when(code >= 0)
                def _():
                    total[...] += jnp.dot(
                        xv[row * KB + k],
                        late[jnp.clip(code, 0, 4 * LATE - 1)],
                        preferred_element_type=jnp.float32,
                    )

            own = xv[entry].astype(jnp.float32)
            fixed[entry] = (1.5 * own - total[...] * (0.5 / (KB * B))).astype(jnp.bfloat16)

    @pl.loop(0, OWN)
    def _(entry):
        @pl.when(some[entry] >= 0)
        def _():
            write(fixed, entry).start()

    pltpu.make_async_copy(out_ref, res, sem).wait()


def finished(todo, out, acc, late, xv):
    return pl.pallas_call(
        finish_kernel,
        out_shape=jax.ShapeDtypeStruct(out.shape, out.dtype),
        in_specs=[pl.BlockSpec(memory_space=pltpu.SMEM)]
        + [pl.BlockSpec(memory_space=pltpu.VMEM)] * 4,
        out_specs=pl.BlockSpec(memory_space=pl.ANY),
        scratch_shapes=[
            pltpu.SMEM((OWN,), jnp.int32),
            pltpu.VMEM((B, B), jnp.float32),
            pltpu.VMEM(out.shape, out.dtype),
            pltpu.SemaphoreType.DMA(()),
        ],
        compiler_params=pltpu.CompilerParams(vmem_limit_bytes=20 * 1024 * 1024),
        name="finish",
    )(todo, out, acc, late, xv)


def local(x_blocks, columns, filter_ids):
    grid_a, grid_c, _ = columns.shape
    table, level = list_tables(columns, filter_ids)
    branches = [
        functools.partial(lambda at, x, c, f, t: sparse(at, grid_a, grid_c, x, t), at)
        for at in range(len(LEVELS))
    ]
    branches.append(lambda x, c, f, t: dense(x, c, f))
    return lax.switch(level[0], branches, x_blocks, columns, filter_ids, table)


def solution(mesh):
    return jax.shard_map(
        local,
        mesh=mesh,
        in_specs=(P("grp", "col", None, None, None), P(), P()),
        out_specs=P("grp", "col", None, None, None),
        check_vma=False,
    )
```

```python
import functools

import jax
import jax.numpy as jnp
from jax import lax
from jax.experimental import pallas as pl
from jax.experimental.pallas import tpu as pltpu
from jax.sharding import PartitionSpec as P

B = 256
KB = 6
KF = 6
RA = 4
OWN = RA * KB
CR = 2 * RA + 2
COLN = CR * KB
ZERO = COLN
FIRST = 6
LATE = 2
RELAY = 4
LEVELS = ((11, 13), (12, 13), (11, 14), (12, 14), (13, 15), (15, 18))

PICKS = OWN * KB
MESH = pl.DeviceIdType.MESH


def padded(cells, sides, width):
    for axis, dim in sides:
        count = lax.axis_size(axis)
        head = lax.slice_in_dim(cells, 0, width, axis=dim)
        tail = lax.slice_in_dim(cells, cells.shape[dim] - width, cells.shape[dim], axis=dim)
        cells = jnp.concatenate(
            [
                lax.ppermute(tail, axis, [(i, (i + 1) % count) for i in range(count)]),
                cells,
                lax.ppermute(head, axis, [((i + 1) % count, i) for i in range(count)]),
            ],
            axis=dim,
        )
    return cells


def block_terms(
    halo, pos_a, pos_c, row_ids, row_cols, left_blocks, stored_table, wanted, grid_a, grid_c
):
    slot_count = halo.shape[2]
    width = halo.shape[3]
    in_use = row_cols >= 0
    source = jnp.where(in_use, row_cols, 0)
    home_a = row_ids // grid_c
    home_c = row_ids % grid_c
    step_a = (source // grid_c - home_a[:, None] + 1) % grid_a - 1
    step_c = (source % grid_c - home_c[:, None] + 1) % grid_c - 1
    place = (pos_a[:, None] + step_a) * halo.shape[1] + pos_c[:, None] + step_c
    flat = halo.reshape((halo.shape[0] * halo.shape[1] * slot_count, width, width))
    stored = stored_table[source]
    matches = stored[:, :, None, :] == wanted[:, None, :, None]
    present = jnp.any(matches, axis=3) & (wanted[:, None, :] >= 0) & in_use[:, :, None]
    slot_of = jnp.argmax(matches.astype(jnp.int32), axis=3)
    block_index = place[:, :, None] * slot_count + slot_of

    def one_row(inputs):
        index_row, present_row, left_row = inputs
        picked = flat[index_row]
        picked = jnp.where(present_row[:, :, None, None], picked, jnp.zeros((), picked.dtype))
        return jnp.einsum("kab,kfbc->fac", left_row, picked, preferred_element_type=jnp.float32)

    return lax.map(one_row, (block_index, present, left_blocks))


def dense(x_blocks, columns, filter_ids):
    grp_count = lax.axis_size("grp")
    col_count = lax.axis_size("col")
    rows_a = x_blocks.shape[0]
    rows_c = x_blocks.shape[1]
    grid_a = rows_a * grp_count
    grid_c = rows_c * col_count
    col_table = columns.reshape(grid_a * grid_c, KB)
    filt_table = filter_ids.reshape(grid_a * grid_c, KF)
    local_rows = rows_a * rows_c
    offsets = jnp.arange(local_rows, dtype=jnp.int32)
    local_a = offsets // rows_c
    local_c = offsets % rows_c
    row_ids = (
        (lax.axis_index("grp") * rows_a + local_a) * grid_c
        + lax.axis_index("col") * rows_c
        + local_c
    )
    row_cols = col_table[row_ids]
    left_blocks = x_blocks.reshape(local_rows, KB, B, B)
    along_col = padded(x_blocks, (("col", 1),), 1)
    near_x = padded(along_col, (("grp", 0),), 1)
    square = block_terms(
        near_x,
        local_a + 1,
        local_c + 1,
        row_ids,
        row_cols,
        left_blocks,
        col_table,
        filt_table[row_ids],
        grid_a,
        grid_c,
    ).astype(jnp.bfloat16)
    square = square.reshape(rows_a, rows_c, KF, B, B)
    square_along = padded(square, (("col", 1),), 1)
    near_square = padded(square_along, (("grp", 0),), 1)
    cubed = block_terms(
        near_square,
        local_a + 1,
        local_c + 1,
        row_ids,
        row_cols,
        left_blocks,
        filt_table,
        row_cols,
        grid_a,
        grid_c,
    )
    in_use = (row_cols >= 0).astype(jnp.float32)
    result = (1.5 * left_blocks.astype(jnp.float32) - cubed * (0.5 / (KB * B))) * in_use[
        :, :, None, None
    ]
    return result.astype(jnp.bfloat16).reshape(x_blocks.shape)


LANES = 128
LISTS = 8
CODE_AT = 0
NEAR_AT = 48
SRC_AT = 96
TABLE_ROWS = 16


def index_kernel(cols_ref, filt_ref, table_ref, level_ref, own_ref, halo_ref, move_ref,
                 cols_s, filt_s):
    grp = lax.axis_index("grp")
    col = lax.axis_index("col")
    core = lax.rem(grp, 2)
    grid_c = cols_ref.shape[1]
    grid_a = cols_ref.shape[2]
    chip = 2 * RA

    def lanes_of(x):
        return jnp.concatenate([x] * (LANES // grid_a), axis=1)

    stored, kept = [], []
    for m in range(KB):
        stored.append(lanes_of(cols_ref[m]))
        kept.append(lanes_of(filt_ref[m]))
        cols_s[m] = stored[m]
        filt_s[m] = kept[m]
    shape = (grid_c, LANES)
    lane = lax.broadcasted_iota(jnp.int32, shape, 1)
    ids = lax.rem(lane, grid_a) * grid_c + lax.broadcasted_iota(jnp.int32, shape, 0)
    in_chip = lax.rem(lane, chip)
    first, last = in_chip == 0, in_chip == chip - 1
    false = jnp.zeros(shape, jnp.int32)

    def either(tests):
        got = tests[0]
        for t in tests[1:]:
            got = got | t
        return got

    totals = []
    for d, step_c in enumerate((1, -1)):
        cols_c = [jnp.roll(x, -step_c, 0) for x in stored]
        filt_c = [jnp.roll(x, -step_c, 0) for x in kept]
        found = []
        for step_a in (-1, 0, 1):
            shift = (-step_a) % LANES
            cols_r = [pltpu.roll(x, shift, 1) if shift else x for x in cols_c]
            filt_r = [pltpu.roll(x, shift, 1) if shift else x for x in filt_c]
            member = either([x == ids for x in cols_r])
            one = [either([stored[m] == x for x in filt_r]) & member & (stored[m] >= 0) for m in range(KB)]
            two = [either([kept[m] == x for x in cols_r]) & member for m in range(KB)]
            found.append((one, two))
        up, mid, down = found
        for phase in (0, 1):
            own_row, halo_row = false, false
            flags = []
            for m in range(KB):
                u, c, w = up[phase][m], mid[phase][m], down[phase][m]
                own = (c | (u & ~first) | (w & ~last)).astype(jnp.int32)
                halo = ((u & first) | (w & last)).astype(jnp.int32)
                flags.append((own, halo))
                own_row = own_row + own
                halo_row = halo_row + halo
            totals.append((phase, d, flags, own_row, halo_row))

    def summed(x, rule):
        at = lax.broadcasted_iota(jnp.int32, (LANES, LANES), 0)
        to = lax.broadcasted_iota(jnp.int32, (LANES, LANES), 1)
        weight = rule(at, to).astype(jnp.float32).astype(jnp.bfloat16)
        return jnp.dot(
            x.astype(jnp.float32).astype(jnp.bfloat16), weight, preferred_element_type=jnp.float32
        ).astype(jnp.int32)

    def same_chip(at, to):
        return (at // chip == lax.rem(to, grid_a) // chip) & (at < grid_a)

    def beside(at, to):
        z = lax.rem(to, grid_a) // chip * chip
        above = lax.rem(z + grid_a - 1, grid_a)
        below = lax.rem(z + chip, grid_a)
        return (at == above) | (at == below)

    def stack(xs):
        return jnp.concatenate(xs, axis=0)

    loads = summed(stack([t[3] for t in totals]), same_chip) + summed(
        stack([t[4] for t in totals]), beside
    )

    def across(x):
        return jnp.where(last, pltpu.roll(x, LANES - 1, 1), pltpu.roll(x, 1, 1))

    kept_own, kept_halo, got0, got1 = [], [], [], []
    for p, (phase, d, flags, _, _) in enumerate(totals):
        load = loads[p * grid_c : (p + 1) * grid_c]
        lead = jnp.where(last, load - across(load), across(load) - load)
        far = jnp.abs(lead)
        count = jnp.zeros(shape, jnp.int32)
        for step in range(RELAY):
            count = count + (far >= 3 * step + 2).astype(jnp.int32)
        ups = (lead > 0).astype(jnp.int32)
        rim = (first | last).astype(jnp.int32)
        both = [own * halo * rim for own, halo in flags]
        lower = [jnp.where(last, own, halo) for own, halo in flags]
        upper = [jnp.where(last, halo, own) for own, halo in flags]
        single = [
            jnp.where(ups > 0, lower[m], upper[m]) * rim - both[m] for m in range(KB)
        ]
        n_both = sum(both[1:], both[0])
        n_single = sum(single[1:], single[0])
        both_rank = jnp.where(last, 0, across(n_both))
        single_rank = n_both + across(n_both) + jnp.where(last, 0, across(n_single))
        own_row, halo_row, moved_row = false, false, false
        for m in range(KB):
            rank = jnp.where(both[m] > 0, both_rank, single_rank)
            moved = ((both[m] + single[m]) > 0) & (rank < count)
            move = jnp.where(moved, rank + 1 + 8 * ups, 0)
            both_rank = both_rank + both[m]
            single_rank = single_rank + single[m]
            own = jnp.where(moved, 0, flags[m][0])
            halo = jnp.where(moved, 0, flags[m][1])
            own_ref[phase, d, m] = own
            halo_ref[phase, d, m] = halo
            move_ref[phase, d, m] = move
            own_row, halo_row = own_row + own, halo_row + halo
            moved_row = moved_row + moved.astype(jnp.int32)
        moved_row = moved_row + across(moved_row)
        kept_own.append(own_row)
        kept_halo.append(halo_row)
        got0.append(jnp.where(first, moved_row * ups, 0))
        got1.append(jnp.where(last, moved_row * (1 - ups), 0))

    def split(n0, n1, total, extra0, extra1):
        half = jnp.clip((total + extra1 - extra0 + 1) >> 1, 0, total)
        return half, jnp.maximum(FIRST - n0, 0), jnp.maximum(FIRST - n1, 0)

    own_all = stack(kept_own)
    n0 = summed(own_all, lambda at, to: same_chip(at, to) & (lax.rem(at, chip) < RA))
    n1 = summed(own_all, lambda at, to: same_chip(at, to) & (lax.rem(at, chip) >= RA))
    total = n0 + n1 + summed(stack(kept_halo), beside)
    extra0 = summed(stack(got0), same_chip)
    extra1 = summed(stack(got1), same_chip)
    half, gap0, gap1 = split(n0, n1, total, extra0, extra1)
    rest = total - half
    fill = jnp.maximum(
        half + jnp.where(half > n0, gap0, 0) + extra0,
        rest + jnp.where(rest > n1, gap1, 0) + extra1,
    )
    most = [jnp.int32(FIRST + RELAY), jnp.int32(FIRST + RELAY)]
    for p, (phase, _, _, _, _) in enumerate(totals):
        most[phase] = jnp.maximum(most[phase], jnp.max(fill[p * grid_c : (p + 1) * grid_c]))
    level = jnp.int32(len(LEVELS))
    for at in reversed(range(len(LEVELS))):
        fits = (most[0] <= LEVELS[at][0]) & (most[1] <= LEVELS[at][1])
        level = jnp.where(fits, at, level)
    level_ref[0] = level

    z = grp // 2
    shift = lax.rem(LANES + 1 - z * chip, LANES)
    west = lax.rem(col + grid_c - 1, grid_c)
    east = lax.rem(col + 1, grid_c)
    row8 = (LISTS, LANES)
    lane8 = lax.broadcasted_iota(jnp.int32, row8, 1)
    rim = (lane8 == 0) | (lane8 == CR - 1)
    lists = [(p, d, c) for p in (0, 1) for d, c in ((0, col), (1, col), (0, west), (1, east))]

    def near(ref_rows):
        return pltpu.roll(jnp.concatenate(ref_rows, axis=0), shift, 1)

    need, in_row, stores, moves = [], [], [], []
    run = jnp.zeros(row8, jnp.int32)
    relayed = jnp.zeros(row8, jnp.int32)
    low_end = lane8 <= 1
    for m in range(KB):
        own = near([own_ref[p, d, m, pl.ds(c, 1), :] for p, d, c in lists])
        halo = near([halo_ref[p, d, m, pl.ds(c, 1), :] for p, d, c in lists])
        flags = jnp.where(lane8 < CR, jnp.where(rim, halo, own), 0)
        need.append(flags)
        in_row.append(run)
        run = run + flags
        move = near([move_ref[p, d, m, pl.ds(c, 1), :] for p, d, c in lists])
        move = jnp.where((lane8 <= 1) | ((lane8 >= CR - 2) & (lane8 < CR)), move, 0)
        mine = (move > 0) & ((move > 8) == low_end)
        moves.append((move, mine))
        relayed = relayed + mine.astype(jnp.int32)
        rows = [cols_s[m, pl.ds(c, 1), :] for c in (west, col, east)]
        rows += [filt_s[m, pl.ds(c, 1), :] for c in (west, col, east)]
        stores.append(near(rows + rows[:2]))
    n0 = summed(run, lambda at, to: (at >= 1) & (at <= RA))
    n1 = summed(run, lambda at, to: (at > RA) & (at <= chip))
    above = summed(run, lambda at, to: at == 0)
    below = summed(run, lambda at, to: at == CR - 1)
    ahead = summed(
        run, lambda at, to: (at < to) & (((at >= 1) & (to <= RA)) | ((at > RA) & (to <= chip)))
    )
    total = n0 + n1 + above + below
    extra0 = summed(relayed, lambda at, to: at <= 1)
    extra1 = summed(relayed, lambda at, to: at > 1)
    half, gap0, gap1 = split(n0, n1, total, extra0, extra1)
    east_list = lax.rem(lax.broadcasted_iota(jnp.int32, row8, 0), 4) == 3
    of0 = (lane8 >= 1) & (lane8 <= RA)
    of1 = (lane8 > RA) & (lane8 <= chip)
    slots = lax.broadcasted_iota(jnp.int32, (32, LANES), 0) + core * 32
    entry = lax.broadcasted_iota(jnp.int32, (32, LANES), 1) * KB
    source = [jnp.zeros((32, LANES), jnp.int32) for _ in range(4)]
    codes = []
    for m in range(KB):
        place = ahead + in_row[m]
        place = jnp.where(lane8 == 0, n0 + in_row[m], place)
        place = jnp.where(lane8 == CR - 1, n0 + above + in_row[m], place)
        place = jnp.where(of1, total - 1 - place, place)
        turned = total - 1 - place
        slot0 = place + jnp.where(of0, 0, gap0)
        slot1 = turned + jnp.where(of1, 0, gap1)
        slot0 = slot0 + jnp.where(slot0 >= FIRST, extra0, 0)
        slot1 = slot1 + jnp.where(slot1 >= FIRST, extra1, 0)
        code = jnp.where(place < half, slot0, 32 + slot1)
        move, mine = moves[m]
        rank = (move & 7) - 1
        code = jnp.where(mine, jnp.where(low_end, FIRST, 32 + FIRST) + rank, code)
        code = jnp.where((move > 0) & ~mine, jnp.where(east_list, 96, 128) + rank, code)
        codes.append(code)
        sent = jnp.where((need[m] > 0) | mine, code, -1)
        for i, at in enumerate((0, 1, 4, 5)):
            same = jnp.broadcast_to(sent[at : at + 1], (32, LANES)) == slots
            source[i] = source[i] + jnp.where(same, entry + m, 0)
    lane32 = lax.broadcasted_iota(jnp.int32, (32, LANES), 1)
    out = jnp.zeros((32, LANES), jnp.int32)
    for i in range(4):
        out = jnp.where(lane32 == i, jnp.sum(source[i], axis=1, keepdims=True), out)
    table_ref[...] = jnp.concatenate(codes + stores + [out], axis=0).T[:TABLE_ROWS]


def list_tables(columns, filter_ids):
    grid_a, grid_c, _ = columns.shape
    ints = lambda *shape: pltpu.VMEM(shape, jnp.int32)
    return pl.pallas_call(
        index_kernel,
        out_shape=(
            jax.ShapeDtypeStruct((TABLE_ROWS, LANES), jnp.int32),
            jax.ShapeDtypeStruct((1,), jnp.int32),
        ),
        in_specs=[pl.BlockSpec(memory_space=pltpu.VMEM)] * 2,
        out_specs=(
            pl.BlockSpec(memory_space=pltpu.VMEM),
            pl.BlockSpec(memory_space=pltpu.SMEM),
        ),
        scratch_shapes=[
            ints(2, 2, KB, grid_c, LANES), ints(2, 2, KB, grid_c, LANES),
            ints(2, 2, KB, grid_c, LANES),
            ints(KB, grid_c, LANES), ints(KF, grid_c, LANES),
        ],
        name="block_lists",
    )(columns.transpose(2, 1, 0), filter_ids.transpose(2, 1, 0))


def kernel(q1, q2, grid_a, grid_c, grp_count, col_count, tab, x_hbm, out_ref, acc_ref, late, xv, todo, pick, colp1, rcv1, snd1, colp2, rcv2,
           snd2, sown, lsem, zsem, hs1, hr1, fs1, fr1, hs2, hr2, fs2, fr2, lr2, ysem):
    grp = lax.axis_index("grp")
    col = lax.axis_index("col")
    core = lax.rem(grp, 2)
    partner = (grp + 1 - 2 * core, col)
    zpeer = (lax.rem(grp + grp_count - 1 + 2 * core, grp_count), col)
    right = (grp, lax.rem(col + 1, col_count))
    left = (grp, lax.rem(col + col_count - 1, col_count))
    own0 = (1 + RA * core) * KB
    zout = (RA - 1) * core * KB
    zdst = (CR - 1) * (1 - core) * KB
    zin = (CR - 1) * core * KB

    to_xv = pltpu.make_async_copy(x_hbm, xv, lsem.at[0])
    to_col = pltpu.make_async_copy(x_hbm, colp1.at[pl.ds(own0, OWN)], lsem.at[1])
    to_xv.start()

    barrier = pltpu.get_barrier_semaphore()
    for peer in (partner, zpeer, right, left):
        pl.semaphore_signal(barrier, inc=1, device_id=peer, device_id_type=MESH)
    pl.semaphore_wait(barrier, 4)

    def remote(src, dst, send, recv, device):
        return pltpu.make_async_remote_copy(
            src_ref=src, dst_ref=dst, send_sem=send, recv_sem=recv,
            device_id=device, device_id_type=MESH,
        )

    def zsend(src, colp, p):
        return remote(src.at[pl.ds(zout, KB)], colp.at[pl.ds(zdst, KB)],
                      zsem.at[p, 0], zsem.at[p, 1], zpeer)

    def zfwd(colp, p):
        here = colp.at[pl.ds(zin, KB)]
        return remote(here, here, zsem.at[p, 2], zsem.at[p, 3], partner)

    def share(src, colp, p):
        return remote(src, colp.at[pl.ds(own0, OWN)], zsem.at[p, 4], zsem.at[p, 5], partner)

    def hop(snd, rcv, hs, hr, q, d, s):
        return remote(snd.at[d, s], rcv.at[(2 * d + core) * q + s], hs, hr.at[s],
                      (right, left)[d])

    def fwd(rcv, fs, fr, q, d, s):
        here = rcv.at[(2 * d + core) * q + s]
        return remote(here, here, fs, fr, partner)

    def late_hop(d, i):
        s = q2 - LATE + i
        return remote(snd2.at[d, s], late.at[(2 * d + core) * LATE + i], hs2, hr2.at[s],
                      (right, left)[d])

    def late_fwd(d, i):
        here = late.at[(2 * d + core) * LATE + i]
        return remote(here, here, fs2, lr2, partner)

    def relay(rcv, p, q, d, s):
        rank = s - FIRST
        return remote(rcv.at[(2 * d + core) * q + s], rcv.at[4 * q + d * RELAY + rank],
                      ysem.at[p, 0], ysem.at[p, 1], zpeer)

    def wait_all(like, sem):
        pltpu.make_async_copy(like, like, sem).wait()

    def right_factor(colp, rcv, q, v):
        is_col = v < 64
        at_col = jnp.where(is_col, v, ZERO)
        at_rcv = jnp.where(is_col, 0, v - 64)
        part = at_rcv >> 5
        slot = at_rcv & 31
        direct = jnp.minimum(part, 3) * q + jnp.minimum(slot, q - 1)
        passed = 4 * q + jnp.clip((part - 4) * RELAY + slot, 0, 2 * RELAY - 1)
        return jnp.where(is_col, colp[at_col], rcv[jnp.where(part < 4, direct, passed)])

    def product(colp, rcv, phase, row, entry):
        acc = None
        for k in range(KB):
            v = pick[phase * PICKS + entry * KB + k]
            term = jnp.dot(xv[row * KB + k], right_factor(colp, rcv, (q1, q2 - LATE)[phase], v),
                           preferred_element_type=jnp.float32)
            acc = term if acc is None else acc + term
        return acc

    def sent(phase, d, s):
        return tab[2 * phase + d, SRC_AT + s]

    def list_entry(phase, d, s):
        return jnp.clip(sent(phase, d, s) - own0, 0, OWN - 1)

    def find_factors(at):
        row = at // KB
        k = at - KB * row
        here = 1 + RA * core + row
        source = tab[here, NEAR_AT + 8 * k + 1]
        in_use = source >= 0
        source = jnp.where(in_use, source, 0)
        step_a = lax.rem(source // grid_c - (grp * RA + row) + 1 + grid_a, grid_a) - 1
        side = lax.rem(lax.rem(source, grid_c) - col + 1 + grid_c, grid_c)
        step_a = jnp.where(in_use, jnp.clip(step_a, -1, 1), 0)
        side = jnp.where(in_use, jnp.minimum(side, 2), 1)
        there = here + step_a
        mark_row = lax.broadcasted_iota(jnp.int32, (8, LANES), 0)
        there_at = lax.broadcasted_iota(jnp.int32, (8, LANES), 1) == at
        marks = todo[...]
        for phase in range(2):
            held, spot = [], []
            for m in range(KB):
                held.append(tab[there, NEAR_AT + 8 * m + side + 3 * phase])
                code = tab[there, CODE_AT + 8 * m + 4 * phase + jnp.where(side == 0, 2, 3)]
                far = code + jnp.where(side == 0, 64, 128)
                spot.append(jnp.where(side == 1, there * KB + m, far))
            for f in range(KF):
                wanted = tab[here, NEAR_AT + 8 * f + 1 + 3 * (1 - phase)]
                usable = in_use & (wanted >= 0)
                got = jnp.int32(ZERO)
                for m in range(KB):
                    got = jnp.where(held[m] == wanted, spot[m], got)
                got = jnp.where(usable, got, ZERO)
                if phase:
                    part, slot = (got - 64) >> 5, (got - 64) & 31
                    waits = (got >= 64) & (part < 4) & (slot >= q2 - LATE)
                    code = jnp.clip(part * LATE + slot - (q2 - LATE), 0, 4 * LATE - 1)
                    marks = jnp.where(there_at & (mark_row == f), jnp.where(waits, code, -1), marks)
                    got = jnp.where(waits, ZERO, got)
                pick[phase * PICKS + (row * KB + f) * KB + k] = got
        todo[...] = marks

    zero = jnp.zeros((B, B), jnp.bfloat16)

    zs1, zf1, sh1 = zsend(xv, colp1, 0), zfwd(colp1, 0), share(xv, colp1, 0)
    to_xv.wait()
    zs1.start()
    to_col.start()
    sh1.start()
    hop1 = functools.partial(hop, snd1, rcv1, hs1, hr1, q1)
    fwd1 = functools.partial(fwd, rcv1, fs1, fr1, q1)
    pass1 = functools.partial(relay, rcv1, 0, q1)

    @pl.loop(0, FIRST)
    def _(s):
        for d in range(2):
            snd1[d, s] = xv[list_entry(0, d, s)]

        @pl.when(s > 0)
        def _():
            for d in range(2):
                hop1(d, s - 1).start()

    colp1[ZERO] = zero
    colp2[ZERO] = zero
    for d in range(2):
        hop1(d, FIRST - 1).start()
    to_col.wait()
    zs1.wait_recv()
    zf1.start()
    sh1.wait_recv()
    zf1.wait_recv()

    @pl.loop(FIRST, q1)
    def _(s):
        for d in range(2):
            snd1[d, s] = colp1[sent(0, d, s)]

        @pl.when(s > FIRST)
        def _():
            for d in range(2):
                hop1(d, s - 1).start()

    for d in range(2):
        hop1(d, q1 - 1).start()

    todo[...] = jnp.full((8, LANES), -1, jnp.int32)
    pl.loop(0, OWN)(find_factors)

    @pl.loop(0, q1)
    def _(s):
        wait_all(rcv1.at[pl.ds(0, 2)], hr1.at[s])
        for d in range(2):
            fwd1(d, s).start()

        @pl.when((s >= FIRST) & (s < FIRST + RELAY))
        def _():
            for d in range(2):
                pass1(d, s).start()

    wait_all(snd1, fr1)
    wait_all(rcv1.at[pl.ds(0, 2 * RELAY)], ysem.at[0, 1])

    zs2, zf2, sh2 = zsend(sown, colp2, 1), zfwd(colp2, 1), share(sown, colp2, 1)
    hop2 = functools.partial(hop, snd2, rcv2, hs2, hr2, q2 - LATE)
    fwd2 = functools.partial(fwd, rcv2, fs2, fr2, q2 - LATE)
    pass2 = functools.partial(relay, rcv2, 1, q2 - LATE)

    @pl.loop(0, 3 + OWN // 2)
    def _(t):
        listed = (t == 0) | (t == 4) | (t == 5)
        slot = jnp.where(listed, jnp.maximum(t - 3, 0), 0)
        at = jnp.where(listed, 3, jnp.where(t < 4, t - 1, t - 3))
        step = at // 3

        @pl.when(t == 4)
        def _():
            zs2.start()

        row = step + core * (RA - 1 - 2 * step)
        for d in range(2):
            own_entry = row * KB + (at - 3 * step) * 2 + d
            entry = jnp.where(listed, list_entry(1, d, slot), own_entry)
            block = product(colp1, rcv1, 0, entry // KB, entry).astype(jnp.bfloat16)
            snd2[d, jnp.where(listed, slot, q2 - 1)] = block
            sown[own_entry] = block
            colp2[own0 + own_entry] = block

        @pl.when(listed)
        def _():
            hop2(0, slot).start()

        @pl.when(t == 1)
        def _():
            hop2(1, 0).start()

        @pl.when((t == 5) | (t == 6))
        def _():
            hop2(1, t - 4).start()

    @pl.loop(3, FIRST)
    def _(s):
        for d in range(2):
            snd2[d, s] = sown[list_entry(1, d, s)]

        @pl.when(s > 3)
        def _():
            for d in range(2):
                hop2(d, s - 1).start()

    sh2.start()
    for d in range(2):
        hop2(d, FIRST - 1).start()
    zs2.wait_recv()
    zf2.start()
    sh2.wait_recv()
    zf2.wait_recv()

    @pl.loop(FIRST, q2 - LATE)
    def _(s):
        for d in range(2):
            snd2[d, s] = colp2[sent(1, d, s)]

        @pl.when(s > FIRST)
        def _():
            for d in range(2):
                hop2(d, s - 1).start()

    for i in range(LATE):
        s = q2 - LATE + i
        for d in range(2):
            snd2[d, s] = colp2[sent(1, d, s)]
        for d in range(2):
            (late_hop(d, i - 1) if i else hop2(d, s - 1)).start()
    for d in range(2):
        late_hop(d, LATE - 1).start()

    @pl.loop(0, q2 - LATE)
    def _(s):
        wait_all(rcv2.at[pl.ds(0, 2)], hr2.at[s])
        for d in range(2):
            fwd2(d, s).start()

        @pl.when((s >= FIRST) & (s < FIRST + RELAY))
        def _():
            for d in range(2):
                pass2(d, s).start()

    wait_all(rcv2.at[pl.ds(0, 2 * (q2 - LATE))], fr2)
    wait_all(rcv2.at[pl.ds(0, 2 * RELAY)], ysem.at[1, 1])

    def pass_late(i):
        wait_all(rcv2.at[pl.ds(0, 2)], hr2.at[q2 - LATE + i])
        for d in range(2):
            late_fwd(d, i).start()

    @pl.loop(0, OWN // 2)
    def _(t):
        row = t // 3
        for u in range(2):
            entry = 2 * t + u
            cubed = product(colp2, rcv2, 1, row, entry)
            in_use = tab[1 + RA * core + row, NEAR_AT + 8 * (entry - row * KB) + 1] >= 0
            own = xv[entry].astype(jnp.float32)
            step = 1.5 * own - cubed * (0.5 / (KB * B))
            out_ref[entry] = jnp.where(in_use, step, 0.0).astype(jnp.bfloat16)
            acc_ref[entry] = cubed

        for i, when in enumerate((5, 10)):

            @pl.when(t == when)
            def _():
                pass_late(i)

    wait_all(late.at[pl.ds(0, 2 * LATE)], lr2)
    zs1.wait_send()
    zf1.wait_send()
    sh1.wait_send()
    zs2.wait_send()
    zf2.wait_send()
    sh2.wait_send()
    for snd, rcv, hs, fs, p in ((snd1, rcv1, hs1, fs1, 0), (snd2, rcv2, hs2, fs2, 1)):
        wait_all(snd, hs)
        wait_all(snd, fs)
        wait_all(rcv.at[pl.ds(0, 2 * RELAY)], ysem.at[p, 0])


def sparse(level, grid_a, grid_c, x_blocks, table):
    q1, q2 = LEVELS[level]
    blocks = x_blocks.reshape(OWN, B, B)
    vm = lambda *lead: pltpu.VMEM((*lead, B, B), jnp.bfloat16)
    dma = lambda *lead: pltpu.SemaphoreType.DMA(lead)
    held = OWN + 2 * COLN + 2 + 6 * (q1 + q2) + 4 * RELAY + 16
    out, acc, late, xv, todo = pl.pallas_call(
        functools.partial(kernel, q1, q2, grid_a, grid_c, lax.axis_size("grp"), lax.axis_size("col")),
        out_shape=(
            pltpu.VMEM(blocks.shape, jnp.bfloat16),
            pltpu.VMEM(blocks.shape, jnp.float32),
            pltpu.VMEM((4 * LATE, B, B), jnp.bfloat16),
            pltpu.VMEM(blocks.shape, jnp.bfloat16),
            pltpu.VMEM((8, LANES), jnp.int32),
        ),
        in_specs=[
            pl.BlockSpec(memory_space=pltpu.SMEM),
            pl.BlockSpec(memory_space=pl.ANY),
        ],
        out_specs=tuple(pl.BlockSpec(memory_space=pltpu.VMEM) for _ in range(5)),
        scratch_shapes=[
            pltpu.SMEM((2 * PICKS,), jnp.int32),
            vm(COLN + 1), vm(4 * q1 + 2 * RELAY), vm(2, q1), vm(COLN + 1),
            vm(4 * (q2 - LATE) + 2 * RELAY), vm(2, q2), vm(OWN),
            dma(2), dma(2, 6),
            dma(), dma(q1), dma(), dma(), dma(), dma(q2), dma(), dma(), dma(), dma(2, 2),
        ],
        compiler_params=pltpu.CompilerParams(
            collective_id=level, has_side_effects=True, vmem_limit_bytes=held * B * B * 2
        ),
        name=f"sign_step_{q1}_{q2}",
    )(table, blocks)
    return finished(todo, out, acc, late, xv).reshape(x_blocks.shape)


def finish_kernel(todo, out_ref, acc_ref, late, xv, res, some, total, fixed, sem):
    def write(src, entry):
        return pltpu.make_async_copy(src.at[entry], res.at[entry], sem)

    @pl.loop(0, KF)
    def _(f):
        for row in range(RA):
            entry = row * KB + f
            latest = todo[f, row * KB]
            for k in range(1, KB):
                latest = jnp.maximum(latest, todo[f, row * KB + k])
            some[entry] = latest

            @pl.when(latest < 0)
            def _():
                write(out_ref, entry).start()

    @pl.loop(0, OWN)
    def _(entry):
        @pl.when(some[entry] >= 0)
        def _():
            row, f = entry // KB, entry % KB
            total[...] = acc_ref[entry]
            for k in range(KB):
                code = todo[f, row * KB + k]

                @pl.when(code >= 0)
                def _():
                    total[...] += jnp.dot(
                        xv[row * KB + k],
                        late[jnp.clip(code, 0, 4 * LATE - 1)],
                        preferred_element_type=jnp.float32,
                    )

            own = xv[entry].astype(jnp.float32)
            fixed[entry] = (1.5 * own - total[...] * (0.5 / (KB * B))).astype(jnp.bfloat16)

    @pl.loop(0, OWN)
    def _(entry):
        @pl.when(some[entry] >= 0)
        def _():
            write(fixed, entry).start()

    pltpu.make_async_copy(out_ref, res, sem).wait()


def finished(todo, out, acc, late, xv):
    return pl.pallas_call(
        finish_kernel,
        out_shape=jax.ShapeDtypeStruct(out.shape, out.dtype),
        in_specs=[pl.BlockSpec(memory_space=pltpu.SMEM)]
        + [pl.BlockSpec(memory_space=pltpu.VMEM)] * 4,
        out_specs=pl.BlockSpec(memory_space=pl.ANY),
        scratch_shapes=[
            pltpu.SMEM((OWN,), jnp.int32),
            pltpu.VMEM((B, B), jnp.float32),
            pltpu.VMEM(out.shape, out.dtype),
            pltpu.SemaphoreType.DMA(()),
        ],
        compiler_params=pltpu.CompilerParams(vmem_limit_bytes=20 * 1024 * 1024),
        name="finish",
    )(todo, out, acc, late, xv)


def local(x_blocks, columns, filter_ids):
    grid_a, grid_c, _ = columns.shape
    table, level = list_tables(columns, filter_ids)
    branches = [
        functools.partial(lambda at, x, c, f, t: sparse(at, grid_a, grid_c, x, t), at)
        for at in range(len(LEVELS))
    ]
    branches.append(lambda x, c, f, t: dense(x, c, f))
    return lax.switch(level[0], branches, x_blocks, columns, filter_ids, table)


def solution(mesh):
    return jax.shard_map(
        local,
        mesh=mesh,
        in_specs=(P("grp", "col", None, None, None), P(), P()),
        out_specs=P("grp", "col", None, None, None),
        check_vma=False,
    )
```
